32 devices in a mesh: seq: 2 (over x), tp: 4 (over z), pp: 4 (over y, core).
Axes of the slice: x: 2, y: 2, z: 4, core: 2. Of those that a mesh axis runs over, the one named last changes fastest.
Arguments:
- queries: bfloat16 [4, 384, 8192], P('pp', 'seq', 'tp'), may hold values from -40 to 40
- keys: bfloat16 [4, 384, 1024], P('pp', 'seq', 'tp'), may hold values from -16 to 16
- values: bfloat16 [4, 384, 1024], P('pp', 'seq', 'tp'), may hold values from -6 to 6
- doc_lengths: int32 [4, 8], P('pp'), may hold values from 1 to 288, 384 in all within a row
- resid: bfloat16 [4, 384, 5120], P('pp', 'seq', 'tp'), may hold values from -8 to 8
- ffn_gain: float32 [4, 5120], P('pp'), may hold values from 0.1 to 1.9
- w_gate: bfloat16 [4, 5120, 12800], P('pp', None, ('seq', 'tp')), may hold values from -0.078125 to 0.078125
- w_up: bfloat16 [4, 5120, 12800], P('pp', None, ('seq', 'tp')), may hold values from -0.078125 to 0.078125
- w_down: bfloat16 [4, 12800, 5120], P('pp', 'seq', 'tp'), may hold values from -0.0546875 to 0.0546875
- kv_gain: float32 [4, 5120], P('pp'), may hold values from 0.1 to 1.9
- key_value_weight: bfloat16 [4, 5120, 2048], P('pp', 'tp'), may hold values from -0.078125 to 0.078125
- k_gain: float32 [4, 128], P('pp'), may hold values from 0.1 to 1.9
Outputs:
- attn_out: bfloat16 [4, 384, 8192], P('pp', 'seq', 'tp')
- layer_out: bfloat16 [4, 384, 5120], P('pp', 'seq', 'tp')
- kv_next: bfloat16 [4, 384, 2048], P('pp', 'seq', 'tp')
The draws below stay inside these ranges and needn't reach their ends.
All inputs are finite; a program needn't handle non-finite values.
Results may differ from the reference program's by a relative error of at most 0.019.
Values may be sent and summed in bfloat16 or wider, within the bound.
A program may use at most 192 MiB of HBM per device.

```python
import math
import jax
import jax.numpy as jnp
import numpy as np
from jax import lax

MODEL_WIDTH = 5120
FF = 12800
QUERY_HEADS = 64
KEY_VALUE_HEADS = 8
HEAD_SIZE = 128
DOCS = 8
BATCH_TOKENS = 384
RELAY_SECTIONS = 4
DOC_MOST = 288


def query_key_pair(key):
    random_keys = jax.random.split(jax.random.fold_in(key, 4242), 2)
    query_bulk = 1.6 * jnp.clip(jax.random.normal(random_keys[0], (RELAY_SECTIONS, BATCH_TOKENS, QUERY_HEADS, HEAD_SIZE), jnp.float32), -6.0, 6.0)
    key_mass = jnp.clip(jax.random.normal(random_keys[1], (RELAY_SECTIONS, BATCH_TOKENS, KEY_VALUE_HEADS, HEAD_SIZE), jnp.float32), -6.0, 6.0)
    query_final = jnp.clip(query_bulk, -40.0, 40.0).reshape(RELAY_SECTIONS, BATCH_TOKENS, QUERY_HEADS * HEAD_SIZE)
    key_ending = jnp.clip(key_mass, -16.0, 16.0).reshape(RELAY_SECTIONS, BATCH_TOKENS, KEY_VALUE_HEADS * HEAD_SIZE)
    return (query_final, key_ending)


def draw_queries(key, part):
    return query_key_pair(key)[0].astype(jnp.bfloat16)


def draw_keys(key, part):
    return query_key_pair(key)[1].astype(jnp.bfloat16)


def draw_resid(key, part):
    random_keys = jax.random.split(jax.random.fold_in(key, 77), 3)
    row_scales = jnp.exp(jax.random.uniform(random_keys[0], (RELAY_SECTIONS, BATCH_TOKENS, 1), jnp.float32, math.log(0.3), math.log(3.0)))
    rising = (1.0 + 2.0 * jnp.arange(MODEL_WIDTH, dtype=jnp.float32) / (MODEL_WIDTH - 1)) / 2.0
    col_scales = jnp.exp(jax.random.uniform(random_keys[1], (RELAY_SECTIONS, 1, MODEL_WIDTH), jnp.float32, math.log(0.3), math.log(3.0))) * rising[None, None, :]
    base_values = jax.random.normal(random_keys[2], (RELAY_SECTIONS, BATCH_TOKENS, MODEL_WIDTH), jnp.float32)
    return jnp.clip(0.5 * base_values * row_scales * col_scales, -8.0, 8.0).astype(jnp.bfloat16)


def block_levels(key, shape, cuts, low, top_value):
    def one(position, blocks):
        heights = jax.random.uniform(jax.random.fold_in(jax.random.fold_in(key, 6), position), (blocks,), jnp.float32, low / len(cuts), top_value / len(cuts))
        return jnp.repeat(jnp.exp(heights), shape[position] // blocks).reshape((-1,) + (1,) * (len(shape) - position - 1))

    factor_of = one(*cuts[0])
    for cut in cuts[1:]:
        factor_of = factor_of * one(*cut)
    return factor_of


def length_profile(number_of, total, most, slope):
    portions = [(1 << 20) // math.isqrt(standing ** slope) + 1 for standing in range(2, number_of + 1)]
    spare, given = total - most - (number_of - 1), [1] * (number_of - 1)
    while spare > 0:
        candidates = [i for i in range(number_of - 1) if given[i] < most]
        pool, left = sum([portions[i] for i in candidates]), spare
        for i in candidates:
            addition = min(most - given[i], max(1, left * portions[i] // pool), spare)
            given[i] = given[i] + addition
            spare = spare - addition
    return np.array([most] + given)


def uneven(key, count, total, most, slope):
    if count == 2:
        one = jax.random.randint(key, (), max(1, total - most), min(most, total - 1) + 1)
        return jnp.stack([one, total - one])
    tallies = jnp.asarray(length_profile(count, total, most, slope), jnp.int32)
    pairs = (count - 1) // 2
    giver, sink = tallies[1:1 + 2 * pairs:2], tallies[2:2 + 2 * pairs:2]
    margin = jnp.minimum(giver - 1, most - sink)
    passed = jax.random.randint(jax.random.fold_in(key, 1), (pairs,), 0, 1 << 20) % (margin + 1)
    tallies = tallies.at[1:1 + 2 * pairs:2].set(giver - passed).at[2:2 + 2 * pairs:2].set(sink + passed)
    return tallies[jax.random.permutation(jax.random.fold_in(key, 2), count)]


def gaussian(own_key, extent, width, most, cuts=(), kind=jnp.bfloat16):
    values = jax.random.normal(own_key, extent, jnp.float32) * width
    if len(cuts) > 0:
        values = block_levels(own_key, extent, cuts, -0.22, 0.18) * values
    return jnp.clip(values, min=-most, max=most).astype(kind)


def setup_inputs(seed: int = 0) -> dict:
    key_of = jax.random.split(jax.random.key(seed), 13)
    return {
        "queries": draw_queries(jax.random.fold_in(key_of[12], 71), 0),
        "keys": draw_keys(jax.random.fold_in(key_of[12], 71), 0),
        "values": gaussian(key_of[2], (RELAY_SECTIONS, BATCH_TOKENS, KEY_VALUE_HEADS * HEAD_SIZE), 1.0, 6.0, ((0, 4), (1, 2), (2, 4))),
        "doc_lengths": jax.vmap(lambda own: uneven(own, DOCS, BATCH_TOKENS, DOC_MOST, 2))(jax.random.split(key_of[3], RELAY_SECTIONS)).reshape((RELAY_SECTIONS, DOCS)).astype(jnp.int32),
        "resid": draw_resid(jax.random.fold_in(key_of[12], 71), 0),
        "ffn_gain": jnp.clip(1.0 + 0.18 * jax.random.normal(key_of[5], (RELAY_SECTIONS, MODEL_WIDTH), jnp.float32), 0.1, 1.9),
        "w_gate": gaussian(key_of[6], (RELAY_SECTIONS, MODEL_WIDTH, FF), MODEL_WIDTH ** -0.5, 0.078125, ((0, 4), (2, 8))),
        "w_up": gaussian(key_of[7], (RELAY_SECTIONS, MODEL_WIDTH, FF), MODEL_WIDTH ** -0.5, 0.078125, ((0, 4), (2, 8))),
        "w_down": gaussian(key_of[8], (RELAY_SECTIONS, FF, MODEL_WIDTH), FF ** -0.5, 0.0546875, ((0, 4), (1, 2), (2, 4))),
        "kv_gain": jnp.clip(1.0 + 0.18 * jax.random.normal(key_of[9], (RELAY_SECTIONS, MODEL_WIDTH), jnp.float32), 0.1, 1.9),
        "key_value_weight": gaussian(key_of[10], (RELAY_SECTIONS, MODEL_WIDTH, 2 * KEY_VALUE_HEADS * HEAD_SIZE), MODEL_WIDTH ** -0.5, 0.078125, ((0, 4), (1, 4))),
        "k_gain": jnp.clip(1.0 + 0.18 * jax.random.normal(key_of[11], (RELAY_SECTIONS, HEAD_SIZE), jnp.float32), 0.1, 1.9),
    }


epsilon = 1e-06
negative = -1e+30

def document_ids(lengths, tally_count):
    bounds = jnp.cumsum(lengths).astype(jnp.int32)
    places = jnp.arange(tally_count, dtype=jnp.int32)
    return lax.optimization_barrier(jnp.sum((places[:, None] >= bounds[None, :]).astype(jnp.int32), axis=1))

def attend_group(query_group, key_group, value_group, visible):
    scores = jnp.einsum('tgd,sd->gts', query_group.astype(jnp.float32), key_group.astype(jnp.float32)) / math.sqrt(HEAD_SIZE)
    masked = jnp.where(visible[None], scores, negative)
    row_peak = lax.optimization_barrier(jnp.max(masked, axis=2, keepdims=True))
    exponent = jnp.where(visible[None], jnp.exp(masked - row_peak), 0.0)
    row_total = lax.optimization_barrier(jnp.sum(exponent, axis=2))
    weights = lax.optimization_barrier(exponent.astype(jnp.bfloat16)).astype(jnp.float32)
    mixed = jnp.einsum('gts,sd->tgd', weights, value_group.astype(jnp.float32))
    return mixed / jnp.transpose(row_total)[:, :, None]

def attend_segment(operands):
    queries, keys, values, lengths = operands
    tally_count = queries.shape[0]
    docs = document_ids(lengths, tally_count)
    places = jnp.arange(tally_count, dtype=jnp.int32)
    visible = (docs[:, None] == docs[None, :]) & (places[None, :] <= places[:, None])
    query_per_head = jnp.moveaxis(queries.reshape(tally_count, KEY_VALUE_HEADS, QUERY_HEADS // KEY_VALUE_HEADS, HEAD_SIZE), 1, 0)
    key_per_head = jnp.moveaxis(keys.reshape(tally_count, KEY_VALUE_HEADS, HEAD_SIZE), 1, 0)
    value_per_head = jnp.moveaxis(values.reshape(tally_count, KEY_VALUE_HEADS, HEAD_SIZE), 1, 0)
    mixed = lax.map(lambda triple: attend_group(triple[0], triple[1], triple[2], visible), (query_per_head, key_per_head, value_per_head))
    return jnp.moveaxis(mixed, 0, 1).reshape(tally_count, QUERY_HEADS * HEAD_SIZE).astype(jnp.bfloat16)

def ffn_segment(operands):
    resid, gain, gate_weight, up_weight, down_weight = operands
    wide = resid.astype(jnp.float32)
    inverse = lax.rsqrt(lax.optimization_barrier(jnp.mean(wide * wide, axis=-1, keepdims=True)) + epsilon)
    normed = (wide * inverse * gain[None, :]).astype(jnp.bfloat16)
    gate_total = jnp.dot(normed, gate_weight, preferred_element_type=jnp.float32)
    up_total = jnp.dot(normed, up_weight, preferred_element_type=jnp.float32)
    hidden = (jax.nn.silu(gate_total) * up_total).astype(jnp.bfloat16)
    return (wide + jnp.dot(hidden, down_weight, preferred_element_type=jnp.float32)).astype(jnp.bfloat16)

def kv_segment(operands):
    incoming, gain, kv_weight, key_gain = operands
    tally_count = incoming.shape[0]
    wide = incoming.astype(jnp.float32)
    inverse = lax.rsqrt(lax.optimization_barrier(jnp.mean(wide * wide, axis=-1, keepdims=True)) + epsilon)
    kv_input = (wide * inverse * gain[None, :]).astype(jnp.bfloat16)
    mapped_rows = jnp.dot(kv_input, kv_weight, preferred_element_type=jnp.float32)
    key_portion = mapped_rows[:, :KEY_VALUE_HEADS * HEAD_SIZE].reshape(tally_count, KEY_VALUE_HEADS, HEAD_SIZE)
    key_square = lax.optimization_barrier(jnp.mean(key_portion * key_portion, axis=2, keepdims=True))
    key_after_norm = key_portion * lax.rsqrt(key_square + epsilon) * key_gain[None, None, :]
    combined = jnp.concatenate([key_after_norm.reshape(tally_count, KEY_VALUE_HEADS * HEAD_SIZE), mapped_rows[:, KEY_VALUE_HEADS * HEAD_SIZE:]], axis=1)
    return combined.astype(jnp.bfloat16)

def reference(queries, keys, values, doc_lengths, resid, ffn_gain, w_gate, w_up, w_down, kv_gain, key_value_weight, k_gain):
    attn_out = lax.map(attend_segment, (queries, keys, values, doc_lengths))
    layer_out = lax.map(ffn_segment, (resid, ffn_gain, w_gate, w_up, w_down))
    incoming = jnp.roll(layer_out, 1, axis=0)
    kv_next = lax.map(kv_segment, (incoming, kv_gain, key_value_weight, k_gain))
    return (attn_out, layer_out, kv_next)
```

```python
import functools
import math

import jax
import jax.numpy as jnp
from jax import lax
from jax.experimental import pallas as pl
from jax.experimental.pallas import tpu as pltpu
from jax.sharding import PartitionSpec as P

MODEL_WIDTH = 5120
QUERY_HEADS = 64
KEY_VALUE_HEADS = 8
HEAD_SIZE = 128


epsilon = 1e-06
negative = -1e30


def passed_along(block, axis, distance):
    count = lax.axis_size(axis)
    return lax.ppermute(block, axis, [(i, (i + distance) % count) for i in range(count)])


def passed_where(block, distance, places):
    seq_count = lax.axis_size("seq")
    tp_count = lax.axis_size("tp")
    route = [
        (s * tp_count + t, ((s + distance) % seq_count) * tp_count + t)
        for s in range(seq_count)
        for t in places
    ]
    return lax.ppermute(block, ("seq", "tp"), route)


def line_gather(block):
    count = lax.axis_size("tp")
    slots = {0: block}
    for k in range(1, count):
        slots[-k] = lax.ppermute(
            slots[1 - k], "tp", [(i, i + 1) for i in range(k - 1, count - 1)]
        )
        slots[k] = lax.ppermute(
            slots[k - 1], "tp", [(i, i - 1) for i in range(1, count - k + 1)]
        )
    return slots


def valid_places(offset, count):
    return [t for t in range(count) if 0 <= t + offset < count]


def pick(slots, offsets, tp_rank):
    picked = slots[offsets[0]]
    for t in range(1, len(offsets)):
        if offsets[t] != offsets[t - 1] or len(set(offsets)) > 1:
            picked = jnp.where(tp_rank == t, slots[offsets[t]], picked)
    return picked


def arrival_order(count):
    table = []
    for t in range(count):
        order = [0]
        for k in range(1, count):
            order += [d for d in (-k, k) if 0 <= t + d < count]
        table.append(order)
    return table


def document_ids(places, bounds):
    return jnp.sum((places[:, None] >= bounds[None, :]).astype(jnp.int32), axis=1)


def seq_gather(block):
    count = lax.axis_size("seq")
    rank = lax.axis_index("seq")
    rows = block.shape[0]
    whole = jnp.zeros((count * rows, block.shape[1]), block.dtype)
    for k in range(count):
        part = block if k == 0 else passed_along(block, "seq", k)
        whole = lax.dynamic_update_slice_in_dim(whole, part, lax.rem(rank - k + count, count) * rows, 0)
    return whole


def attend_rows(query_rows, query_places, keys_local, values_local, lengths):
    bounds = jnp.cumsum(lengths)
    query_docs = document_ids(query_places, bounds)
    row_count = query_rows.shape[0]
    kv_heads = keys_local.shape[1] // HEAD_SIZE
    group_width = QUERY_HEADS // KEY_VALUE_HEADS
    query_four = query_rows.reshape(row_count, kv_heads, group_width, HEAD_SIZE)
    inv_root = 1.0 / math.sqrt(HEAD_SIZE)
    key_piece = seq_gather(keys_local)
    value_piece = seq_gather(values_local)
    key_count = key_piece.shape[0]

    key_places = jnp.arange(key_count, dtype=jnp.int32)
    key_docs = document_ids(key_places, bounds)
    visible = (query_docs[:, None] == key_docs[None, :]) & (
        key_places[None, :] <= query_places[:, None]
    )
    scores = (
        jnp.einsum(
            "rkgd,nkd->kgrn",
            query_four,
            key_piece.reshape(key_count, kv_heads, HEAD_SIZE),
            preferred_element_type=jnp.float32,
        )
        * inv_root
    )
    masked = jnp.where(visible, scores, negative)
    row_max = jnp.max(masked, axis=3)
    exponent = jnp.where(visible, jnp.exp(masked - row_max[..., None]), 0.0)
    running_sum = jnp.sum(exponent, axis=3)
    weighted = jnp.einsum(
        "kgrn,nkd->kgrd",
        exponent.astype(jnp.bfloat16),
        value_piece.reshape(key_count, kv_heads, HEAD_SIZE),
        preferred_element_type=jnp.float32,
    )
    mixed = weighted / running_sum[..., None]
    return (
        jnp.transpose(mixed, (2, 0, 1, 3))
        .reshape(row_count, kv_heads * group_width * HEAD_SIZE)
        .astype(jnp.bfloat16)
    )


def plain_body(
    queries,
    keys,
    values,
    doc_lengths,
    resid,
    ffn_gain,
    w_gate,
    w_up,
    w_down,
    kv_gain,
    key_value_weight,
    k_gain,
):
    seq_count = lax.axis_size("seq")
    seq_rank = lax.axis_index("seq")
    tp_count = lax.axis_size("tp")
    tp_rank = lax.axis_index("tp")
    tok_rows = queries.shape[1]
    lengths = doc_lengths[0]
    query_local = queries[0]
    query_places = seq_rank * tok_rows + jnp.arange(tok_rows, dtype=jnp.int32)
    attended = attend_rows(query_local, query_places, keys[0], values[0], lengths)
    resid_local = resid[0]
    wide = resid_local.astype(jnp.float32)
    features = resid_local.shape[1]
    hidden_local = w_gate.shape[2]
    slots = line_gather(resid_local)
    groups = [slots]
    for k in range(1, seq_count):
        groups.append(
            {d: passed_where(slots[d], k, valid_places(d, tp_count)) for d in sorted(slots, key=abs)}
        )
    gain = ffn_gain[0]
    table = arrival_order(tp_count)
    down_weight = w_down[0]
    totals = []
    ready = None
    for group in groups:
        if ready is not None:
            offsets_here = sorted(group)
            tied = lax.optimization_barrier(tuple(group[d] for d in offsets_here) + (ready,))
            group = dict(zip(offsets_here, tied[:-1]))
        pieces = [
            pick(group, [j - t for t in range(tp_count)], tp_rank).astype(jnp.float32)
            for j in range(tp_count)
        ]
        squares = sum(jnp.sum(piece * piece, axis=1) for piece in pieces)
        inverse = lax.rsqrt(squares / MODEL_WIDTH + epsilon)
        normed = jnp.concatenate(
            [
                (
                    pieces[j] * inverse[:, None] * gain[None, j * features : (j + 1) * features]
                ).astype(jnp.bfloat16)
                for j in range(tp_count)
            ],
            axis=1,
        )
        gate_total = jnp.dot(normed, w_gate[0], preferred_element_type=jnp.float32)
        up_total = jnp.dot(normed, w_up[0], preferred_element_type=jnp.float32)
        hidden = (jax.nn.silu(gate_total) * up_total).astype(jnp.bfloat16)
        ready = hidden
        hidden_slots = line_gather(hidden)
        total = None
        for m in range(tp_count):
            offsets = [table[t][m] for t in range(tp_count)]
            block = pick(hidden_slots, offsets, tp_rank)
            place = tp_rank + jnp.asarray(offsets, jnp.int32)[tp_rank]
            rows = lax.dynamic_slice_in_dim(down_weight, place * hidden_local, hidden_local)
            term = jnp.dot(block, rows, preferred_element_type=jnp.float32)
            total = term if total is None else total + term
        totals.append(total)
    update_rows = totals[0]
    for k in range(1, seq_count):
        update_rows = update_rows + passed_along(
            totals[k].astype(jnp.bfloat16), "seq", -k
        ).astype(jnp.float32)
    layer_local = (wide + update_rows).astype(jnp.bfloat16)
    incoming = passed_along(layer_local, "pp", 1)
    incoming_wide = incoming.astype(jnp.float32)
    own_square = jnp.sum(incoming_wide * incoming_wide, axis=1)
    incoming_total = own_square
    for k in range(1, tp_count):
        incoming_total = incoming_total + passed_along(own_square, "tp", k)
    scale_rows = lax.rsqrt(incoming_total / MODEL_WIDTH + epsilon)
    kv_gain_part = lax.dynamic_slice_in_dim(kv_gain[0], tp_rank * features, features)
    kv_input = (incoming_wide * kv_gain_part[None, :]).astype(jnp.bfloat16)
    kv_weight = key_value_weight[0]
    span = kv_weight.shape[1] // tp_count
    mapped_rows = jnp.dot(kv_input, kv_weight, preferred_element_type=jnp.float32)
    kv_span = lax.dynamic_slice_in_dim(mapped_rows, tp_rank * span, span, 1)
    mapped_bits = mapped_rows.astype(jnp.bfloat16)
    for k in range(1, tp_count):
        part = lax.dynamic_slice_in_dim(mapped_bits, lax.rem(tp_rank + k, tp_count) * span, span, 1)
        kv_span = kv_span + passed_along(part, "tp", k).astype(jnp.float32)
    kv_span = kv_span * scale_rows[:, None]
    span_width = kv_span.shape[1]
    heads_here = span_width // HEAD_SIZE
    divide_heads = kv_span.reshape(tok_rows, heads_here, HEAD_SIZE)
    mean_square = jnp.mean(divide_heads * divide_heads, axis=2, keepdims=True)
    norm_applied = divide_heads * lax.rsqrt(mean_square + epsilon) * k_gain[0][None, None, :]
    head_index_list = tp_rank * heads_here + jnp.arange(heads_here, dtype=jnp.int32)
    kv_result = (
        jnp.where((head_index_list < KEY_VALUE_HEADS)[None, :, None], norm_applied, divide_heads)
        .reshape(tok_rows, span_width)
        .astype(jnp.bfloat16)
    )
    return (attended[None], layer_local[None], kv_result[None])


MESH = pl.DeviceIdType.MESH


def relay_kernel(
    sizes,
    lengths_ref,
    queries_ref,
    keys_ref,
    values_ref,
    resid_ref,
    ffn_gain_ref,
    w_gate_ref,
    w_up_ref,
    w_down_ref,
    kv_gain_ref,
    kv_weight_ref,
    k_gain_ref,
    attn_ref,
    layer_ref,
    kv_next_ref,
    gate_w,
    up_w,
    down_w,
    x_buf,
    h_buf,
    g_buf,
    own_acc,
    other_acc,
    part_in,
    stream_in,
    y_buf,
    kv_in,
    kv_own,
    square_buf,
    kv_out,
    local_sem,
    out_sem,
    xz_send,
    xz_recv,
    xs_send,
    xs_recv,
    a_send,
    a_recv,
    h_send,
    h_recv,
    p_send,
    p_recv,
    r_send,
    r_recv,
    kv_send,
    kv_recv,
    sq_send,
    sq_recv,
):
    seq_count, tp_count, pp_count = sizes
    s = lax.axis_index("seq")
    t = lax.axis_index("tp")
    p = lax.axis_index("pp")
    rows = resid_ref.shape[1]
    features = resid_ref.shape[2]
    units = w_gate_ref.shape[1]
    width = w_gate_ref.shape[2]
    span = kv_next_ref.shape[2]
    half = rows // 2
    tail = 32 if half % 32 == 0 and half > 32 else 16
    kv_heads = keys_ref.shape[2] // HEAD_SIZE
    group = queries_ref.shape[2] // keys_ref.shape[2]
    group_span = group * HEAD_SIZE

    pieces = (
        (0, half),
        (rows, half),
        (rows + half, half),
        (half, half - tail),
        (rows - tail, tail),
    )
    own_pieces = (0, 3, 4)

    def rows_of(c):
        return pl.ds(c * half, half)

    def remote(src, dst, send, recv, where):
        return pltpu.make_async_remote_copy(
            src_ref=src,
            dst_ref=dst,
            send_sem=send,
            recv_sem=recv,
            device_id=where,
            device_id_type=MESH,
        )

    def next_on_line(d):
        return lax.rem(t + 2 * d - 1 + tp_count, tp_count)

    def has_next(d):
        place = t + 2 * d - 1
        return (place >= 0) & (place < tp_count)

    def x_line(d, c, block, own=False):
        dst = x_buf.at[0, block, rows_of(c)]
        src = resid_ref.at[0, rows_of(c)] if own else dst
        return remote(
            src, dst, xz_send.at[d, c, block], xz_recv.at[d, c, block], {"tp": next_on_line(d)}
        )

    def x_across(c, block, own=False):
        src = resid_ref.at[0, rows_of(c)] if own else x_buf.at[0, block, rows_of(c)]
        return remote(
            src,
            x_buf.at[1, block, rows_of(c)],
            xs_send.at[c, block],
            xs_recv.at[c, block],
            {"seq": 1 - s},
        )

    def h_line(d, piece, block):
        first, count = pieces[piece]
        ref = h_buf.at[block, pl.ds(first, count)]
        return remote(
            ref, ref, h_send.at[d, piece, block], h_recv.at[d, piece, block], {"tp": next_on_line(d)}
        )

    key_row = kv_heads * rows
    kv_width = kv_heads * HEAD_SIZE

    def query_place(i):
        return down_w.at[pl.ds(i * rows, rows), pl.ds(0, group_span)]

    def key_place(side, which):
        return down_w.at[
            pl.ds(key_row + side * rows, rows), pl.ds(which * kv_width, kv_width)
        ]

    attn_rows = key_row + seq_count * rows

    def a_across(which):
        src = keys_ref if which == 0 else values_ref
        return remote(
            src.at[0],
            key_place(s, which),
            a_send.at[which],
            a_recv.at[which],
            {"seq": 1 - s},
        )

    def a_arrived(which):
        src = keys_ref if which == 0 else values_ref
        return remote(
            src.at[0],
            key_place(1 - s, which),
            a_send.at[which],
            a_recv.at[which],
            {"seq": 1 - s},
        )

    loads = {}

    def load(name, src, dst):
        loads[name] = pltpu.make_async_copy(src, dst, local_sem.at[len(loads)])
        loads[name].start()

    for i in range(kv_heads):
        load(
            ("q", i),
            queries_ref.at[0, :, pl.ds(i * group_span, group_span)],
            query_place(i),
        )
    load("k", keys_ref.at[0], key_place(s, 0))
    load("v", values_ref.at[0], key_place(s, 1))
    load("x", resid_ref.at[0], x_buf.at[0, t])
    load("gate", w_gate_ref.at[0], gate_w)
    load("up", w_up_ref.at[0], up_w)
    down_rows = w_down_ref.shape[1]
    load(
        "down1",
        w_down_ref.at[0, pl.ds(attn_rows, down_rows - attn_rows)],
        down_w.at[pl.ds(attn_rows, down_rows - attn_rows)],
    )

    barrier = pltpu.get_barrier_semaphore()
    for k in range(1, tp_count):
        pl.semaphore_signal(
            barrier, inc=1, device_id={"tp": lax.rem(t + k, tp_count)}, device_id_type=MESH
        )
    pl.semaphore_signal(barrier, inc=1, device_id={"seq": 1 - s}, device_id_type=MESH)
    for k in (1, pp_count - 1):
        pl.semaphore_signal(
            barrier, inc=1, device_id={"pp": lax.rem(p + k, pp_count)}, device_id_type=MESH
        )
    pl.semaphore_wait(barrier, tp_count - 1 + 1 + 2)

    def send_own_x(d, c, when):
        @pl.when(has_next(d) & when)
        def _():
            x_line(d, c, t, True).start()

    late_low = (t >= 2) & (t <= tp_count - 2)
    late_high = (t >= 1) & (t <= tp_count - 3)
    always = t >= 0
    a_across(0).start()
    a_across(1).start()
    for d in (0, 1):
        send_own_x(d, 0, always)
    x_across(0, t, True).start()
    send_own_x(0, 1, jnp.logical_not(late_low))
    send_own_x(1, 1, jnp.logical_not(late_high))

    def x_events(c, k):
        for d in (0, 1):
            block = t + k * (1 - 2 * d)
            block_safe = lax.rem(block + tp_count, tp_count)

            @pl.when((block >= 0) & (block < tp_count))
            def _():
                x_line(d, c, block_safe).wait_recv()

                @pl.when(has_next(d))
                def _():
                    x_line(d, c, block_safe).start()

                x_across(c, block_safe).start()

    bias = own_acc.at[:, pl.ds(0, seq_count * rows)]
    row_id = lax.broadcasted_iota(jnp.int32, (rows, seq_count * rows), 0) + s * rows
    col_id = lax.broadcasted_iota(jnp.int32, (rows, seq_count * rows), 1)
    bound = lengths_ref[0, 0]
    begin = jnp.zeros_like(row_id)
    for k in range(1, lengths_ref.shape[1]):
        begin = jnp.where(row_id >= bound, bound, begin)
        bound = bound + lengths_ref[0, k]
    own_acc[:, : seq_count * rows] = jnp.where(
        (col_id <= row_id) & (col_id >= begin), 0.0, negative
    )
    inv_root = 1.0 / math.sqrt(HEAD_SIZE)

    def attend(first, last):
        def one(index, carry):
            i = index // group
            j = lax.rem(index, group)
            place = pl.ds(pl.multiple_of(i * rows, 16), rows)
            lanes = pl.ds(pl.multiple_of(j * HEAD_SIZE, HEAD_SIZE), HEAD_SIZE)
            query = down_w[place, lanes]
            key = down_w[
                key_row : key_row + seq_count * rows,
                pl.ds(pl.multiple_of(i * HEAD_SIZE, HEAD_SIZE), HEAD_SIZE),
            ]
            value = down_w[
                key_row : key_row + seq_count * rows,
                pl.ds(pl.multiple_of(kv_width + i * HEAD_SIZE, HEAD_SIZE), HEAD_SIZE),
            ]
            scores = lax.dot_general(
                query, key, (((1,), (1,)), ((), ())), preferred_element_type=jnp.float32
            )
            masked = scores * inv_root + bias[...]
            peak = jnp.max(masked, axis=1, keepdims=True)
            expo = jnp.exp(masked - peak)
            total = jnp.sum(expo, axis=1, keepdims=True)
            mixed = jnp.dot(
                expo.astype(jnp.bfloat16), value, preferred_element_type=jnp.float32
            )
            down_w[place, lanes] = (mixed / total).astype(jnp.bfloat16)
            return carry

        lax.fori_loop(first, last, one, 0)

    heads = kv_heads * group
    for i in range(kv_heads):
        loads[("q", i)].wait()
    loads["k"].wait()
    loads["v"].wait()
    a_arrived(0).wait_recv()
    a_arrived(1).wait_recv()
    cuts = [heads * i // 4 for i in range(5)]
    attend(cuts[0], cuts[1])
    x_events(0, 1)
    send_own_x(0, 1, late_low)
    send_own_x(1, 1, late_high)
    attend(cuts[1], cuts[2])
    for k in range(2, tp_count - 1):
        x_events(0, k)
    x_across(1, t, True).start()
    attend(cuts[2], cuts[3])
    x_events(1, 1)
    attend(cuts[3], cuts[4])
    attn_copies = [
        pltpu.make_async_copy(
            query_place(i),
            attn_ref.at[0, :, pl.ds(i * group_span, group_span)],
            out_sem.at[i],
        )
        for i in range(kv_heads)
    ]
    for copy in attn_copies:
        copy.start()
    x_events(0, tp_count - 1)
    loads["x"].wait()
    for copy in attn_copies:
        copy.wait()
    load("down0", w_down_ref.at[0, pl.ds(0, attn_rows)], down_w.at[pl.ds(0, attn_rows)])

    lane_tiles = features // 128
    block_n = 256
    full_tiles = units // block_n
    rest = units - full_tiles * block_n

    def normalise(side, c):
        def squares(block, acc):
            for j in range(lane_tiles):
                x = x_buf[side, block, rows_of(c), j * 128 : (j + 1) * 128].astype(jnp.float32)
                acc = acc + x * x
            return acc

        total = lax.fori_loop(0, tp_count, squares, jnp.zeros((half, 128), jnp.float32))
        inverse = lax.rsqrt(jnp.sum(total, axis=1, keepdims=True) / width + epsilon)

        def write(block, carry):
            for j in range(lane_tiles):
                x = x_buf[side, block, rows_of(c), j * 128 : (j + 1) * 128].astype(jnp.float32)
                lanes = pl.ds(pl.multiple_of(block * features + j * 128, 128), 128)
                g_buf[:, lanes] = (x * inverse * ffn_gain_ref[0:1, lanes]).astype(jnp.bfloat16)
            return carry

        lax.fori_loop(0, tp_count, write, 0)

    def gated(first, lanes):
        both = (((1,), (1,)), ((), ()))
        x = g_buf[...]
        g = lax.dot_general(x, gate_w[lanes, :], both, preferred_element_type=jnp.float32)
        u = lax.dot_general(x, up_w[lanes, :], both, preferred_element_type=jnp.float32)
        h_buf[t, pl.ds(first, half), lanes] = (g / (1.0 + jnp.exp(-g)) * u).astype(jnp.bfloat16)

    def hidden_tiles(first, low, high):
        def one(i, carry):
            gated(first, pl.ds(pl.multiple_of(i * block_n, block_n), block_n))
            return carry

        lax.fori_loop(low, high, one, 0)

    def hidden_rest(first):
        if rest:
            gated(first, pl.ds(full_tiles * block_n, rest))

    def send_hidden(piece):
        for d in (0, 1):

            @pl.when(has_next(d))
            def _():
                h_line(d, piece, t).start()

    def acc_of(piece):
        first, count = pieces[piece]
        if piece in own_pieces:
            return own_acc.at[pl.ds(first, count)]
        return other_acc.at[pl.ds(0, count)]

    down_n = 256 if features % 256 == 0 else 128

    def down(piece, block, fresh):
        first, count = pieces[piece]
        acc = acc_of(piece)

        def one(i, carry):
            lanes = pl.ds(pl.multiple_of(i * down_n, down_n), down_n)
            term = jnp.dot(
                h_buf[block, pl.ds(first, count), :],
                down_w[pl.ds(pl.multiple_of(block * units, 16), units), lanes],
                preferred_element_type=jnp.float32,
            )
            if fresh:
                acc[:, lanes] = term
            else:
                acc[:, lanes] += term
            return carry

        lax.fori_loop(0, features // down_n, one, 0)

    def hidden_events(piece, low, high):
        def one(index, carry):
            k = index // 2 + 1
            d = lax.rem(index, 2)
            block = t + k * (1 - 2 * d)
            block_safe = lax.rem(block + tp_count, tp_count)

            @pl.when((block >= 0) & (block < tp_count))
            def _():
                h_line(d, piece, block_safe).wait_recv()

                @pl.when(has_next(d))
                def _():
                    h_line(d, piece, block_safe).start()

                down(piece, block_safe, False)

            return carry

        lax.fori_loop(2 * (low - 1), 2 * (high - 1), one, 0)

    def wait_other_x(c):
        def one(block, carry):
            x_across(c, block).wait_recv()
            return carry

        lax.fori_loop(0, tp_count, one, 0)

    def part_copy(c):
        return remote(
            x_buf.at[1, 0, rows_of(c)],
            part_in.at[rows_of(c)],
            p_send.at[c],
            p_recv.at[c],
            {"seq": 1 - s},
        )

    def send_part(c):
        x_buf[1, 0, rows_of(c)] = other_acc[...].astype(jnp.bfloat16)
        part_copy(c).start()

    def stream_copy(q):
        first, count = pieces[own_pieces[q]]
        return remote(
            x_buf.at[1, 1, pl.ds(first, count)],
            stream_in.at[pl.ds(first, count)],
            r_send.at[q],
            r_recv.at[q],
            {"pp": lax.rem(p + 1, pp_count)},
        )

    def layer_copy(q):
        first, count = pieces[own_pieces[q]]
        return pltpu.make_async_copy(
            x_buf.at[1, 1, pl.ds(first, count)],
            layer_ref.at[0, pl.ds(first, count)],
            out_sem.at[kv_heads + q],
        )

    def finish_layer(q):
        first, count = pieces[own_pieces[q]]
        place = pl.ds(first, count)
        x_buf[1, 1, place] = (
            x_buf[0, t, place].astype(jnp.float32)
            + (own_acc[place, :] + part_in[place, :].astype(jnp.float32))
        ).astype(jnp.bfloat16)
        stream_copy(q).start()
        layer_copy(q).start()

    def kv_place(q, k):
        first, count = pieces[own_pieces[q]]
        c = first // half
        return pl.ds(first - c * half, count), pl.ds((c * tp_count + k) * span, span)

    def kv_copy(q, k, source, target):
        first, count = pieces[own_pieces[q]]
        part, lanes = kv_place(q, k)
        return remote(
            g_buf.at[part, lanes],
            kv_in.at[source, pl.ds(first, count)],
            kv_send.at[q, k],
            kv_recv.at[q, source],
            {"tp": target},
        )

    def square_copy(q, k, source, target):
        first, count = pieces[own_pieces[q]]
        ref = square_buf.at[source, pl.ds(first, count)]
        return remote(ref, ref, sq_send.at[q, k], sq_recv.at[q, source], {"tp": target})

    def start_kv(q):
        first, count = pieces[own_pieces[q]]
        place = pl.ds(first, count)
        stream_copy(q).wait_recv()
        total = jnp.zeros((count, 128), jnp.float32)
        for j in range(lane_tiles):
            lanes = slice(j * 128, (j + 1) * 128)
            x = stream_in[place, lanes].astype(jnp.float32)
            total = total + x * x
            gain = kv_gain_ref[0:1, pl.ds(pl.multiple_of(t * features + j * 128, 128), 128)]
            y_buf[0:count, lanes] = (x * gain).astype(jnp.bfloat16)
        square_buf[t, place, :] = total
        for k in range(1, tp_count):
            square_copy(q, k, t, lax.rem(t + k, tp_count)).start()
        for k in list(range(1, tp_count)) + [0]:
            target = lax.rem(t + k, tp_count)
            term = jnp.dot(
                y_buf[0:count, :],
                gate_w[0:features, pl.ds(pl.multiple_of(target * span, HEAD_SIZE), span)],
                preferred_element_type=jnp.float32,
            )
            if k:
                part, lanes = kv_place(q, k)
                g_buf[part, lanes] = term.astype(jnp.bfloat16)
                kv_copy(q, k, t, target).start()
            else:
                kv_own[place, :] = term

    def kv_out_copy(q):
        first, count = pieces[own_pieces[q]]
        return pltpu.make_async_copy(
            kv_out.at[pl.ds(first, count)],
            kv_next_ref.at[0, pl.ds(first, count)],
            out_sem.at[kv_heads + 3 + q],
        )

    def finish_kv(q):
        first, count = pieces[own_pieces[q]]
        place = pl.ds(first, count)
        total = kv_own[place, :]
        square = square_buf[t, place, :]
        for k in range(1, tp_count):
            source = lax.rem(t + tp_count - k, tp_count)
            kv_copy(q, k, source, t).wait_recv()
            square_copy(q, k, source, t).wait_recv()
            total = total + kv_in[source, place, :].astype(jnp.float32)
            square = square + square_buf[source, place, :]
        scale = lax.rsqrt(jnp.sum(square, axis=1, keepdims=True) / width + epsilon)
        total = total * scale
        heads_here = span // HEAD_SIZE
        for h in range(heads_here):
            lanes = slice(h * HEAD_SIZE, (h + 1) * HEAD_SIZE)
            x = total[:, lanes]
            mean_square = jnp.mean(x * x, axis=1, keepdims=True)
            after = x * lax.rsqrt(mean_square + epsilon) * k_gain_ref[0:1, :]
            head = jnp.zeros_like(x, jnp.int32) + (t * heads_here + h)
            kv_out[place, lanes] = jnp.where(head < KEY_VALUE_HEADS, after, x).astype(jnp.bfloat16)
        kv_out_copy(q).start()

    last = tp_count
    loads["gate"].wait()
    loads["up"].wait()
    normalise(0, 0)
    hidden_tiles(0, 0, full_tiles)
    hidden_rest(0)
    for k in range(2, tp_count - 1):
        x_events(1, k)
    send_hidden(0)
    wait_other_x(0)
    normalise(1, 0)
    hidden_tiles(rows, 0, full_tiles // 2)
    x_events(1, tp_count - 1)
    hidden_tiles(rows, full_tiles // 2, full_tiles)
    hidden_rest(rows)
    send_hidden(1)
    loads["down0"].wait()
    loads["down1"].wait()
    down(0, t, True)
    hidden_events(0, 1, 2)
    normalise(0, 1)
    hidden_tiles(half, 0, full_tiles)
    hidden_rest(half)
    hidden_events(0, 2, last)
    wait_other_x(1)
    normalise(1, 1)
    hidden_tiles(rows + half, 0, full_tiles)
    hidden_rest(rows + half)
    send_hidden(2)
    send_hidden(3)
    send_hidden(4)
    load(
        "kv",
        kv_weight_ref.at[0],
        gate_w.at[pl.ds(0, features), pl.ds(0, tp_count * span)],
    )
    down(1, t, True)
    hidden_events(1, 1, last)
    send_part(0)
    down(2, t, True)
    hidden_events(2, 1, 2)
    part_copy(0).wait_recv()
    finish_layer(0)
    hidden_events(2, 2, last)
    send_part(1)
    loads["kv"].wait()
    down(3, t, True)
    hidden_events(3, 1, 2)
    start_kv(0)
    hidden_events(3, 2, last)
    part_copy(1).wait_recv()
    finish_layer(1)
    finish_kv(0)
    down(4, t, True)
    hidden_events(4, 1, 2)
    start_kv(1)
    hidden_events(4, 2, last)
    finish_layer(2)
    finish_kv(1)
    start_kv(2)
    finish_kv(2)

    def sends_left(c, carry):
        def one(block, inner):
            for d in (0, 1):
                came = (block - t) * (1 - 2 * d) >= 0

                @pl.when(has_next(d) & came)
                def _():
                    x_line(d, c, block).wait_send()

            x_across(c, block).wait_send()
            return inner

        return lax.fori_loop(0, tp_count, one, carry)

    lax.fori_loop(0, 2, sends_left, 0)
    for piece in range(len(pieces)):

        def one(block, carry):
            for d in (0, 1):
                came = (block - t) * (1 - 2 * d) >= 0

                @pl.when(has_next(d) & came)
                def _():
                    h_line(d, piece, block).wait_send()

            return carry

        lax.fori_loop(0, tp_count, one, 0)
    for which in (0, 1):
        a_across(which).wait_send()
        part_copy(which).wait_send()
    for q in range(3):
        stream_copy(q).wait_send()
        layer_copy(q).wait()
        kv_out_copy(q).wait()
        for k in range(1, tp_count):
            kv_copy(q, k, t, lax.rem(t + k, tp_count)).wait_send()
            square_copy(q, k, t, lax.rem(t + k, tp_count)).wait_send()


def fits(shape, queries, keys, doc_lengths, resid, w_gate, w_down, key_value_weight):
    rows, features = resid.shape[1:]
    units = w_gate.shape[2]
    span = key_value_weight.shape[2] // shape["tp"]
    tp_span = key_value_weight.shape[2]
    group_span = HEAD_SIZE * queries.shape[2] // keys.shape[2]
    return (
        shape["seq"] == 2
        and shape["pp"] >= 3
        and shape["tp"] >= 3
        and rows % 64 == 0
        and features % 128 == 0
        and units % 16 == 0
        and span % HEAD_SIZE == 0
        and features <= units
        and tp_span <= resid.shape[2] * shape["tp"]
        and 2 * span <= features
        and group_span <= features
        and keys.shape[2] * 2 <= features
        and 2 * rows <= features
        and queries.shape[2] // group_span * rows + 2 * rows < w_down.shape[1]
    )


def body(
    shape,
    queries,
    keys,
    values,
    doc_lengths,
    resid,
    ffn_gain,
    w_gate,
    w_up,
    w_down,
    kv_gain,
    key_value_weight,
    k_gain,
):
    if not fits(shape, queries, keys, doc_lengths, resid, w_gate, w_down, key_value_weight):
        return plain_body(
            queries,
            keys,
            values,
            doc_lengths,
            resid,
            ffn_gain,
            w_gate,
            w_up,
            w_down,
            kv_gain,
            key_value_weight,
            k_gain,
        )
    sizes = (shape["seq"], shape["tp"], shape["pp"])
    tp_count = shape["tp"]
    rows, features = resid.shape[1:]
    width, units = w_gate.shape[1:]
    span = key_value_weight.shape[2] // tp_count
    half = rows // 2
    kv_heads = keys.shape[2] // HEAD_SIZE
    bf16, f32 = jnp.bfloat16, jnp.float32
    hbm = pl.BlockSpec(memory_space=pl.ANY)
    vmem = pl.BlockSpec(memory_space=pltpu.VMEM)
    smem = pl.BlockSpec(memory_space=pltpu.SMEM)
    dma = pltpu.SemaphoreType.DMA
    return tuple(
        pl.pallas_call(
            functools.partial(relay_kernel, sizes),
            out_shape=(
                jax.ShapeDtypeStruct(queries.shape, bf16),
                jax.ShapeDtypeStruct(resid.shape, bf16),
                jax.ShapeDtypeStruct((1, rows, span), bf16),
            ),
            in_specs=[smem, hbm, hbm, hbm, hbm, vmem, hbm, hbm, hbm, vmem, hbm, vmem],
            out_specs=(hbm, hbm, hbm),
            scratch_shapes=[
                pltpu.VMEM((units, width), bf16),
                pltpu.VMEM((units, width), bf16),
                pltpu.VMEM(w_down.shape[1:], bf16),
                pltpu.VMEM((2, tp_count, rows, features), bf16),
                pltpu.VMEM((tp_count, 2 * rows, units), bf16),
                pltpu.VMEM((half, width), bf16),
                pltpu.VMEM((rows, features), f32),
                pltpu.VMEM((half, features), f32),
                pltpu.VMEM((rows, features), bf16),
                pltpu.VMEM((rows, features), bf16),
                pltpu.VMEM((half, features), bf16),
                pltpu.VMEM((tp_count, rows, span), bf16),
                pltpu.VMEM((rows, span), f32),
                pltpu.VMEM((tp_count, rows, 128), f32),
                pltpu.VMEM((rows, span), bf16),
                dma((kv_heads + 8,)),
                dma((kv_heads + 6,)),
                dma((2, 2, tp_count)),
                dma((2, 2, tp_count)),
                dma((2, tp_count)),
                dma((2, tp_count)),
                dma((2,)),
                dma((2,)),
                dma((2, 5, tp_count)),
                dma((2, 5, tp_count)),
                dma((2,)),
                dma((2,)),
                dma((3,)),
                dma((3,)),
                dma((3, tp_count)),
                dma((3, tp_count)),
                dma((3, tp_count)),
                dma((3, tp_count)),
            ],
            compiler_params=pltpu.CompilerParams(
                collective_id=0, has_side_effects=True, vmem_limit_bytes=67043328
            ),
            name="relay_step",
        )(
            doc_lengths,
            queries,
            keys,
            values,
            resid,
            ffn_gain,
            jnp.swapaxes(w_gate, 1, 2),
            jnp.swapaxes(w_up, 1, 2),
            w_down,
            kv_gain,
            key_value_weight,
            k_gain,
        )
    )


def solution(mesh):
    placed = (
        P("pp", "seq", "tp"),
        P("pp", "seq", "tp"),
        P("pp", "seq", "tp"),
        P("pp", None),
        P("pp", "seq", "tp"),
        P("pp", None),
        P("pp", None, ("seq", "tp")),
        P("pp", None, ("seq", "tp")),
        P("pp", "seq", "tp"),
        P("pp", None),
        P("pp", "tp", None),
        P("pp", None),
    )
    return jax.shard_map(
        functools.partial(body, dict(mesh.shape)),
        mesh=mesh,
        in_specs=placed,
        out_specs=(P("pp", "seq", "tp"), P("pp", "seq", "tp"), P("pp", "seq", "tp")),
        check_vma=False,
    )
```

```python
import functools
import math

import jax
import jax.numpy as jnp
from jax import lax
from jax.experimental import pallas as pl
from jax.experimental.pallas import tpu as pltpu
from jax.sharding import PartitionSpec as P

MODEL_WIDTH = 5120
QUERY_HEADS = 64
KEY_VALUE_HEADS = 8
HEAD_SIZE = 128


epsilon = 1e-06
negative = -1e30


def passed_along(block, axis, distance):
    count = lax.axis_size(axis)
    return lax.ppermute(block, axis, [(i, (i + distance) % count) for i in range(count)])


def passed_where(block, distance, places):
    seq_count = lax.axis_size("seq")
    tp_count = lax.axis_size("tp")
    route = [
        (s * tp_count + t, ((s + distance) % seq_count) * tp_count + t)
        for s in range(seq_count)
        for t in places
    ]
    return lax.ppermute(block, ("seq", "tp"), route)


def line_gather(block):
    count = lax.axis_size("tp")
    slots = {0: block}
    for k in range(1, count):
        slots[-k] = lax.ppermute(
            slots[1 - k], "tp", [(i, i + 1) for i in range(k - 1, count - 1)]
        )
        slots[k] = lax.ppermute(
            slots[k - 1], "tp", [(i, i - 1) for i in range(1, count - k + 1)]
        )
    return slots


def valid_places(offset, count):
    return [t for t in range(count) if 0 <= t + offset < count]


def pick(slots, offsets, tp_rank):
    picked = slots[offsets[0]]
    for t in range(1, len(offsets)):
        if offsets[t] != offsets[t - 1] or len(set(offsets)) > 1:
            picked = jnp.where(tp_rank == t, slots[offsets[t]], picked)
    return picked


def arrival_order(count):
    table = []
    for t in range(count):
        order = [0]
        for k in range(1, count):
            order += [d for d in (-k, k) if 0 <= t + d < count]
        table.append(order)
    return table


def document_ids(places, bounds):
    return jnp.sum((places[:, None] >= bounds[None, :]).astype(jnp.int32), axis=1)


def seq_gather(block):
    count = lax.axis_size("seq")
    rank = lax.axis_index("seq")
    rows = block.shape[0]
    whole = jnp.zeros((count * rows, block.shape[1]), block.dtype)
    for k in range(count):
        part = block if k == 0 else passed_along(block, "seq", k)
        whole = lax.dynamic_update_slice_in_dim(whole, part, lax.rem(rank - k + count, count) * rows, 0)
    return whole


def attend_rows(query_rows, query_places, keys_local, values_local, lengths):
    bounds = jnp.cumsum(lengths)
    query_docs = document_ids(query_places, bounds)
    row_count = query_rows.shape[0]
    kv_heads = keys_local.shape[1] // HEAD_SIZE
    group_width = QUERY_HEADS // KEY_VALUE_HEADS
    query_four = query_rows.reshape(row_count, kv_heads, group_width, HEAD_SIZE)
    inv_root = 1.0 / math.sqrt(HEAD_SIZE)
    key_piece = seq_gather(keys_local)
    value_piece = seq_gather(values_local)
    key_count = key_piece.shape[0]

    key_places = jnp.arange(key_count, dtype=jnp.int32)
    key_docs = document_ids(key_places, bounds)
    visible = (query_docs[:, None] == key_docs[None, :]) & (
        key_places[None, :] <= query_places[:, None]
    )
    scores = (
        jnp.einsum(
            "rkgd,nkd->kgrn",
            query_four,
            key_piece.reshape(key_count, kv_heads, HEAD_SIZE),
            preferred_element_type=jnp.float32,
        )
        * inv_root
    )
    masked = jnp.where(visible, scores, negative)
    row_max = jnp.max(masked, axis=3)
    exponent = jnp.where(visible, jnp.exp(masked - row_max[..., None]), 0.0)
    running_sum = jnp.sum(exponent, axis=3)
    weighted = jnp.einsum(
        "kgrn,nkd->kgrd",
        exponent.astype(jnp.bfloat16),
        value_piece.reshape(key_count, kv_heads, HEAD_SIZE),
        preferred_element_type=jnp.float32,
    )
    mixed = weighted / running_sum[..., None]
    return (
        jnp.transpose(mixed, (2, 0, 1, 3))
        .reshape(row_count, kv_heads * group_width * HEAD_SIZE)
        .astype(jnp.bfloat16)
    )


def plain_body(
    queries,
    keys,
    values,
    doc_lengths,
    resid,
    ffn_gain,
    w_gate,
    w_up,
    w_down,
    kv_gain,
    key_value_weight,
    k_gain,
):
    seq_count = lax.axis_size("seq")
    seq_rank = lax.axis_index("seq")
    tp_count = lax.axis_size("tp")
    tp_rank = lax.axis_index("tp")
    tok_rows = queries.shape[1]
    lengths = doc_lengths[0]
    query_local = queries[0]
    query_places = seq_rank * tok_rows + jnp.arange(tok_rows, dtype=jnp.int32)
    attended = attend_rows(query_local, query_places, keys[0], values[0], lengths)
    resid_local = resid[0]
    wide = resid_local.astype(jnp.float32)
    features = resid_local.shape[1]
    hidden_local = w_gate.shape[2]
    slots = line_gather(resid_local)
    groups = [slots]
    for k in range(1, seq_count):
        groups.append(
            {d: passed_where(slots[d], k, valid_places(d, tp_count)) for d in sorted(slots, key=abs)}
        )
    gain = ffn_gain[0]
    table = arrival_order(tp_count)
    down_weight = w_down[0]
    totals = []
    ready = None
    for group in groups:
        if ready is not None:
            offsets_here = sorted(group)
            tied = lax.optimization_barrier(tuple(group[d] for d in offsets_here) + (ready,))
            group = dict(zip(offsets_here, tied[:-1]))
        pieces = [
            pick(group, [j - t for t in range(tp_count)], tp_rank).astype(jnp.float32)
            for j in range(tp_count)
        ]
        squares = sum(jnp.sum(piece * piece, axis=1) for piece in pieces)
        inverse = lax.rsqrt(squares / MODEL_WIDTH + epsilon)
        normed = jnp.concatenate(
            [
                (
                    pieces[j] * inverse[:, None] * gain[None, j * features : (j + 1) * features]
                ).astype(jnp.bfloat16)
                for j in range(tp_count)
            ],
            axis=1,
        )
        gate_total = jnp.dot(normed, w_gate[0], preferred_element_type=jnp.float32)
        up_total = jnp.dot(normed, w_up[0], preferred_element_type=jnp.float32)
        hidden = (jax.nn.silu(gate_total) * up_total).astype(jnp.bfloat16)
        ready = hidden
        hidden_slots = line_gather(hidden)
        total = None
        for m in range(tp_count):
            offsets = [table[t][m] for t in range(tp_count)]
            block = pick(hidden_slots, offsets, tp_rank)
            place = tp_rank + jnp.asarray(offsets, jnp.int32)[tp_rank]
            rows = lax.dynamic_slice_in_dim(down_weight, place * hidden_local, hidden_local)
            term = jnp.dot(block, rows, preferred_element_type=jnp.float32)
            total = term if total is None else total + term
        totals.append(total)
    update_rows = totals[0]
    for k in range(1, seq_count):
        update_rows = update_rows + passed_along(
            totals[k].astype(jnp.bfloat16), "seq", -k
        ).astype(jnp.float32)
    layer_local = (wide + update_rows).astype(jnp.bfloat16)
    incoming = passed_along(layer_local, "pp", 1)
    incoming_wide = incoming.astype(jnp.float32)
    own_square = jnp.sum(incoming_wide * incoming_wide, axis=1)
    incoming_total = own_square
    for k in range(1, tp_count):
        incoming_total = incoming_total + passed_along(own_square, "tp", k)
    scale_rows = lax.rsqrt(incoming_total / MODEL_WIDTH + epsilon)
    kv_gain_part = lax.dynamic_slice_in_dim(kv_gain[0], tp_rank * features, features)
    kv_input = (incoming_wide * kv_gain_part[None, :]).astype(jnp.bfloat16)
    kv_weight = key_value_weight[0]
    span = kv_weight.shape[1] // tp_count
    mapped_rows = jnp.dot(kv_input, kv_weight, preferred_element_type=jnp.float32)
    kv_span = lax.dynamic_slice_in_dim(mapped_rows, tp_rank * span, span, 1)
    mapped_bits = mapped_rows.astype(jnp.bfloat16)
    for k in range(1, tp_count):
        part = lax.dynamic_slice_in_dim(mapped_bits, lax.rem(tp_rank + k, tp_count) * span, span, 1)
        kv_span = kv_span + passed_along(part, "tp", k).astype(jnp.float32)
    kv_span = kv_span * scale_rows[:, None]
    span_width = kv_span.shape[1]
    heads_here = span_width // HEAD_SIZE
    divide_heads = kv_span.reshape(tok_rows, heads_here, HEAD_SIZE)
    mean_square = jnp.mean(divide_heads * divide_heads, axis=2, keepdims=True)
    norm_applied = divide_heads * lax.rsqrt(mean_square + epsilon) * k_gain[0][None, None, :]
    head_index_list = tp_rank * heads_here + jnp.arange(heads_here, dtype=jnp.int32)
    kv_result = (
        jnp.where((head_index_list < KEY_VALUE_HEADS)[None, :, None], norm_applied, divide_heads)
        .reshape(tok_rows, span_width)
        .astype(jnp.bfloat16)
    )
    return (attended[None], layer_local[None], kv_result[None])


MESH = pl.DeviceIdType.MESH


def relay_kernel(
    sizes,
    lengths_ref,
    queries_ref,
    keys_ref,
    values_ref,
    resid_ref,
    ffn_gain_ref,
    w_gate_ref,
    w_up_ref,
    w_down_ref,
    kv_gain_ref,
    kv_weight_ref,
    k_gain_ref,
    attn_ref,
    layer_ref,
    kv_next_ref,
    gate_w,
    up_w,
    down_w,
    x_buf,
    h_buf,
    h_tail,
    g_buf,
    own_acc,
    other_acc,
    part_in,
    stream_in,
    y_buf,
    kv_in,
    kv_own,
    square_buf,
    square_tmp,
    kv_out,
    local_sem,
    out_sem,
    xz_send,
    xz_recv,
    xs_send,
    xs_recv,
    a_send,
    a_recv,
    h_send,
    h_recv,
    p_send,
    p_recv,
    r_send,
    r_recv,
    kv_send,
    kv_recv,
    sq_send,
    sq_recv,
    relay_recv,
    relay_sum,
):
    seq_count, tp_count, pp_count = sizes
    s = lax.axis_index("seq")
    t = lax.axis_index("tp")
    p = lax.axis_index("pp")
    rows = resid_ref.shape[1]
    features = resid_ref.shape[2]
    units = w_gate_ref.shape[1]
    width = w_gate_ref.shape[2]
    span = kv_next_ref.shape[2]
    half = rows // 2
    tail = 32 if half % 32 == 0 and half > 32 else 16
    kv_heads = keys_ref.shape[2] // HEAD_SIZE
    group = queries_ref.shape[2] // keys_ref.shape[2]
    group_span = group * HEAD_SIZE

    pieces = (
        (0, 0, half),
        (half, 0, half),
        (3 * half, half, half),
        (2 * half, half, half - tail),
        (3 * half - tail, rows - tail, tail),
    )
    main = units // 128 * 128
    rest = units - main
    block_n = 256 if main % 256 == 0 else 128
    full_tiles = main // block_n
    split = full_tiles // 2 * block_n
    early, late = (0,), (1, 2) if rest else (1,)
    whole = early + late
    own_pieces = (0, 3, 4)

    def rows_of(c):
        return pl.ds(c * half, half)

    def remote(src, dst, send, recv, where):
        return pltpu.make_async_remote_copy(
            src_ref=src,
            dst_ref=dst,
            send_sem=send,
            recv_sem=recv,
            device_id=where,
            device_id_type=MESH,
        )

    def next_on_line(d):
        return lax.rem(t + 2 * d - 1 + tp_count, tp_count)

    def has_next(d):
        place = t + 2 * d - 1
        return (place >= 0) & (place < tp_count)

    def x_line(d, c, block, own=False):
        dst = x_buf.at[0, block, rows_of(c)]
        src = resid_ref.at[0, rows_of(c)] if own else dst
        return remote(
            src, dst, xz_send.at[d, c, block], xz_recv.at[d, c, block], {"tp": next_on_line(d)}
        )

    def x_across(c, block, own=False):
        src = resid_ref.at[0, rows_of(c)] if own else x_buf.at[0, block, rows_of(c)]
        return remote(
            src,
            x_buf.at[1, block, rows_of(c)],
            xs_send.at[c, block],
            xs_recv.at[c, block],
            {"seq": 1 - s},
        )

    def h_line(d, piece, block, sub):
        first, _, count = pieces[piece]
        if sub == 2:
            ref = h_tail.at[block, pl.ds(first // 2, count // 2)]
        else:
            lanes = pl.ds(0, split) if sub == 0 else pl.ds(split, main - split)
            ref = h_buf.at[block, pl.ds(first, count), lanes]
        return remote(
            ref,
            ref,
            h_send.at[d, piece, block, sub],
            h_recv.at[d, piece, block, sub],
            {"tp": next_on_line(d)},
        )

    key_row = kv_heads * rows
    kv_width = kv_heads * HEAD_SIZE

    def query_place(i):
        return down_w.at[pl.ds(i * rows, rows), pl.ds(0, group_span)]

    def key_place(side, which):
        return down_w.at[
            pl.ds(key_row + side * rows, rows), pl.ds(which * kv_width, kv_width)
        ]

    attn_rows = key_row + seq_count * rows

    def a_across(which):
        src = keys_ref if which == 0 else values_ref
        return remote(
            src.at[0],
            key_place(s, which),
            a_send.at[which],
            a_recv.at[which],
            {"seq": 1 - s},
        )

    def a_arrived(which):
        src = keys_ref if which == 0 else values_ref
        return remote(
            src.at[0],
            key_place(1 - s, which),
            a_send.at[which],
            a_recv.at[which],
            {"seq": 1 - s},
        )

    loads = {}

    def load(name, src, dst):
        loads[name] = pltpu.make_async_copy(src, dst, local_sem.at[len(loads)])
        loads[name].start()

    for i in range(kv_heads):
        load(
            ("q", i),
            queries_ref.at[0, :, pl.ds(i * group_span, group_span)],
            query_place(i),
        )
    load("k", keys_ref.at[0], key_place(s, 0))
    load("v", values_ref.at[0], key_place(s, 1))
    load("x", resid_ref.at[0], x_buf.at[0, t])
    load("gate", w_gate_ref.at[0], gate_w)
    load("up", w_up_ref.at[0], up_w)
    down_rows = w_down_ref.shape[1]
    load(
        "down1",
        w_down_ref.at[0, pl.ds(attn_rows, down_rows - attn_rows)],
        down_w.at[pl.ds(attn_rows, down_rows - attn_rows)],
    )

    barrier = pltpu.get_barrier_semaphore()
    for k in range(1, tp_count):
        pl.semaphore_signal(
            barrier, inc=1, device_id={"tp": lax.rem(t + k, tp_count)}, device_id_type=MESH
        )
    pl.semaphore_signal(barrier, inc=1, device_id={"seq": 1 - s}, device_id_type=MESH)
    for k in (1, pp_count - 1):
        pl.semaphore_signal(
            barrier, inc=1, device_id={"pp": lax.rem(p + k, pp_count)}, device_id_type=MESH
        )
    pl.semaphore_wait(barrier, tp_count - 1 + 1 + 2)

    def send_own_x(d, c, when):
        @pl.when(has_next(d) & when)
        def _():
            x_line(d, c, t, True).start()

    late_low = (t >= 2) & (t <= tp_count - 2)
    late_high = (t >= 1) & (t <= tp_count - 3)
    always = t >= 0
    a_across(0).start()
    a_across(1).start()
    for d in (0, 1):
        send_own_x(d, 0, always)
    x_across(0, t, True).start()
    send_own_x(0, 1, jnp.logical_not(late_low))
    send_own_x(1, 1, jnp.logical_not(late_high))

    def x_events(c, k):
        for d in (0, 1):
            block = t + k * (1 - 2 * d)
            block_safe = lax.rem(block + tp_count, tp_count)

            @pl.when((block >= 0) & (block < tp_count))
            def _():
                x_line(d, c, block_safe).wait_recv()

                @pl.when(has_next(d))
                def _():
                    x_line(d, c, block_safe).start()

                x_across(c, block_safe).start()

    bias = own_acc.at[:, pl.ds(0, seq_count * rows)]
    row_id = lax.broadcasted_iota(jnp.int32, (rows, seq_count * rows), 0) + s * rows
    col_id = lax.broadcasted_iota(jnp.int32, (rows, seq_count * rows), 1)
    bound = lengths_ref[0, 0]
    begin = jnp.zeros_like(row_id)
    for k in range(1, lengths_ref.shape[1]):
        begin = jnp.where(row_id >= bound, bound, begin)
        bound = bound + lengths_ref[0, k]
    own_acc[:, : seq_count * rows] = jnp.where(
        (col_id <= row_id) & (col_id >= begin), 0.0, negative
    )
    inv_root = 1.0 / math.sqrt(HEAD_SIZE)

    def attend(first, last):
        def one(index, carry):
            i = index // group
            j = lax.rem(index, group)
            place = pl.ds(pl.multiple_of(i * rows, 16), rows)
            lanes = pl.ds(pl.multiple_of(j * HEAD_SIZE, HEAD_SIZE), HEAD_SIZE)
            query = down_w[place, lanes]
            key = down_w[
                key_row : key_row + seq_count * rows,
                pl.ds(pl.multiple_of(i * HEAD_SIZE, HEAD_SIZE), HEAD_SIZE),
            ]
            value = down_w[
                key_row : key_row + seq_count * rows,
                pl.ds(pl.multiple_of(kv_width + i * HEAD_SIZE, HEAD_SIZE), HEAD_SIZE),
            ]
            scores = lax.dot_general(
                query, key, (((1,), (1,)), ((), ())), preferred_element_type=jnp.float32
            )
            masked = scores * inv_root + bias[...]
            peak = jnp.max(masked, axis=1, keepdims=True)
            expo = jnp.exp(masked - peak)
            total = jnp.sum(expo, axis=1, keepdims=True)
            mixed = jnp.dot(
                expo.astype(jnp.bfloat16), value, preferred_element_type=jnp.float32
            )
            down_w[place, lanes] = (mixed / total).astype(jnp.bfloat16)
            return carry

        lax.fori_loop(first, last, one, 0)

    heads = kv_heads * group
    for i in range(kv_heads):
        loads[("q", i)].wait()
    loads["k"].wait()
    loads["v"].wait()
    a_arrived(0).wait_recv()
    a_arrived(1).wait_recv()
    cuts = [heads * i // 4 for i in range(5)]
    attend(cuts[0], cuts[1])
    x_events(0, 1)
    send_own_x(0, 1, late_low)
    send_own_x(1, 1, late_high)
    attend(cuts[1], cuts[2])
    for k in range(2, tp_count - 1):
        x_events(0, k)
    x_across(1, t, True).start()
    attend(cuts[2], cuts[4])
    attn_copies = [
        pltpu.make_async_copy(
            query_place(i),
            attn_ref.at[0, :, pl.ds(i * group_span, group_span)],
            out_sem.at[i],
        )
        for i in range(kv_heads)
    ]
    for copy in attn_copies:
        copy.start()
    x_events(0, tp_count - 1)
    loads["x"].wait()
    for copy in attn_copies:
        copy.wait()
    load("down0", w_down_ref.at[0, pl.ds(0, attn_rows)], down_w.at[pl.ds(0, attn_rows)])

    lane_tiles = features // 128

    def normalise(side, c, first):
        def squares(block, acc):
            for j in range(lane_tiles):
                x = x_buf[side, block, rows_of(c), j * 128 : (j + 1) * 128].astype(jnp.float32)
                acc = acc + x * x
            return acc

        total = lax.fori_loop(0, tp_count, squares, jnp.zeros((half, 128), jnp.float32))
        inverse = lax.rsqrt(jnp.sum(total, axis=1, keepdims=True) / width + epsilon)

        def write(block, carry):
            for j in range(lane_tiles):
                x = x_buf[side, block, rows_of(c), j * 128 : (j + 1) * 128].astype(jnp.float32)
                lanes = pl.ds(pl.multiple_of(block * features + j * 128, 128), 128)
                g_buf[first : first + half, lanes] = (
                    x * inverse * ffn_gain_ref[0:1, lanes]
                ).astype(jnp.bfloat16)
            return carry

        lax.fori_loop(0, tp_count, write, 0)

    def gated(count, place):
        both = (((1,), (1,)), ((), ()))
        x = g_buf[0:count, :]
        g = lax.dot_general(x, gate_w[place, :], both, preferred_element_type=jnp.float32)
        u = lax.dot_general(x, up_w[place, :], both, preferred_element_type=jnp.float32)
        return g / (1.0 + jnp.exp(-g)) * u

    def hidden_group(group_pieces, hooks):
        first = pieces[group_pieces[0]][0]
        count = sum(pieces[piece][2] for piece in group_pieces)

        def one(i, carry):
            place = pl.ds(pl.multiple_of(i * block_n, block_n), block_n)
            h_buf[t, pl.ds(first, count), place] = gated(count, place).astype(jnp.bfloat16)
            for index, hook in hooks.items():
                pl.when(i == index)(hook)
            return carry

        lax.fori_loop(0, full_tiles, one, 0)
        if rest:
            hidden = gated(count, pl.ds(main, rest))
            for piece in group_pieces:
                start, _, size = pieces[piece]
                low = hidden[start - first : start - first + size // 2]
                high = hidden[start - first + size // 2 : start - first + size]
                h_tail[t, pl.ds(start // 2, size // 2), :] = jnp.concatenate(
                    [low, high], axis=1
                ).astype(jnp.bfloat16)

    def send_hidden(piece, subs):
        for d in (0, 1):

            @pl.when(has_next(d))
            def _():
                for sub in subs:
                    h_line(d, piece, t, sub).start()

    def forward(piece, subs, k):
        if k > tp_count - 2:
            return
        for d in (0, 1):
            block = t + k * (1 - 2 * d)
            block_safe = lax.rem(block + tp_count, tp_count)

            @pl.when((block >= 0) & (block < tp_count) & has_next(d))
            def _():
                for sub in subs:
                    h_line(d, piece, block_safe, sub).wait_recv()
                    h_line(d, piece, block_safe, sub).start()

    def forwards(piece, subs, low):
        for k in range(low, tp_count - 1):
            forward(piece, subs, k)

    down_n = 256 if features % 256 == 0 else 128

    def down(piece, block, fresh):
        first, own_first, count = pieces[piece]
        acc = own_acc.at[pl.ds(own_first, count)] if piece in own_pieces else other_acc
        if rest:
            packed = h_tail[block, pl.ds(first // 2, count // 2), :]
            extra = jnp.concatenate([packed[:, :rest], packed[:, rest:]], axis=0)

        def one(i, carry):
            lanes = pl.ds(pl.multiple_of(i * down_n, down_n), down_n)
            term = jnp.dot(
                h_buf[block, pl.ds(first, count), :],
                down_w[pl.ds(pl.multiple_of(block * units, 16), main), lanes],
                preferred_element_type=jnp.float32,
            )
            if rest:
                term = term + jnp.dot(
                    extra,
                    down_w[pl.ds(pl.multiple_of(block * units + main, 16), rest), lanes],
                    preferred_element_type=jnp.float32,
                )
            if fresh:
                acc[:, lanes] = term
            else:
                acc[:, lanes] += term
            return carry

        lax.fori_loop(0, features // down_n, one, 0)

    def down_others(piece):
        def one(index, carry):
            k = index // 2 + 1
            d = lax.rem(index, 2)
            block = t + k * (1 - 2 * d)
            block_safe = lax.rem(block + tp_count, tp_count)

            @pl.when((block >= 0) & (block < tp_count))
            def _():
                @pl.when(jnp.logical_not(has_next(d)))
                def _():
                    for sub in whole:
                        h_line(d, piece, block_safe, sub).wait_recv()

                down(piece, block_safe, False)

            return carry

        lax.fori_loop(0, 2 * (tp_count - 1), one, 0)

    def wait_other_x(c):
        def one(block, carry):
            x_across(c, block).wait_recv()
            return carry

        lax.fori_loop(0, tp_count, one, 0)

    def part_copy(c):
        return remote(
            x_buf.at[1, 0, rows_of(c)],
            part_in.at[rows_of(c)],
            p_send.at[c],
            p_recv.at[c],
            {"seq": 1 - s},
        )

    def send_part(c):
        x_buf[1, 0, rows_of(c)] = other_acc[...].astype(jnp.bfloat16)
        part_copy(c).start()

    def stream_copy(q):
        _, first, count = pieces[own_pieces[q]]
        return remote(
            x_buf.at[1, 1, pl.ds(first, count)],
            stream_in.at[pl.ds(first, count)],
            r_send.at[q],
            r_recv.at[q],
            {"pp": lax.rem(p + 1, pp_count)},
        )

    def layer_copy(q):
        _, first, count = pieces[own_pieces[q]]
        return pltpu.make_async_copy(
            x_buf.at[1, 1, pl.ds(first, count)],
            layer_ref.at[0, pl.ds(first, count)],
            out_sem.at[kv_heads + q],
        )

    def finish_layer(q):
        _, first, count = pieces[own_pieces[q]]
        place = pl.ds(first, count)
        x_buf[1, 1, place] = (
            x_buf[0, t, place].astype(jnp.float32)
            + (own_acc[place, :] + part_in[place, :].astype(jnp.float32))
        ).astype(jnp.bfloat16)
        stream_copy(q).start()
        layer_copy(q).start()

    def own_place(q):
        _, first, count = pieces[own_pieces[q]]
        return pl.ds(first, count)

    def kv_copy(q, k, source, target):
        return remote(
            g_buf.at[own_place(q), pl.ds(k * span, span)],
            kv_in.at[source, own_place(q)],
            kv_send.at[q, k],
            kv_recv.at[q, source],
            {"tp": target},
        )

    def relay_copy(q, k, slot, target):
        return remote(
            g_buf.at[own_place(q), pl.ds(k * span, span)],
            x_buf.at[1, 2, own_place(q), pl.ds(slot * span, span)],
            kv_send.at[q, k],
            relay_recv.at[q, slot],
            {"tp": target},
        )

    def square_copy(q, k, source, target):
        ref = square_buf.at[q, source]
        return remote(ref, ref, sq_send.at[q, k], sq_recv.at[q, source], {"tp": target})

    def relays(q):
        return q < 2

    def start_kv(q):
        _, first, count = pieces[own_pieces[q]]
        place = pl.ds(first, count)
        stream_copy(q).wait_recv()
        total = jnp.zeros((count, 128), jnp.float32)
        for j in range(lane_tiles):
            lanes = slice(j * 128, (j + 1) * 128)
            x = stream_in[place, lanes].astype(jnp.float32)
            total = total + x * x
            gain = kv_gain_ref[0:1, pl.ds(pl.multiple_of(t * features + j * 128, 128), 128)]
            y_buf[0:count, lanes] = (x * gain).astype(jnp.bfloat16)
        if count < 128:
            square_tmp[...] = jnp.zeros_like(square_tmp)
        square_tmp[0:count, :] = jnp.broadcast_to(
            jnp.sum(total, axis=1, keepdims=True), (count, 128)
        )
        square_buf[q, t] = jnp.transpose(square_tmp[...])[0:8]
        for k in range(1, tp_count):
            square_copy(q, k, t, lax.rem(t + k, tp_count)).start()
        for k in list(range(1, tp_count)) + [0]:
            target = lax.rem(t + k, tp_count)
            term = jnp.dot(
                y_buf[0:count, :],
                gate_w[0:features, pl.ds(pl.multiple_of(target * span, HEAD_SIZE), span)],
                preferred_element_type=jnp.float32,
            )
            if k == 0:
                kv_own[place, :] = term
            elif not relays(q):
                g_buf[place, k * span : (k + 1) * span] = term.astype(jnp.bfloat16)
                kv_copy(q, k, t, target).start()
            else:
                low = (target == 0) & (t >= 1)
                high = (target == tp_count - 1) & (t <= tp_count - 2)
                at_relay = (low & (t == 1)) | (high & (t == tp_count - 2))

                @pl.when(at_relay)
                def _():
                    relay_sum[0:count, :] = term

                @pl.when(jnp.logical_not(at_relay))
                def _():
                    g_buf[place, k * span : (k + 1) * span] = term.astype(jnp.bfloat16)

                @pl.when(low & (t >= 2))
                def _():
                    relay_copy(q, k, lax.rem(t - 2 + tp_count, tp_count), 1).start()

                @pl.when(high & (t <= tp_count - 3))
                def _():
                    slot = lax.rem(2 * tp_count - 3 - t, tp_count)
                    relay_copy(q, k, slot, tp_count - 2).start()

                @pl.when(jnp.logical_not(low) & jnp.logical_not(high))
                def _():
                    kv_copy(q, k, t, target).start()

    def relay_kv(q):
        _, first, count = pieces[own_pieces[q]]
        place = pl.ds(first, count)
        for end, relay in ((0, 1), (tp_count - 1, tp_count - 2)):
            k = (end - relay + tp_count) % tp_count

            @pl.when(t == relay)
            def _():
                total = relay_sum[0:count, :]
                for slot in range(tp_count - 2):
                    relay_copy(q, k, slot, relay).wait_recv()
                    total = total + x_buf[
                        1, 2, place, slot * span : (slot + 1) * span
                    ].astype(jnp.float32)
                g_buf[place, k * span : (k + 1) * span] = total.astype(jnp.bfloat16)
                kv_copy(q, k, t, end).start()

    def kv_out_copy(q):
        _, first, count = pieces[own_pieces[q]]
        return pltpu.make_async_copy(
            kv_out.at[pl.ds(first, count)],
            kv_next_ref.at[0, pl.ds(first, count)],
            out_sem.at[kv_heads + 3 + q],
        )

    def finish_kv(q):
        _, first, count = pieces[own_pieces[q]]
        place = pl.ds(first, count)
        square = square_buf[q, t]
        for k in range(1, tp_count):
            source = lax.rem(t + tp_count - k, tp_count)
            square_copy(q, k, source, t).wait_recv()
            square = square + square_buf[q, source]
        column = jnp.transpose(jnp.broadcast_to(square[0:1], (128, 128)))[0:count, 0:1]
        scale = lax.rsqrt(column / width + epsilon)
        for k in range(1, tp_count):
            source = lax.rem(t + tp_count - k, tp_count)
            through = ((t == 0) & (source > 1)) | (
                (t == tp_count - 1) & (source < tp_count - 2)
            )
            if relays(q):

                @pl.when(jnp.logical_not(through))
                def _():
                    kv_copy(q, k, source, t).wait_recv()
                    kv_own[place, :] += kv_in[source, place, :].astype(jnp.float32)

            else:
                kv_copy(q, k, source, t).wait_recv()
                kv_own[place, :] += kv_in[source, place, :].astype(jnp.float32)
        total = kv_own[place, :]
        total = total * scale
        heads_here = span // HEAD_SIZE
        for h in range(heads_here):
            lanes = slice(h * HEAD_SIZE, (h + 1) * HEAD_SIZE)
            x = total[:, lanes]
            mean_square = jnp.mean(x * x, axis=1, keepdims=True)
            after = x * lax.rsqrt(mean_square + epsilon) * k_gain_ref[0:1, :]
            head = jnp.zeros_like(x, jnp.int32) + (t * heads_here + h)
            kv_out[place, lanes] = jnp.where(head < KEY_VALUE_HEADS, after, x).astype(jnp.bfloat16)
        kv_out_copy(q).start()

    def x_left():
        def one(index, carry):
            c = index // tp_count
            block = lax.rem(index, tp_count)
            for d in (0, 1):
                came = (block - t) * (1 - 2 * d) >= 0

                @pl.when(has_next(d) & came)
                def _():
                    x_line(d, c, block).wait_send()

            x_across(c, block).wait_send()
            return carry

        lax.fori_loop(0, 2 * tp_count, one, 0)

    def hidden_left(piece):
        def one(block, carry):
            for d in (0, 1):
                came = (block - t) * (1 - 2 * d) >= 0

                @pl.when(has_next(d) & came)
                def _():
                    for sub in whole:
                        h_line(d, piece, block, sub).wait_send()

            return carry

        lax.fori_loop(0, tp_count, one, 0)

    def kv_left(q):
        stream_copy(q).wait_send()
        layer_copy(q).wait()
        for k in range(1, tp_count):
            kv_copy(q, k, t, lax.rem(t + k, tp_count)).wait_send()
            square_copy(q, k, t, lax.rem(t + k, tp_count)).wait_send()

    loads["gate"].wait()
    loads["up"].wait()
    normalise(0, 0, 0)
    x_events(1, 1)
    middle = full_tiles // 2 - 1

    def first_half_of_0():
        send_hidden(0, early)
        for k in range(2, tp_count - 1):
            x_events(1, k)

    hidden_group((0,), {middle: first_half_of_0})
    send_hidden(0, late)
    x_events(1, tp_count - 1)
    wait_other_x(0)
    forward(0, early, 1)
    normalise(1, 0, 0)
    forward(0, late, 1)
    normalise(0, 1, half)

    def first_half_of_1():
        send_hidden(1, early)
        forwards(0, late, 2)

    hidden_group(
        (1, 3, 4),
        {
            0: functools.partial(forwards, 0, early, 2),
            middle: first_half_of_1,
            full_tiles - 1: functools.partial(forward, 1, early, 1),
        },
    )
    send_hidden(1, late)
    wait_other_x(1)
    forward(1, late, 1)
    normalise(1, 1, 0)
    forwards(1, early, 2)

    def first_half_of_2():
        send_hidden(2, early)
        forwards(1, late, 2)

    hidden_group((2,), {middle: first_half_of_2})
    send_hidden(2, late)
    send_hidden(3, whole)
    send_hidden(4, whole)
    load(
        "kv",
        kv_weight_ref.at[0],
        gate_w.at[pl.ds(0, features), pl.ds(0, tp_count * span)],
    )
    loads["down0"].wait()
    loads["down1"].wait()
    forward(2, early, 1)
    down(0, t, True)
    forward(2, late, 1)
    down_others(0)
    forwards(2, early, 2)
    down(1, t, True)
    forwards(2, late, 2)
    down_others(1)
    send_part(0)
    forward(3, whole, 1)
    down(2, t, True)
    forward(4, whole, 1)
    x_left()
    down_others(2)
    send_part(1)
    forwards(3, whole, 2)
    part_copy(0).wait_recv()
    finish_layer(0)
    forwards(4, whole, 2)
    hidden_left(0)
    hidden_left(1)
    loads["kv"].wait()
    start_kv(0)
    down(3, t, True)
    relay_kv(0)
    down_others(3)
    part_copy(1).wait_recv()
    finish_layer(1)
    finish_kv(0)
    down(4, t, True)
    hidden_left(2)
    start_kv(1)
    relay_kv(1)
    down_others(4)
    finish_layer(2)
    finish_kv(1)
    for which in (0, 1):
        a_across(which).wait_send()
        part_copy(which).wait_send()
    kv_left(0)
    start_kv(2)
    hidden_left(3)
    hidden_left(4)
    kv_left(1)
    finish_kv(2)
    kv_left(2)
    for q in range(3):
        kv_out_copy(q).wait()


def settle_kernel(a_ref, b_ref, c_ref, a_out, b_out, c_out, a_buf, b_buf, c_buf, sem):
    pairs = ((a_ref, a_buf, a_out), (b_ref, b_buf, b_out), (c_ref, c_buf, c_out))
    into = [pltpu.make_async_copy(src, buf, sem.at[i]) for i, (src, buf, _) in enumerate(pairs)]
    out = [pltpu.make_async_copy(buf, dst, sem.at[3 + i]) for i, (_, buf, dst) in enumerate(pairs)]
    for copy in into:
        copy.start()
    for i in range(3):
        into[i].wait()
        out[i].start()
    for copy in out:
        copy.wait()


def fits(shape, queries, keys, doc_lengths, resid, w_gate, w_down, key_value_weight):
    rows, features = resid.shape[1:]
    units = w_gate.shape[2]
    span = key_value_weight.shape[2] // shape["tp"]
    tp_span = key_value_weight.shape[2]
    group_span = HEAD_SIZE * queries.shape[2] // keys.shape[2]
    return (
        shape["seq"] == 2
        and shape["pp"] >= 3
        and shape["tp"] >= 3
        and rows % 64 == 0
        and features % 128 == 0
        and units % 128 in (0, 64)
        and units >= 512
        and rows <= 256
        and (shape["tp"] - 2) * span <= features
        and span % HEAD_SIZE == 0
        and features <= units
        and tp_span <= resid.shape[2] * shape["tp"]
        and 2 * span <= features
        and group_span <= features
        and keys.shape[2] * 2 <= features
        and 2 * rows <= features
        and queries.shape[2] // group_span * rows + 2 * rows < w_down.shape[1]
    )


def body(
    shape,
    queries,
    keys,
    values,
    doc_lengths,
    resid,
    ffn_gain,
    w_gate,
    w_up,
    w_down,
    kv_gain,
    key_value_weight,
    k_gain,
):
    if not fits(shape, queries, keys, doc_lengths, resid, w_gate, w_down, key_value_weight):
        return plain_body(
            queries,
            keys,
            values,
            doc_lengths,
            resid,
            ffn_gain,
            w_gate,
            w_up,
            w_down,
            kv_gain,
            key_value_weight,
            k_gain,
        )
    sizes = (shape["seq"], shape["tp"], shape["pp"])
    tp_count = shape["tp"]
    rows, features = resid.shape[1:]
    width, units = w_gate.shape[1:]
    span = key_value_weight.shape[2] // tp_count
    half = rows // 2
    kv_heads = keys.shape[2] // HEAD_SIZE
    bf16, f32 = jnp.bfloat16, jnp.float32
    hbm = pl.BlockSpec(memory_space=pl.ANY)
    vmem = pl.BlockSpec(memory_space=pltpu.VMEM)
    smem = pl.BlockSpec(memory_space=pltpu.SMEM)
    dma = pltpu.SemaphoreType.DMA
    parts = pl.pallas_call(
            functools.partial(relay_kernel, sizes),
            out_shape=(
                jax.ShapeDtypeStruct(queries.shape, bf16),
                jax.ShapeDtypeStruct(resid.shape, bf16),
                jax.ShapeDtypeStruct((1, rows, span), bf16),
            ),
            in_specs=[smem, hbm, hbm, hbm, hbm, vmem, hbm, hbm, hbm, vmem, hbm, vmem],
            out_specs=(hbm, hbm, hbm),
            scratch_shapes=[
                pltpu.VMEM((units, width), bf16),
                pltpu.VMEM((units, width), bf16),
                pltpu.VMEM(w_down.shape[1:], bf16),
                pltpu.VMEM((2, tp_count, rows, features), bf16),
                pltpu.VMEM((tp_count, 2 * rows, units // 128 * 128), bf16),
                pltpu.VMEM((tp_count, rows, 128), bf16),
                pltpu.VMEM((rows, width), bf16),
                pltpu.VMEM((rows, features), f32),
                pltpu.VMEM((half, features), f32),
                pltpu.VMEM((rows, features), bf16),
                pltpu.VMEM((rows, features), bf16),
                pltpu.VMEM((half, features), bf16),
                pltpu.VMEM((tp_count, rows, span), bf16),
                pltpu.VMEM((rows, span), f32),
                pltpu.VMEM((3, tp_count, 8, 128), f32),
                pltpu.VMEM((128, 128), f32),
                pltpu.VMEM((rows, span), bf16),
                dma((kv_heads + 8,)),
                dma((kv_heads + 6,)),
                dma((2, 2, tp_count)),
                dma((2, 2, tp_count)),
                dma((2, tp_count)),
                dma((2, tp_count)),
                dma((2,)),
                dma((2,)),
                dma((2, 5, tp_count, 3)),
                dma((2, 5, tp_count, 3)),
                dma((2,)),
                dma((2,)),
                dma((3,)),
                dma((3,)),
                dma((3, tp_count)),
                dma((3, tp_count)),
                dma((3, tp_count)),
                dma((3, tp_count)),
                dma((2, tp_count)),
                pltpu.VMEM((half, span), f32),
            ],
            compiler_params=pltpu.CompilerParams(
                collective_id=0, has_side_effects=True, vmem_limit_bytes=67043328
            ),
            name="relay_step",
        )(
            doc_lengths,
            queries,
            keys,
            values,
            resid,
            ffn_gain,
            jnp.swapaxes(w_gate, 1, 2),
            jnp.swapaxes(w_up, 1, 2),
            w_down,
            kv_gain,
            key_value_weight,
            k_gain,
        )
    hbm_shapes = [jax.ShapeDtypeStruct(part.shape, part.dtype) for part in parts]
    return tuple(
        pl.pallas_call(
            settle_kernel,
            out_shape=tuple(hbm_shapes),
            in_specs=[hbm] * 3,
            out_specs=(hbm,) * 3,
            scratch_shapes=[pltpu.VMEM(part.shape, part.dtype) for part in parts] + [dma((6,))],
            name="settle",
        )(*parts)
    )


def solution(mesh):
    placed = (
        P("pp", "seq", "tp"),
        P("pp", "seq", "tp"),
        P("pp", "seq", "tp"),
        P("pp", None),
        P("pp", "seq", "tp"),
        P("pp", None),
        P("pp", None, ("seq", "tp")),
        P("pp", None, ("seq", "tp")),
        P("pp", "seq", "tp"),
        P("pp", None),
        P("pp", "tp", None),
        P("pp", None),
    )
    return jax.shard_map(
        functools.partial(body, dict(mesh.shape)),
        mesh=mesh,
        in_specs=placed,
        out_specs=(P("pp", "seq", "tp"), P("pp", "seq", "tp"), P("pp", "seq", "tp")),
        check_vma=False,
    )
```

```python
import functools
import math

import jax
import jax.numpy as jnp
from jax import lax
from jax.experimental import pallas as pl
from jax.experimental.pallas import tpu as pltpu
from jax.sharding import PartitionSpec as P

MODEL_WIDTH = 5120
QUERY_HEADS = 64
KEY_VALUE_HEADS = 8
HEAD_SIZE = 128


epsilon = 1e-06
negative = -1e30


def passed_along(block, axis, distance):
    count = lax.axis_size(axis)
    return lax.ppermute(block, axis, [(i, (i + distance) % count) for i in range(count)])


def passed_where(block, distance, places):
    seq_count = lax.axis_size("seq")
    tp_count = lax.axis_size("tp")
    route = [
        (s * tp_count + t, ((s + distance) % seq_count) * tp_count + t)
        for s in range(seq_count)
        for t in places
    ]
    return lax.ppermute(block, ("seq", "tp"), route)


def line_gather(block):
    count = lax.axis_size("tp")
    slots = {0: block}
    for k in range(1, count):
        slots[-k] = lax.ppermute(
            slots[1 - k], "tp", [(i, i + 1) for i in range(k - 1, count - 1)]
        )
        slots[k] = lax.ppermute(
            slots[k - 1], "tp", [(i, i - 1) for i in range(1, count - k + 1)]
        )
    return slots


def valid_places(offset, count):
    return [t for t in range(count) if 0 <= t + offset < count]


def pick(slots, offsets, tp_rank):
    picked = slots[offsets[0]]
    for t in range(1, len(offsets)):
        if offsets[t] != offsets[t - 1] or len(set(offsets)) > 1:
            picked = jnp.where(tp_rank == t, slots[offsets[t]], picked)
    return picked


def arrival_order(count):
    table = []
    for t in range(count):
        order = [0]
        for k in range(1, count):
            order += [d for d in (-k, k) if 0 <= t + d < count]
        table.append(order)
    return table


def document_ids(places, bounds):
    return jnp.sum((places[:, None] >= bounds[None, :]).astype(jnp.int32), axis=1)


def seq_gather(block):
    count = lax.axis_size("seq")
    rank = lax.axis_index("seq")
    rows = block.shape[0]
    whole = jnp.zeros((count * rows, block.shape[1]), block.dtype)
    for k in range(count):
        part = block if k == 0 else passed_along(block, "seq", k)
        whole = lax.dynamic_update_slice_in_dim(whole, part, lax.rem(rank - k + count, count) * rows, 0)
    return whole


def attend_rows(query_rows, query_places, keys_local, values_local, lengths):
    bounds = jnp.cumsum(lengths)
    query_docs = document_ids(query_places, bounds)
    row_count = query_rows.shape[0]
    kv_heads = keys_local.shape[1] // HEAD_SIZE
    group_width = QUERY_HEADS // KEY_VALUE_HEADS
    query_four = query_rows.reshape(row_count, kv_heads, group_width, HEAD_SIZE)
    inv_root = 1.0 / math.sqrt(HEAD_SIZE)
    key_piece = seq_gather(keys_local)
    value_piece = seq_gather(values_local)
    key_count = key_piece.shape[0]

    key_places = jnp.arange(key_count, dtype=jnp.int32)
    key_docs = document_ids(key_places, bounds)
    visible = (query_docs[:, None] == key_docs[None, :]) & (
        key_places[None, :] <= query_places[:, None]
    )
    scores = (
        jnp.einsum(
            "rkgd,nkd->kgrn",
            query_four,
            key_piece.reshape(key_count, kv_heads, HEAD_SIZE),
            preferred_element_type=jnp.float32,
        )
        * inv_root
    )
    masked = jnp.where(visible, scores, negative)
    row_max = jnp.max(masked, axis=3)
    exponent = jnp.where(visible, jnp.exp(masked - row_max[..., None]), 0.0)
    running_sum = jnp.sum(exponent, axis=3)
    weighted = jnp.einsum(
        "kgrn,nkd->kgrd",
        exponent.astype(jnp.bfloat16),
        value_piece.reshape(key_count, kv_heads, HEAD_SIZE),
        preferred_element_type=jnp.float32,
    )
    mixed = weighted / running_sum[..., None]
    return (
        jnp.transpose(mixed, (2, 0, 1, 3))
        .reshape(row_count, kv_heads * group_width * HEAD_SIZE)
        .astype(jnp.bfloat16)
    )


def plain_body(
    queries,
    keys,
    values,
    doc_lengths,
    resid,
    ffn_gain,
    w_gate,
    w_up,
    w_down,
    kv_gain,
    key_value_weight,
    k_gain,
):
    seq_count = lax.axis_size("seq")
    seq_rank = lax.axis_index("seq")
    tp_count = lax.axis_size("tp")
    tp_rank = lax.axis_index("tp")
    tok_rows = queries.shape[1]
    lengths = doc_lengths[0]
    query_local = queries[0]
    query_places = seq_rank * tok_rows + jnp.arange(tok_rows, dtype=jnp.int32)
    attended = attend_rows(query_local, query_places, keys[0], values[0], lengths)
    resid_local = resid[0]
    wide = resid_local.astype(jnp.float32)
    features = resid_local.shape[1]
    hidden_local = w_gate.shape[2]
    slots = line_gather(resid_local)
    groups = [slots]
    for k in range(1, seq_count):
        groups.append(
            {d: passed_where(slots[d], k, valid_places(d, tp_count)) for d in sorted(slots, key=abs)}
        )
    gain = ffn_gain[0]
    table = arrival_order(tp_count)
    down_weight = w_down[0]
    totals = []
    ready = None
    for group in groups:
        if ready is not None:
            offsets_here = sorted(group)
            tied = lax.optimization_barrier(tuple(group[d] for d in offsets_here) + (ready,))
            group = dict(zip(offsets_here, tied[:-1]))
        pieces = [
            pick(group, [j - t for t in range(tp_count)], tp_rank).astype(jnp.float32)
            for j in range(tp_count)
        ]
        squares = sum(jnp.sum(piece * piece, axis=1) for piece in pieces)
        inverse = lax.rsqrt(squares / MODEL_WIDTH + epsilon)
        normed = jnp.concatenate(
            [
                (
                    pieces[j] * inverse[:, None] * gain[None, j * features : (j + 1) * features]
                ).astype(jnp.bfloat16)
                for j in range(tp_count)
            ],
            axis=1,
        )
        gate_total = jnp.dot(normed, w_gate[0], preferred_element_type=jnp.float32)
        up_total = jnp.dot(normed, w_up[0], preferred_element_type=jnp.float32)
        hidden = (jax.nn.silu(gate_total) * up_total).astype(jnp.bfloat16)
        ready = hidden
        hidden_slots = line_gather(hidden)
        total = None
        for m in range(tp_count):
            offsets = [table[t][m] for t in range(tp_count)]
            block = pick(hidden_slots, offsets, tp_rank)
            place = tp_rank + jnp.asarray(offsets, jnp.int32)[tp_rank]
            rows = lax.dynamic_slice_in_dim(down_weight, place * hidden_local, hidden_local)
            term = jnp.dot(block, rows, preferred_element_type=jnp.float32)
            total = term if total is None else total + term
        totals.append(total)
    update_rows = totals[0]
    for k in range(1, seq_count):
        update_rows = update_rows + passed_along(
            totals[k].astype(jnp.bfloat16), "seq", -k
        ).astype(jnp.float32)
    layer_local = (wide + update_rows).astype(jnp.bfloat16)
    incoming = passed_along(layer_local, "pp", 1)
    incoming_wide = incoming.astype(jnp.float32)
    own_square = jnp.sum(incoming_wide * incoming_wide, axis=1)
    incoming_total = own_square
    for k in range(1, tp_count):
        incoming_total = incoming_total + passed_along(own_square, "tp", k)
    scale_rows = lax.rsqrt(incoming_total / MODEL_WIDTH + epsilon)
    kv_gain_part = lax.dynamic_slice_in_dim(kv_gain[0], tp_rank * features, features)
    kv_input = (incoming_wide * kv_gain_part[None, :]).astype(jnp.bfloat16)
    kv_weight = key_value_weight[0]
    span = kv_weight.shape[1] // tp_count
    mapped_rows = jnp.dot(kv_input, kv_weight, preferred_element_type=jnp.float32)
    kv_span = lax.dynamic_slice_in_dim(mapped_rows, tp_rank * span, span, 1)
    mapped_bits = mapped_rows.astype(jnp.bfloat16)
    for k in range(1, tp_count):
        part = lax.dynamic_slice_in_dim(mapped_bits, lax.rem(tp_rank + k, tp_count) * span, span, 1)
        kv_span = kv_span + passed_along(part, "tp", k).astype(jnp.float32)
    kv_span = kv_span * scale_rows[:, None]
    span_width = kv_span.shape[1]
    heads_here = span_width // HEAD_SIZE
    divide_heads = kv_span.reshape(tok_rows, heads_here, HEAD_SIZE)
    mean_square = jnp.mean(divide_heads * divide_heads, axis=2, keepdims=True)
    norm_applied = divide_heads * lax.rsqrt(mean_square + epsilon) * k_gain[0][None, None, :]
    head_index_list = tp_rank * heads_here + jnp.arange(heads_here, dtype=jnp.int32)
    kv_result = (
        jnp.where((head_index_list < KEY_VALUE_HEADS)[None, :, None], norm_applied, divide_heads)
        .reshape(tok_rows, span_width)
        .astype(jnp.bfloat16)
    )
    return (attended[None], layer_local[None], kv_result[None])


MESH = pl.DeviceIdType.MESH


def relay_kernel(
    sizes,
    lengths_ref,
    queries_ref,
    keys_ref,
    values_ref,
    resid_ref,
    ffn_gain_ref,
    w_gate_ref,
    w_up_ref,
    w_down_ref,
    kv_gain_ref,
    kv_weight_ref,
    k_gain_ref,
    attn_ref,
    layer_ref,
    kv_next_ref,
    gate_w,
    up_w,
    down_w,
    x_buf,
    h_buf,
    h_tail,
    g_buf,
    own_acc,
    other_acc,
    part_in,
    stream_in,
    y_buf,
    kv_in,
    kv_own,
    square_buf,
    square_tmp,
    kv_out,
    local_sem,
    out_sem,
    xz_send,
    xz_recv,
    xs_send,
    xs_recv,
    a_send,
    a_recv,
    h_send,
    h_recv,
    p_send,
    p_recv,
    r_send,
    r_recv,
    kv_send,
    kv_recv,
    sq_send,
    sq_recv,
    relay_recv,
    relay_sum,
):
    seq_count, tp_count, pp_count = sizes
    s = lax.axis_index("seq")
    t = lax.axis_index("tp")
    p = lax.axis_index("pp")
    rows = resid_ref.shape[1]
    features = resid_ref.shape[2]
    units = w_gate_ref.shape[1]
    width = w_gate_ref.shape[2]
    span = kv_next_ref.shape[2]
    half = rows // 2
    tail = 32 if half % 32 == 0 and half > 32 else 16
    kv_heads = keys_ref.shape[2] // HEAD_SIZE
    group = queries_ref.shape[2] // keys_ref.shape[2]
    group_span = group * HEAD_SIZE

    pieces = (
        (0, 0, half),
        (half, 0, half),
        (3 * half, half, half),
        (2 * half, half, half - tail),
        (3 * half - tail, rows - tail, tail),
    )
    main = units // 128 * 128
    rest = units - main
    block_n = 256 if main % 256 == 0 else 128
    full_tiles = main // block_n
    split = full_tiles // 2 * block_n
    early, late = (0,), (1, 2) if rest else (1,)
    whole = early + late
    own_pieces = (0, 3, 4)

    def rows_of(c):
        return pl.ds(c * half, half)

    def remote(src, dst, send, recv, where):
        return pltpu.make_async_remote_copy(
            src_ref=src,
            dst_ref=dst,
            send_sem=send,
            recv_sem=recv,
            device_id=where,
            device_id_type=MESH,
        )

    def next_on_line(d):
        return lax.rem(t + 2 * d - 1 + tp_count, tp_count)

    def has_next(d):
        place = t + 2 * d - 1
        return (place >= 0) & (place < tp_count)

    def x_line(d, c, block, own=False):
        dst = x_buf.at[0, block, rows_of(c)]
        src = resid_ref.at[0, rows_of(c)] if own else dst
        return remote(
            src, dst, xz_send.at[d, c, block], xz_recv.at[d, c, block], {"tp": next_on_line(d)}
        )

    def x_across(c, block, own=False):
        src = resid_ref.at[0, rows_of(c)] if own else x_buf.at[0, block, rows_of(c)]
        return remote(
            src,
            x_buf.at[1, block, rows_of(c)],
            xs_send.at[c, block],
            xs_recv.at[c, block],
            {"seq": 1 - s},
        )

    def subs_of(piece):
        return whole if piece < 3 else (3,) + ((2,) if rest else ())

    def h_line(d, piece, block, sub):
        first, _, count = pieces[piece]
        if sub == 2:
            ref = h_tail.at[block, pl.ds(first // 2, count // 2)]
        else:
            lanes = (pl.ds(0, split), pl.ds(split, main - split), None, pl.ds(0, main))[sub]
            ref = h_buf.at[block, pl.ds(first, count), lanes]
        come = lax.rem((block - t) * (1 - 2 * d) + tp_count, tp_count)
        arrived = lax.rem(come + tp_count - 2, tp_count - 1)
        slot = sub if piece < 3 else (0, 1)[sub == 2]
        recv = 3 * piece + slot if piece < 3 else 9 + 2 * (piece - 3) + slot
        sent = recv if piece < 3 else (recv - 9 if recv < 12 else 9)
        return (
            lambda: remote(
                ref,
                ref,
                h_send.at[d, sent, come],
                h_recv.at[d, recv, come],
                {"tp": next_on_line(d)},
            ),
            lambda: remote(
                ref,
                ref,
                h_send.at[d, sent, arrived],
                h_recv.at[d, recv, arrived],
                {"tp": next_on_line(d)},
            ),
        )

    def h_out(d, piece, block, sub):
        return h_line(d, piece, block, sub)[0]()

    def h_in(d, piece, block, sub):
        return h_line(d, piece, block, sub)[1]()

    key_row = kv_heads * rows
    kv_width = kv_heads * HEAD_SIZE

    def query_place(i):
        return down_w.at[pl.ds(i * rows, rows), pl.ds(0, group_span)]

    def key_place(side, which):
        return down_w.at[
            pl.ds(key_row + side * rows, rows), pl.ds(which * kv_width, kv_width)
        ]

    attn_rows = key_row + seq_count * rows

    def a_across(which):
        src = keys_ref if which == 0 else values_ref
        return remote(
            src.at[0],
            key_place(s, which),
            a_send.at[which],
            a_recv.at[which],
            {"seq": 1 - s},
        )

    def a_arrived(which):
        src = keys_ref if which == 0 else values_ref
        return remote(
            src.at[0],
            key_place(1 - s, which),
            a_send.at[which],
            a_recv.at[which],
            {"seq": 1 - s},
        )

    loads = {}

    def load(name, src, dst):
        loads[name] = pltpu.make_async_copy(src, dst, local_sem.at[len(loads)])
        loads[name].start()

    for i in range(kv_heads):
        load(
            ("q", i),
            queries_ref.at[0, :, pl.ds(i * group_span, group_span)],
            query_place(i),
        )
    load("k", keys_ref.at[0], key_place(s, 0))
    load("v", values_ref.at[0], key_place(s, 1))
    load("x", resid_ref.at[0], x_buf.at[0, t])
    load("gate", w_gate_ref.at[0], gate_w)
    load("up", w_up_ref.at[0], up_w)
    down_rows = w_down_ref.shape[1]
    load(
        "down1",
        w_down_ref.at[0, pl.ds(attn_rows, down_rows - attn_rows)],
        down_w.at[pl.ds(attn_rows, down_rows - attn_rows)],
    )

    barrier = pltpu.get_barrier_semaphore()
    for k in range(1, tp_count):
        pl.semaphore_signal(
            barrier, inc=1, device_id={"tp": lax.rem(t + k, tp_count)}, device_id_type=MESH
        )
    pl.semaphore_signal(barrier, inc=1, device_id={"seq": 1 - s}, device_id_type=MESH)
    for k in (1, pp_count - 1):
        pl.semaphore_signal(
            barrier, inc=1, device_id={"pp": lax.rem(p + k, pp_count)}, device_id_type=MESH
        )
    pl.semaphore_wait(barrier, tp_count - 1 + 1 + 2)

    def send_own_x(d, c, when):
        @pl.when(has_next(d) & when)
        def _():
            x_line(d, c, t, True).start()

    late_low = (t >= 2) & (t <= tp_count - 2)
    late_high = (t >= 1) & (t <= tp_count - 3)
    always = t >= 0
    a_across(0).start()
    a_across(1).start()
    for d in (0, 1):
        send_own_x(d, 0, always)
    x_across(0, t, True).start()
    send_own_x(0, 1, jnp.logical_not(late_low))
    send_own_x(1, 1, jnp.logical_not(late_high))

    def x_events(c, k):
        for d in (0, 1):
            block = t + k * (1 - 2 * d)
            block_safe = lax.rem(block + tp_count, tp_count)

            @pl.when((block >= 0) & (block < tp_count))
            def _():
                x_line(d, c, block_safe).wait_recv()

                @pl.when(has_next(d))
                def _():
                    x_line(d, c, block_safe).start()

                x_across(c, block_safe).start()

    bias = own_acc.at[:, pl.ds(0, seq_count * rows)]
    row_id = lax.broadcasted_iota(jnp.int32, (rows, seq_count * rows), 0) + s * rows
    col_id = lax.broadcasted_iota(jnp.int32, (rows, seq_count * rows), 1)
    bound = lengths_ref[0, 0]
    begin = jnp.zeros_like(row_id)
    for k in range(1, lengths_ref.shape[1]):
        begin = jnp.where(row_id >= bound, bound, begin)
        bound = bound + lengths_ref[0, k]
    own_acc[:, : seq_count * rows] = jnp.where(
        (col_id <= row_id) & (col_id >= begin), 0.0, negative
    )
    inv_root = 1.0 / math.sqrt(HEAD_SIZE)

    def attend(first, last):
        def one(index, carry):
            i = index // group
            j = lax.rem(index, group)
            place = pl.ds(pl.multiple_of(i * rows, 16), rows)
            lanes = pl.ds(pl.multiple_of(j * HEAD_SIZE, HEAD_SIZE), HEAD_SIZE)
            query = down_w[place, lanes]
            key = down_w[
                key_row : key_row + seq_count * rows,
                pl.ds(pl.multiple_of(i * HEAD_SIZE, HEAD_SIZE), HEAD_SIZE),
            ]
            value = down_w[
                key_row : key_row + seq_count * rows,
                pl.ds(pl.multiple_of(kv_width + i * HEAD_SIZE, HEAD_SIZE), HEAD_SIZE),
            ]
            scores = lax.dot_general(
                query, key, (((1,), (1,)), ((), ())), preferred_element_type=jnp.float32
            )
            masked = scores * inv_root + bias[...]
            peak = jnp.max(masked, axis=1, keepdims=True)
            expo = jnp.exp(masked - peak)
            total = jnp.sum(expo, axis=1, keepdims=True)
            mixed = jnp.dot(
                expo.astype(jnp.bfloat16), value, preferred_element_type=jnp.float32
            )
            down_w[place, lanes] = (mixed / total).astype(jnp.bfloat16)
            return carry

        lax.fori_loop(first, last, one, 0)

    heads = kv_heads * group
    middle_head = heads // 2
    x_events(0, 1)
    send_own_x(0, 1, late_low)
    send_own_x(1, 1, late_high)
    for i in range(kv_heads):
        loads[("q", i)].wait()
    loads["k"].wait()
    loads["v"].wait()
    a_arrived(0).wait_recv()
    a_arrived(1).wait_recv()
    attend(0, middle_head)
    for k in range(2, tp_count - 1):
        x_events(0, k)
    x_across(1, t, True).start()
    attend(middle_head, heads)
    attn_copies = [
        pltpu.make_async_copy(
            query_place(i),
            attn_ref.at[0, :, pl.ds(i * group_span, group_span)],
            out_sem.at[i],
        )
        for i in range(kv_heads)
    ]
    for copy in attn_copies:
        copy.start()
    x_events(0, tp_count - 1)
    loads["x"].wait()
    for copy in attn_copies:
        copy.wait()
    load("down0", w_down_ref.at[0, pl.ds(0, attn_rows)], down_w.at[pl.ds(0, attn_rows)])

    lane_tiles = features // 128

    def normalise(side, c, first):
        def squares(block, acc):
            for j in range(lane_tiles):
                x = x_buf[side, block, rows_of(c), j * 128 : (j + 1) * 128].astype(jnp.float32)
                acc = acc + x * x
            return acc

        total = lax.fori_loop(0, tp_count, squares, jnp.zeros((half, 128), jnp.float32))
        inverse = lax.rsqrt(jnp.sum(total, axis=1, keepdims=True) / width + epsilon)

        def write(block, carry):
            for j in range(lane_tiles):
                x = x_buf[side, block, rows_of(c), j * 128 : (j + 1) * 128].astype(jnp.float32)
                lanes = pl.ds(pl.multiple_of(block * features + j * 128, 128), 128)
                g_buf[first : first + half, lanes] = (
                    x * inverse * ffn_gain_ref[0:1, lanes]
                ).astype(jnp.bfloat16)
            return carry

        lax.fori_loop(0, tp_count, write, 0)

    def gated(count, place):
        both = (((1,), (1,)), ((), ()))
        x = g_buf[0:count, :]
        g = lax.dot_general(x, gate_w[place, :], both, preferred_element_type=jnp.float32)
        u = lax.dot_general(x, up_w[place, :], both, preferred_element_type=jnp.float32)
        return g / (1.0 + jnp.exp(-g)) * u

    def hidden_group(group_pieces, hooks):
        first = pieces[group_pieces[0]][0]
        count = sum(pieces[piece][2] for piece in group_pieces)

        def one(i, carry):
            place = pl.ds(pl.multiple_of(i * block_n, block_n), block_n)
            h_buf[t, pl.ds(first, count), place] = gated(count, place).astype(jnp.bfloat16)
            for index, hook in hooks.items():
                pl.when(i == index)(hook)
            return carry

        lax.fori_loop(0, full_tiles, one, 0)
        if rest:
            hidden = gated(count, pl.ds(main, rest))
            for piece in group_pieces:
                start, _, size = pieces[piece]
                low = hidden[start - first : start - first + size // 2]
                high = hidden[start - first + size // 2 : start - first + size]
                h_tail[t, pl.ds(start // 2, size // 2), :] = jnp.concatenate(
                    [low, high], axis=1
                ).astype(jnp.bfloat16)

    def send_hidden(piece, subs):
        for d in (0, 1):

            @pl.when(has_next(d))
            def _():
                for sub in subs:
                    h_out(d, piece, t, sub).start()

    def forward(piece, subs, k):
        if k > tp_count - 2:
            return
        for d in (0, 1):
            block = t + k * (1 - 2 * d)
            block_safe = lax.rem(block + tp_count, tp_count)

            @pl.when((block >= 0) & (block < tp_count) & has_next(d))
            def _():
                for sub in subs:
                    h_in(d, piece, block_safe, sub).wait_recv()
                    h_out(d, piece, block_safe, sub).start()

    def forwards(piece, subs, low):
        for k in range(low, tp_count - 1):
            forward(piece, subs, k)

    down_n = 256 if features % 256 == 0 else 128

    def down(group_pieces, block, fresh):
        first, own_first, _ = pieces[group_pieces[0]]
        count = sum(pieces[piece][2] for piece in group_pieces)
        own = group_pieces[0] in own_pieces
        acc = own_acc.at[pl.ds(own_first, count)] if own else other_acc
        if rest:
            extra = []
            for piece in group_pieces:
                start, _, size = pieces[piece]
                packed = h_tail[block, pl.ds(start // 2, size // 2), :]
                extra += [packed[:, :rest], packed[:, rest:]]
            extra = jnp.concatenate(extra, axis=0)

        def one(i, carry):
            lanes = pl.ds(pl.multiple_of(i * down_n, down_n), down_n)
            term = jnp.dot(
                h_buf[block, pl.ds(first, count), :],
                down_w[pl.ds(pl.multiple_of(block * units, 16), main), lanes],
                preferred_element_type=jnp.float32,
            )
            if rest:
                term = term + jnp.dot(
                    extra,
                    down_w[pl.ds(pl.multiple_of(block * units + main, 16), rest), lanes],
                    preferred_element_type=jnp.float32,
                )
            if fresh:
                acc[:, lanes] = term
            else:
                acc[:, lanes] += term
            return carry

        lax.fori_loop(0, features // down_n, one, 0)

    def down_others(group_pieces, low, high):
        def one(index, carry):
            k = index // 2 + 1
            d = lax.rem(index, 2)
            block = t + k * (1 - 2 * d)
            block_safe = lax.rem(block + tp_count, tp_count)

            @pl.when((block >= 0) & (block < tp_count))
            def _():
                @pl.when(jnp.logical_not(has_next(d)))
                def _():
                    for piece in group_pieces:
                        for sub in subs_of(piece):
                            h_in(d, piece, block_safe, sub).wait_recv()

                down(group_pieces, block_safe, False)

            return carry

        lax.fori_loop(2 * (low - 1), 2 * (high - 1), one, 0)

    def wait_other_x(c):
        def one(block, carry):
            x_across(c, block).wait_recv()
            return carry

        lax.fori_loop(0, tp_count, one, 0)

    def part_copy(c):
        return remote(
            x_buf.at[1, 0, rows_of(c)],
            part_in.at[rows_of(c)],
            p_send.at[c],
            p_recv.at[c],
            {"seq": 1 - s},
        )

    def send_part(c):
        x_buf[1, 0, rows_of(c)] = other_acc[...].astype(jnp.bfloat16)
        part_copy(c).start()

    def stream_copy(q):
        _, first, count = pieces[own_pieces[q]]
        return remote(
            x_buf.at[1, 1, pl.ds(first, count)],
            stream_in.at[pl.ds(first, count)],
            r_send.at[q],
            r_recv.at[q],
            {"pp": lax.rem(p + 1, pp_count)},
        )

    def layer_copy(q):
        _, first, count = pieces[own_pieces[q]]
        return pltpu.make_async_copy(
            x_buf.at[1, 1, pl.ds(first, count)],
            layer_ref.at[0, pl.ds(first, count)],
            out_sem.at[kv_heads + q],
        )

    def finish_layer(q):
        _, first, count = pieces[own_pieces[q]]
        place = pl.ds(first, count)
        x_buf[1, 1, place] = (
            x_buf[0, t, place].astype(jnp.float32)
            + (own_acc[place, :] + part_in[place, :].astype(jnp.float32))
        ).astype(jnp.bfloat16)
        stream_copy(q).start()
        layer_copy(q).start()

    def own_place(q):
        _, first, count = pieces[own_pieces[q]]
        return pl.ds(first, count)

    def kv_copy(q, k, source, target):
        return remote(
            g_buf.at[own_place(q), pl.ds(k * span, span)],
            kv_in.at[source, own_place(q)],
            kv_send.at[q, k],
            kv_recv.at[q, source],
            {"tp": target},
        )

    def relay_copy(q, k, slot, target):
        return remote(
            g_buf.at[own_place(q), pl.ds(k * span, span)],
            x_buf.at[1, 2, own_place(q), pl.ds(slot * span, span)],
            kv_send.at[q, k],
            relay_recv.at[slot],
            {"tp": target},
        )

    def square_copy(q, k, source, target):
        ref = square_buf.at[q, source]
        return remote(ref, ref, sq_send.at[q, k], sq_recv.at[q, source], {"tp": target})

    def relays(q):
        return q < 1

    def start_kv(q):
        _, first, count = pieces[own_pieces[q]]
        place = pl.ds(first, count)
        stream_copy(q).wait_recv()
        total = jnp.zeros((count, 128), jnp.float32)
        for j in range(lane_tiles):
            lanes = slice(j * 128, (j + 1) * 128)
            x = stream_in[place, lanes].astype(jnp.float32)
            total = total + x * x
            gain = kv_gain_ref[0:1, pl.ds(pl.multiple_of(t * features + j * 128, 128), 128)]
            y_buf[0:count, lanes] = (x * gain).astype(jnp.bfloat16)
        if count < 128:
            square_tmp[...] = jnp.zeros_like(square_tmp)
        square_tmp[0:count, :] = jnp.broadcast_to(
            jnp.sum(total, axis=1, keepdims=True), (count, 128)
        )
        square_buf[q, t] = jnp.transpose(square_tmp[...])[0:8]
        for k in range(1, tp_count):
            square_copy(q, k, t, lax.rem(t + k, tp_count)).start()
        for k in list(range(1, tp_count)) + [0]:
            target = lax.rem(t + k, tp_count)
            term = jnp.dot(
                y_buf[0:count, :],
                gate_w[0:features, pl.ds(pl.multiple_of(target * span, HEAD_SIZE), span)],
                preferred_element_type=jnp.float32,
            )
            if k == 0:
                kv_own[place, :] = term
            elif not relays(q):
                g_buf[place, k * span : (k + 1) * span] = term.astype(jnp.bfloat16)
                kv_copy(q, k, t, target).start()
            else:
                low = (target == 0) & (t >= 1)
                high = (target == tp_count - 1) & (t <= tp_count - 2)
                at_relay = (low & (t == 1)) | (high & (t == tp_count - 2))

                @pl.when(at_relay)
                def _():
                    relay_sum[0:count, :] = term

                @pl.when(jnp.logical_not(at_relay))
                def _():
                    g_buf[place, k * span : (k + 1) * span] = term.astype(jnp.bfloat16)

                @pl.when(low & (t >= 2))
                def _():
                    relay_copy(q, k, lax.rem(t - 2 + tp_count, tp_count), 1).start()

                @pl.when(high & (t <= tp_count - 3))
                def _():
                    slot = lax.rem(2 * tp_count - 3 - t, tp_count)
                    relay_copy(q, k, slot, tp_count - 2).start()

                @pl.when(jnp.logical_not(low) & jnp.logical_not(high))
                def _():
                    kv_copy(q, k, t, target).start()

    def relay_kv(q):
        _, first, count = pieces[own_pieces[q]]
        place = pl.ds(first, count)
        for end, relay in ((0, 1), (tp_count - 1, tp_count - 2)):
            k = (end - relay + tp_count) % tp_count

            @pl.when(t == relay)
            def _():
                total = relay_sum[0:count, :]
                for slot in range(tp_count - 2):
                    relay_copy(q, k, slot, relay).wait_recv()
                    total = total + x_buf[
                        1, 2, place, slot * span : (slot + 1) * span
                    ].astype(jnp.float32)
                g_buf[place, k * span : (k + 1) * span] = total.astype(jnp.bfloat16)
                kv_copy(q, k, t, end).start()

    def kv_out_copy(q):
        _, first, count = pieces[own_pieces[q]]
        return pltpu.make_async_copy(
            kv_out.at[pl.ds(first, count)],
            kv_next_ref.at[0, pl.ds(first, count)],
            out_sem.at[kv_heads + 3 + q],
        )

    def finish_kv(q):
        _, first, count = pieces[own_pieces[q]]
        place = pl.ds(first, count)
        square = square_buf[q, t]
        for k in range(1, tp_count):
            source = lax.rem(t + tp_count - k, tp_count)
            square_copy(q, k, source, t).wait_recv()
            square = square + square_buf[q, source]
        column = jnp.transpose(jnp.broadcast_to(square[0:1], (128, 128)))[0:count, 0:1]
        scale = lax.rsqrt(column / width + epsilon)
        for k in range(1, tp_count):
            source = lax.rem(t + tp_count - k, tp_count)
            through = ((t == 0) & (source > 1)) | (
                (t == tp_count - 1) & (source < tp_count - 2)
            )
            if relays(q):

                @pl.when(jnp.logical_not(through))
                def _():
                    kv_copy(q, k, source, t).wait_recv()
                    kv_own[place, :] += kv_in[source, place, :].astype(jnp.float32)

            else:
                kv_copy(q, k, source, t).wait_recv()
                kv_own[place, :] += kv_in[source, place, :].astype(jnp.float32)
        total = kv_own[place, :]
        total = total * scale
        heads_here = span // HEAD_SIZE
        for h in range(heads_here):
            lanes = slice(h * HEAD_SIZE, (h + 1) * HEAD_SIZE)
            x = total[:, lanes]
            mean_square = jnp.mean(x * x, axis=1, keepdims=True)
            after = x * lax.rsqrt(mean_square + epsilon) * k_gain_ref[0:1, :]
            head = jnp.zeros_like(x, jnp.int32) + (t * heads_here + h)
            kv_out[place, lanes] = jnp.where(head < KEY_VALUE_HEADS, after, x).astype(jnp.bfloat16)
        kv_out_copy(q).start()

    def x_left():
        def one(index, carry):
            c = index // tp_count
            block = lax.rem(index, tp_count)
            for d in (0, 1):
                came = (block - t) * (1 - 2 * d) >= 0

                @pl.when(has_next(d) & came)
                def _():
                    x_line(d, c, block).wait_send()

            x_across(c, block).wait_send()
            return carry

        lax.fori_loop(0, 2 * tp_count, one, 0)

    def hidden_left(piece):
        def one(block, carry):
            for d in (0, 1):
                came = (block - t) * (1 - 2 * d) >= 0

                @pl.when(has_next(d) & came)
                def _():
                    for sub in subs_of(piece):
                        h_out(d, piece, block, sub).wait_send()

            return carry

        lax.fori_loop(0, tp_count, one, 0)

    def kv_left(q):
        stream_copy(q).wait_send()
        layer_copy(q).wait()
        for k in range(1, tp_count):
            kv_copy(q, k, t, lax.rem(t + k, tp_count)).wait_send()
            square_copy(q, k, t, lax.rem(t + k, tp_count)).wait_send()

    last = tp_count
    loads["gate"].wait()
    loads["up"].wait()
    normalise(0, 0, 0)
    x_events(1, 1)
    middle = full_tiles // 2 - 1

    def first_half_of_0():
        send_hidden(0, early)
        for k in range(2, tp_count - 1):
            x_events(1, k)

    hidden_group((0,), {middle: first_half_of_0})
    send_hidden(0, late)
    x_events(1, tp_count - 1)
    wait_other_x(0)
    forward(0, early, 1)
    normalise(1, 0, 0)
    normalise(0, 1, half)

    def first_half_of_1():
        forward(0, late, 1)
        send_hidden(1, early)

    hidden_group(
        (1, 3, 4),
        {
            middle: first_half_of_1,
            middle + 1: functools.partial(forwards, 0, early, 2),
            full_tiles - 1: functools.partial(forwards, 0, late, 2),
        },
    )
    send_hidden(1, late)
    wait_other_x(1)
    forward(1, early, 1)
    normalise(1, 1, 0)
    hidden_group(
        (2,),
        {
            middle: functools.partial(send_hidden, 2, early),
            middle + 1: functools.partial(forward, 1, late, 1),
            middle + 2: functools.partial(forwards, 1, early, 2),
        },
    )
    send_hidden(2, late)
    load(
        "kv",
        kv_weight_ref.at[0],
        gate_w.at[pl.ds(0, features), pl.ds(0, tp_count * span)],
    )
    forward(2, early, 1)
    loads["down0"].wait()
    loads["down1"].wait()
    down((0,), t, True)
    forwards(1, late, 2)
    down_others((0,), 1, last)
    forward(2, late, 1)
    hidden_left(0)
    send_hidden(3, subs_of(3))
    send_hidden(4, subs_of(4))
    down((1,), t, True)
    forwards(2, early, 2)
    down_others((1,), 1, last)
    send_part(0)
    forwards(2, late, 2)
    down((2,), t, True)
    down_others((2,), 1, 2)
    forward(3, subs_of(3), 1)
    x_left()
    down_others((2,), 2, last - 1)
    part_copy(0).wait_recv()
    finish_layer(0)
    forwards(3, subs_of(3), 2)
    forward(4, subs_of(4), 1)
    hidden_left(1)
    loads["kv"].wait()
    start_kv(0)
    down_others((2,), last - 1, last)
    send_part(1)
    forwards(4, subs_of(4), 2)
    down((3, 4), t, True)
    down_others((3, 4), 1, 2)
    down_others((3,), 2, last)
    part_copy(1).wait_recv()
    finish_layer(1)
    relay_kv(0)
    down_others((4,), 2, last)
    finish_layer(2)
    start_kv(1)
    finish_kv(0)
    for which in (0, 1):
        a_across(which).wait_send()
        part_copy(which).wait_send()
    start_kv(2)
    hidden_left(2)
    hidden_left(3)
    hidden_left(4)
    kv_left(0)
    finish_kv(1)
    kv_left(1)
    finish_kv(2)
    kv_left(2)
    for q in range(3):
        kv_out_copy(q).wait()


def settle_kernel(a_ref, b_ref, c_ref, a_out, b_out, c_out, a_buf, b_buf, c_buf, sem):
    pairs = ((a_ref, a_buf, a_out), (b_ref, b_buf, b_out), (c_ref, c_buf, c_out))
    into = [pltpu.make_async_copy(src, buf, sem.at[i]) for i, (src, buf, _) in enumerate(pairs)]
    out = [pltpu.make_async_copy(buf, dst, sem.at[3 + i]) for i, (_, buf, dst) in enumerate(pairs)]
    for copy in into:
        copy.start()
    for i in range(3):
        into[i].wait()
        out[i].start()
    for copy in out:
        copy.wait()


def fits(shape, queries, keys, doc_lengths, resid, w_gate, w_down, key_value_weight):
    rows, features = resid.shape[1:]
    units = w_gate.shape[2]
    span = key_value_weight.shape[2] // shape["tp"]
    tp_span = key_value_weight.shape[2]
    group_span = HEAD_SIZE * queries.shape[2] // keys.shape[2]
    return (
        shape["seq"] == 2
        and shape["pp"] >= 3
        and shape["tp"] >= 3
        and rows % 64 == 0
        and features % 128 == 0
        and units % 128 in (0, 64)
        and units >= 512
        and rows <= 256
        and (shape["tp"] - 2) * span <= features
        and span % HEAD_SIZE == 0
        and features <= units
        and tp_span <= resid.shape[2] * shape["tp"]
        and 2 * span <= features
        and group_span <= features
        and keys.shape[2] * 2 <= features
        and 2 * rows <= features
        and queries.shape[2] // group_span * rows + 2 * rows < w_down.shape[1]
    )


def body(
    shape,
    queries,
    keys,
    values,
    doc_lengths,
    resid,
    ffn_gain,
    w_gate,
    w_up,
    w_down,
    kv_gain,
    key_value_weight,
    k_gain,
):
    if not fits(shape, queries, keys, doc_lengths, resid, w_gate, w_down, key_value_weight):
        return plain_body(
            queries,
            keys,
            values,
            doc_lengths,
            resid,
            ffn_gain,
            w_gate,
            w_up,
            w_down,
            kv_gain,
            key_value_weight,
            k_gain,
        )
    sizes = (shape["seq"], shape["tp"], shape["pp"])
    tp_count = shape["tp"]
    rows, features = resid.shape[1:]
    width, units = w_gate.shape[1:]
    span = key_value_weight.shape[2] // tp_count
    half = rows // 2
    kv_heads = keys.shape[2] // HEAD_SIZE
    bf16, f32 = jnp.bfloat16, jnp.float32
    hbm = pl.BlockSpec(memory_space=pl.ANY)
    vmem = pl.BlockSpec(memory_space=pltpu.VMEM)
    smem = pl.BlockSpec(memory_space=pltpu.SMEM)
    dma = pltpu.SemaphoreType.DMA
    parts = pl.pallas_call(
            functools.partial(relay_kernel, sizes),
            out_shape=(
                jax.ShapeDtypeStruct(queries.shape, bf16),
                jax.ShapeDtypeStruct(resid.shape, bf16),
                jax.ShapeDtypeStruct((1, rows, span), bf16),
            ),
            in_specs=[smem, hbm, hbm, hbm, hbm, vmem, hbm, hbm, hbm, vmem, hbm, vmem],
            out_specs=(hbm, hbm, hbm),
            scratch_shapes=[
                pltpu.VMEM((units, width), bf16),
                pltpu.VMEM((units, width), bf16),
                pltpu.VMEM(w_down.shape[1:], bf16),
                pltpu.VMEM((2, tp_count, rows, features), bf16),
                pltpu.VMEM((tp_count, 2 * rows, units // 128 * 128), bf16),
                pltpu.VMEM((tp_count, rows, 128), bf16),
                pltpu.VMEM((rows, width), bf16),
                pltpu.VMEM((rows, features), f32),
                pltpu.VMEM((half, features), f32),
                pltpu.VMEM((rows, features), bf16),
                pltpu.VMEM((rows, features), bf16),
                pltpu.VMEM((half, features), bf16),
                pltpu.VMEM((tp_count, rows, span), bf16),
                pltpu.VMEM((rows, span), f32),
                pltpu.VMEM((3, tp_count, 8, 128), f32),
                pltpu.VMEM((128, 128), f32),
                pltpu.VMEM((rows, span), bf16),
                dma((kv_heads + 8,)),
                dma((kv_heads + 6,)),
                dma((2, 2, tp_count)),
                dma((2, 2, tp_count)),
                dma((2, tp_count)),
                dma((2, tp_count)),
                dma((2,)),
                dma((2,)),
                dma((2, 10, tp_count - 1)),
                dma((2, 13, tp_count - 1)),
                dma((2,)),
                dma((2,)),
                dma((3,)),
                dma((3,)),
                dma((3, tp_count)),
                dma((3, tp_count)),
                dma((3, tp_count)),
                dma((3, tp_count)),
                dma((tp_count - 2,)),
                pltpu.VMEM((half, span), f32),
            ],
            compiler_params=pltpu.CompilerParams(
                collective_id=0, has_side_effects=True, vmem_limit_bytes=67043328
            ),
            name="relay_step",
        )(
            doc_lengths,
            queries,
            keys,
            values,
            resid,
            ffn_gain,
            jnp.swapaxes(w_gate, 1, 2),
            jnp.swapaxes(w_up, 1, 2),
            w_down,
            kv_gain,
            key_value_weight,
            k_gain,
        )
    hbm_shapes = [jax.ShapeDtypeStruct(part.shape, part.dtype) for part in parts]
    return tuple(
        pl.pallas_call(
            settle_kernel,
            out_shape=tuple(hbm_shapes),
            in_specs=[hbm] * 3,
            out_specs=(hbm,) * 3,
            scratch_shapes=[pltpu.VMEM(part.shape, part.dtype) for part in parts] + [dma((6,))],
            name="settle",
        )(*parts)
    )


def solution(mesh):
    placed = (
        P("pp", "seq", "tp"),
        P("pp", "seq", "tp"),
        P("pp", "seq", "tp"),
        P("pp", None),
        P("pp", "seq", "tp"),
        P("pp", None),
        P("pp", None, ("seq", "tp")),
        P("pp", None, ("seq", "tp")),
        P("pp", "seq", "tp"),
        P("pp", None),
        P("pp", "tp", None),
        P("pp", None),
    )
    return jax.shard_map(
        functools.partial(body, dict(mesh.shape)),
        mesh=mesh,
        in_specs=placed,
        out_specs=(P("pp", "seq", "tp"), P("pp", "seq", "tp"), P("pp", "seq", "tp")),
        check_vma=False,
    )
```

```python
import functools
import math

import jax
import jax.numpy as jnp
from jax import lax
from jax.experimental import pallas as pl
from jax.experimental.pallas import tpu as pltpu
from jax.sharding import PartitionSpec as P

MODEL_WIDTH = 5120
QUERY_HEADS = 64
KEY_VALUE_HEADS = 8
HEAD_SIZE = 128


epsilon = 1e-06
negative = -1e30


def passed_along(block, axis, distance):
    count = lax.axis_size(axis)
    return lax.ppermute(block, axis, [(i, (i + distance) % count) for i in range(count)])


def passed_where(block, distance, places):
    seq_count = lax.axis_size("seq")
    tp_count = lax.axis_size("tp")
    route = [
        (s * tp_count + t, ((s + distance) % seq_count) * tp_count + t)
        for s in range(seq_count)
        for t in places
    ]
    return lax.ppermute(block, ("seq", "tp"), route)


def line_gather(block):
    count = lax.axis_size("tp")
    slots = {0: block}
    for k in range(1, count):
        slots[-k] = lax.ppermute(
            slots[1 - k], "tp", [(i, i + 1) for i in range(k - 1, count - 1)]
        )
        slots[k] = lax.ppermute(
            slots[k - 1], "tp", [(i, i - 1) for i in range(1, count - k + 1)]
        )
    return slots


def valid_places(offset, count):
    return [t for t in range(count) if 0 <= t + offset < count]


def pick(slots, offsets, tp_rank):
    picked = slots[offsets[0]]
    for t in range(1, len(offsets)):
        if offsets[t] != offsets[t - 1] or len(set(offsets)) > 1:
            picked = jnp.where(tp_rank == t, slots[offsets[t]], picked)
    return picked


def arrival_order(count):
    table = []
    for t in range(count):
        order = [0]
        for k in range(1, count):
            order += [d for d in (-k, k) if 0 <= t + d < count]
        table.append(order)
    return table


def document_ids(places, bounds):
    return jnp.sum((places[:, None] >= bounds[None, :]).astype(jnp.int32), axis=1)


def seq_gather(block):
    count = lax.axis_size("seq")
    rank = lax.axis_index("seq")
    rows = block.shape[0]
    whole = jnp.zeros((count * rows, block.shape[1]), block.dtype)
    for k in range(count):
        part = block if k == 0 else passed_along(block, "seq", k)
        whole = lax.dynamic_update_slice_in_dim(whole, part, lax.rem(rank - k + count, count) * rows, 0)
    return whole


def attend_rows(query_rows, query_places, keys_local, values_local, lengths):
    bounds = jnp.cumsum(lengths)
    query_docs = document_ids(query_places, bounds)
    row_count = query_rows.shape[0]
    kv_heads = keys_local.shape[1] // HEAD_SIZE
    group_width = QUERY_HEADS // KEY_VALUE_HEADS
    query_four = query_rows.reshape(row_count, kv_heads, group_width, HEAD_SIZE)
    inv_root = 1.0 / math.sqrt(HEAD_SIZE)
    key_piece = seq_gather(keys_local)
    value_piece = seq_gather(values_local)
    key_count = key_piece.shape[0]

    key_places = jnp.arange(key_count, dtype=jnp.int32)
    key_docs = document_ids(key_places, bounds)
    visible = (query_docs[:, None] == key_docs[None, :]) & (
        key_places[None, :] <= query_places[:, None]
    )
    scores = (
        jnp.einsum(
            "rkgd,nkd->kgrn",
            query_four,
            key_piece.reshape(key_count, kv_heads, HEAD_SIZE),
            preferred_element_type=jnp.float32,
        )
        * inv_root
    )
    masked = jnp.where(visible, scores, negative)
    row_max = jnp.max(masked, axis=3)
    exponent = jnp.where(visible, jnp.exp(masked - row_max[..., None]), 0.0)
    running_sum = jnp.sum(exponent, axis=3)
    weighted = jnp.einsum(
        "kgrn,nkd->kgrd",
        exponent.astype(jnp.bfloat16),
        value_piece.reshape(key_count, kv_heads, HEAD_SIZE),
        preferred_element_type=jnp.float32,
    )
    mixed = weighted / running_sum[..., None]
    return (
        jnp.transpose(mixed, (2, 0, 1, 3))
        .reshape(row_count, kv_heads * group_width * HEAD_SIZE)
        .astype(jnp.bfloat16)
    )


def plain_body(
    queries,
    keys,
    values,
    doc_lengths,
    resid,
    ffn_gain,
    w_gate,
    w_up,
    w_down,
    kv_gain,
    key_value_weight,
    k_gain,
):
    seq_count = lax.axis_size("seq")
    seq_rank = lax.axis_index("seq")
    tp_count = lax.axis_size("tp")
    tp_rank = lax.axis_index("tp")
    tok_rows = queries.shape[1]
    lengths = doc_lengths[0]
    query_local = queries[0]
    query_places = seq_rank * tok_rows + jnp.arange(tok_rows, dtype=jnp.int32)
    attended = attend_rows(query_local, query_places, keys[0], values[0], lengths)
    resid_local = resid[0]
    wide = resid_local.astype(jnp.float32)
    features = resid_local.shape[1]
    hidden_local = w_gate.shape[2]
    slots = line_gather(resid_local)
    groups = [slots]
    for k in range(1, seq_count):
        groups.append(
            {d: passed_where(slots[d], k, valid_places(d, tp_count)) for d in sorted(slots, key=abs)}
        )
    gain = ffn_gain[0]
    table = arrival_order(tp_count)
    down_weight = w_down[0]
    totals = []
    ready = None
    for group in groups:
        if ready is not None:
            offsets_here = sorted(group)
            tied = lax.optimization_barrier(tuple(group[d] for d in offsets_here) + (ready,))
            group = dict(zip(offsets_here, tied[:-1]))
        pieces = [
            pick(group, [j - t for t in range(tp_count)], tp_rank).astype(jnp.float32)
            for j in range(tp_count)
        ]
        squares = sum(jnp.sum(piece * piece, axis=1) for piece in pieces)
        inverse = lax.rsqrt(squares / MODEL_WIDTH + epsilon)
        normed = jnp.concatenate(
            [
                (
                    pieces[j] * inverse[:, None] * gain[None, j * features : (j + 1) * features]
                ).astype(jnp.bfloat16)
                for j in range(tp_count)
            ],
            axis=1,
        )
        gate_total = jnp.dot(normed, w_gate[0], preferred_element_type=jnp.float32)
        up_total = jnp.dot(normed, w_up[0], preferred_element_type=jnp.float32)
        hidden = (jax.nn.silu(gate_total) * up_total).astype(jnp.bfloat16)
        ready = hidden
        hidden_slots = line_gather(hidden)
        total = None
        for m in range(tp_count):
            offsets = [table[t][m] for t in range(tp_count)]
            block = pick(hidden_slots, offsets, tp_rank)
            place = tp_rank + jnp.asarray(offsets, jnp.int32)[tp_rank]
            rows = lax.dynamic_slice_in_dim(down_weight, place * hidden_local, hidden_local)
            term = jnp.dot(block, rows, preferred_element_type=jnp.float32)
            total = term if total is None else total + term
        totals.append(total)
    update_rows = totals[0]
    for k in range(1, seq_count):
        update_rows = update_rows + passed_along(
            totals[k].astype(jnp.bfloat16), "seq", -k
        ).astype(jnp.float32)
    layer_local = (wide + update_rows).astype(jnp.bfloat16)
    incoming = passed_along(layer_local, "pp", 1)
    incoming_wide = incoming.astype(jnp.float32)
    own_square = jnp.sum(incoming_wide * incoming_wide, axis=1)
    incoming_total = own_square
    for k in range(1, tp_count):
        incoming_total = incoming_total + passed_along(own_square, "tp", k)
    scale_rows = lax.rsqrt(incoming_total / MODEL_WIDTH + epsilon)
    kv_gain_part = lax.dynamic_slice_in_dim(kv_gain[0], tp_rank * features, features)
    kv_input = (incoming_wide * kv_gain_part[None, :]).astype(jnp.bfloat16)
    kv_weight = key_value_weight[0]
    span = kv_weight.shape[1] // tp_count
    mapped_rows = jnp.dot(kv_input, kv_weight, preferred_element_type=jnp.float32)
    kv_span = lax.dynamic_slice_in_dim(mapped_rows, tp_rank * span, span, 1)
    mapped_bits = mapped_rows.astype(jnp.bfloat16)
    for k in range(1, tp_count):
        part = lax.dynamic_slice_in_dim(mapped_bits, lax.rem(tp_rank + k, tp_count) * span, span, 1)
        kv_span = kv_span + passed_along(part, "tp", k).astype(jnp.float32)
    kv_span = kv_span * scale_rows[:, None]
    span_width = kv_span.shape[1]
    heads_here = span_width // HEAD_SIZE
    divide_heads = kv_span.reshape(tok_rows, heads_here, HEAD_SIZE)
    mean_square = jnp.mean(divide_heads * divide_heads, axis=2, keepdims=True)
    norm_applied = divide_heads * lax.rsqrt(mean_square + epsilon) * k_gain[0][None, None, :]
    head_index_list = tp_rank * heads_here + jnp.arange(heads_here, dtype=jnp.int32)
    kv_result = (
        jnp.where((head_index_list < KEY_VALUE_HEADS)[None, :, None], norm_applied, divide_heads)
        .reshape(tok_rows, span_width)
        .astype(jnp.bfloat16)
    )
    return (attended[None], layer_local[None], kv_result[None])


MESH = pl.DeviceIdType.MESH


def part_rows(rows):
    second = max(rows // 3 // 64 * 64, 64)
    return rows - second, second


def relay_kernel(
    sizes,
    lengths_ref,
    queries_ref,
    keys_ref,
    values_ref,
    resid_ref,
    ffn_gain_ref,
    w_gate_ref,
    w_up_ref,
    w_down_ref,
    kv_gain_ref,
    kv_weight_ref,
    k_gain_ref,
    attn_ref,
    layer_ref,
    kv_next_ref,
    gate_w,
    up_w,
    down_w,
    x_buf,
    h_buf,
    h_tail,
    g_buf,
    own_acc,
    other_acc,
    part_in,
    stream_in,
    y_buf,
    kv_in,
    kv_own,
    square_buf,
    square_tmp,
    kv_out,
    local_sem,
    out_sem,
    xz_send,
    xz_recv,
    xs_send,
    xs_recv,
    a_send,
    a_recv,
    h_send,
    h_recv,
    p_send,
    p_recv,
    r_send,
    r_recv,
    kv_recv,
    sq_send,
    sq_recv,
    relay_recv,
    relay_sum,
):
    seq_count, tp_count, pp_count = sizes
    s = lax.axis_index("seq")
    t = lax.axis_index("tp")
    p = lax.axis_index("pp")
    rows = resid_ref.shape[1]
    features = resid_ref.shape[2]
    units = w_gate_ref.shape[1]
    width = w_gate_ref.shape[2]
    span = kv_next_ref.shape[2]
    parts = part_rows(rows)
    tail = parts[1] // 2
    kv_heads = keys_ref.shape[2] // HEAD_SIZE
    group = queries_ref.shape[2] // keys_ref.shape[2]
    group_span = group * HEAD_SIZE

    pieces = (
        (0, 0, parts[0]),
        (parts[0], 0, parts[0]),
        (2 * parts[0] + parts[1], parts[0], parts[1]),
        (2 * parts[0], parts[0], parts[1] - tail),
        (2 * parts[0] + parts[1] - tail, rows - tail, tail),
    )
    main = units // 128 * 128
    rest = units - main
    block_n = 256 if main % 256 == 0 else 128
    full_tiles = main // block_n
    split = full_tiles // 2 * block_n
    early, late = (0,), (1, 2) if rest else (1,)
    whole = early + late
    own_pieces = (0, 3, 4)

    def rows_of(c):
        return pl.ds(c * parts[0], parts[c])

    def remote(src, dst, send, recv, where):
        return pltpu.make_async_remote_copy(
            src_ref=src,
            dst_ref=dst,
            send_sem=send,
            recv_sem=recv,
            device_id=where,
            device_id_type=MESH,
        )

    def next_on_line(d):
        return lax.rem(t + 2 * d - 1 + tp_count, tp_count)

    def has_next(d):
        place = t + 2 * d - 1
        return (place >= 0) & (place < tp_count)

    def recv_slot(d, block):
        return lax.rem(block + d + tp_count - 2, tp_count - 1)

    def x_line(d, c, block, own=False):
        dst = x_buf.at[0, block, rows_of(c)]
        src = resid_ref.at[0, rows_of(c)] if own else dst
        return remote(
            src,
            dst,
            xz_send.at[c, block + 1 - d],
            xz_recv.at[c, recv_slot(d, block)],
            {"tp": next_on_line(d)},
        )

    def x_across(c, block, own=False):
        src = resid_ref.at[0, rows_of(c)] if own else x_buf.at[0, block, rows_of(c)]
        return remote(
            src,
            x_buf.at[1, block, rows_of(c)],
            xs_send.at[c, block],
            xs_recv.at[c, block],
            {"seq": 1 - s},
        )

    def subs_of(piece):
        return whole if piece < 3 else (3,) + ((2,) if rest else ())

    def h_line(d, piece, block, sub):
        first, _, count = pieces[piece]
        if sub == 2:
            ref = h_tail.at[block, pl.ds(first // 2, count // 2)]
        else:
            lanes = (pl.ds(0, split), pl.ds(split, main - split), None, pl.ds(0, main))[sub]
            ref = h_buf.at[block, pl.ds(first, count), lanes]
        slot = sub if piece < 3 else (0, 1)[sub == 2]
        recv = 3 * piece + slot if piece < 3 else 9 + 2 * (piece - 3) + slot
        sent = recv if piece < 3 else (recv - 9 if recv < 12 else 9)
        return remote(
            ref,
            ref,
            h_send.at[sent, block + 1 - d],
            h_recv.at[recv, recv_slot(d, block)],
            {"tp": next_on_line(d)},
        )

    key_row = kv_heads * rows
    kv_width = kv_heads * HEAD_SIZE

    def query_place(i):
        return down_w.at[pl.ds(i * rows, rows), pl.ds(0, group_span)]

    def key_place(side, which):
        return down_w.at[
            pl.ds(key_row + side * rows, rows), pl.ds(which * kv_width, kv_width)
        ]

    attn_rows = key_row + seq_count * rows

    def a_across(which):
        src = keys_ref if which == 0 else values_ref
        return remote(
            src.at[0],
            key_place(s, which),
            a_send.at[which],
            a_recv.at[which],
            {"seq": 1 - s},
        )

    def a_arrived(which):
        src = keys_ref if which == 0 else values_ref
        return remote(
            src.at[0],
            key_place(1 - s, which),
            a_send.at[which],
            a_recv.at[which],
            {"seq": 1 - s},
        )

    loads = {}

    def load(name, src, dst):
        loads[name] = pltpu.make_async_copy(src, dst, local_sem.at[len(loads)])
        loads[name].start()

    for i in range(kv_heads):
        load(
            ("q", i),
            queries_ref.at[0, :, pl.ds(i * group_span, group_span)],
            query_place(i),
        )
    load("k", keys_ref.at[0], key_place(s, 0))
    load("v", values_ref.at[0], key_place(s, 1))
    load("x", resid_ref.at[0], x_buf.at[0, t])
    load("gate", w_gate_ref.at[0], gate_w)
    load("up", w_up_ref.at[0], up_w)
    down_rows = w_down_ref.shape[1]
    load(
        "down1",
        w_down_ref.at[0, pl.ds(attn_rows, down_rows - attn_rows)],
        down_w.at[pl.ds(attn_rows, down_rows - attn_rows)],
    )

    barrier = pltpu.get_barrier_semaphore()
    for k in range(1, tp_count):
        pl.semaphore_signal(
            barrier, inc=1, device_id={"tp": lax.rem(t + k, tp_count)}, device_id_type=MESH
        )
    pl.semaphore_signal(barrier, inc=1, device_id={"seq": 1 - s}, device_id_type=MESH)
    for k in (1, pp_count - 1):
        pl.semaphore_signal(
            barrier, inc=1, device_id={"pp": lax.rem(p + k, pp_count)}, device_id_type=MESH
        )
    pl.semaphore_wait(barrier, tp_count - 1 + 1 + 2)

    def send_own_x(d, c, when):
        @pl.when(has_next(d) & when)
        def _():
            x_line(d, c, t, True).start()

    late_low = (t >= 2) & (t <= tp_count - 2)
    late_high = (t >= 1) & (t <= tp_count - 3)
    always = t >= 0
    a_across(0).start()
    a_across(1).start()
    for d in (0, 1):
        send_own_x(d, 0, always)
    x_across(0, t, True).start()
    send_own_x(0, 1, jnp.logical_not(late_low))
    send_own_x(1, 1, jnp.logical_not(late_high))

    def x_events(c, k):
        for d in (0, 1):
            block = t + k * (1 - 2 * d)
            block_safe = lax.rem(block + tp_count, tp_count)

            @pl.when((block >= 0) & (block < tp_count))
            def _():
                x_line(d, c, block_safe).wait_recv()

                @pl.when(has_next(d))
                def _():
                    x_line(d, c, block_safe).start()

                x_across(c, block_safe).start()

    bias = own_acc.at[:, pl.ds(0, seq_count * rows)]
    row_id = lax.broadcasted_iota(jnp.int32, (rows, seq_count * rows), 0) + s * rows
    col_id = lax.broadcasted_iota(jnp.int32, (rows, seq_count * rows), 1)
    bound = lengths_ref[0, 0]
    begin = jnp.zeros_like(row_id)
    for k in range(1, lengths_ref.shape[1]):
        begin = jnp.where(row_id >= bound, bound, begin)
        bound = bound + lengths_ref[0, k]
    own_acc[:, : seq_count * rows] = jnp.where(
        (col_id <= row_id) & (col_id >= begin), 0.0, negative
    )
    inv_root = 1.0 / math.sqrt(HEAD_SIZE)

    def attend(first, last):
        def one(index, carry):
            i = index // group
            j = lax.rem(index, group)
            place = pl.ds(pl.multiple_of(i * rows, 16), rows)
            lanes = pl.ds(pl.multiple_of(j * HEAD_SIZE, HEAD_SIZE), HEAD_SIZE)
            query = down_w[place, lanes]
            key = down_w[
                key_row : key_row + seq_count * rows,
                pl.ds(pl.multiple_of(i * HEAD_SIZE, HEAD_SIZE), HEAD_SIZE),
            ]
            value = down_w[
                key_row : key_row + seq_count * rows,
                pl.ds(pl.multiple_of(kv_width + i * HEAD_SIZE, HEAD_SIZE), HEAD_SIZE),
            ]
            scores = lax.dot_general(
                query, key, (((1,), (1,)), ((), ())), preferred_element_type=jnp.float32
            )
            masked = scores * inv_root + bias[...]
            peak = jnp.max(masked, axis=1, keepdims=True)
            expo = jnp.exp(masked - peak)
            total = jnp.sum(expo, axis=1, keepdims=True)
            mixed = jnp.dot(
                expo.astype(jnp.bfloat16), value, preferred_element_type=jnp.float32
            )
            down_w[place, lanes] = (mixed / total).astype(jnp.bfloat16)
            return carry

        lax.fori_loop(first, last, one, 0)

    heads = kv_heads * group
    middle_head = heads // 2
    x_events(0, 1)
    send_own_x(0, 1, late_low)
    send_own_x(1, 1, late_high)
    for i in range(kv_heads):
        loads[("q", i)].wait()
    loads["k"].wait()
    loads["v"].wait()
    a_arrived(0).wait_recv()
    a_arrived(1).wait_recv()
    attend(0, middle_head)
    for k in range(2, tp_count - 1):
        x_events(0, k)
    x_across(1, t, True).start()
    attend(middle_head, heads)
    attn_copies = [
        pltpu.make_async_copy(
            query_place(i),
            attn_ref.at[0, :, pl.ds(i * group_span, group_span)],
            out_sem.at[i],
        )
        for i in range(kv_heads)
    ]
    for copy in attn_copies:
        copy.start()
    x_events(0, tp_count - 1)
    loads["x"].wait()
    for copy in attn_copies:
        copy.wait()
    load("down0", w_down_ref.at[0, pl.ds(0, attn_rows)], down_w.at[pl.ds(0, attn_rows)])

    lane_tiles = features // 128

    def normalise(side, c, first):
        def squares(block, acc):
            for j in range(lane_tiles):
                x = x_buf[side, block, rows_of(c), j * 128 : (j + 1) * 128].astype(jnp.float32)
                acc = acc + x * x
            return acc

        total = lax.fori_loop(0, tp_count, squares, jnp.zeros((parts[c], 128), jnp.float32))
        inverse = lax.rsqrt(jnp.sum(total, axis=1, keepdims=True) / width + epsilon)

        def write(block, carry):
            for j in range(lane_tiles):
                x = x_buf[side, block, rows_of(c), j * 128 : (j + 1) * 128].astype(jnp.float32)
                lanes = pl.ds(pl.multiple_of(block * features + j * 128, 128), 128)
                g_buf[first : first + parts[c], lanes] = (
                    x * inverse * ffn_gain_ref[0:1, lanes]
                ).astype(jnp.bfloat16)
            return carry

        lax.fori_loop(0, tp_count, write, 0)

    def gated(count, place):
        both = (((1,), (1,)), ((), ()))
        x = g_buf[0:count, :]
        g = lax.dot_general(x, gate_w[place, :], both, preferred_element_type=jnp.float32)
        u = lax.dot_general(x, up_w[place, :], both, preferred_element_type=jnp.float32)
        return g / (1.0 + jnp.exp(-g)) * u

    def hidden_group(group_pieces, hooks):
        first = pieces[group_pieces[0]][0]
        count = sum(pieces[piece][2] for piece in group_pieces)

        def one(i, carry):
            place = pl.ds(pl.multiple_of(i * block_n, block_n), block_n)
            h_buf[t, pl.ds(first, count), place] = gated(count, place).astype(jnp.bfloat16)
            for index, hook in hooks.items():
                pl.when(i == index)(hook)
            return carry

        lax.fori_loop(0, full_tiles, one, 0)
        if rest:
            hidden = gated(count, pl.ds(main, rest))
            for piece in group_pieces:
                start, _, size = pieces[piece]
                low = hidden[start - first : start - first + size // 2]
                high = hidden[start - first + size // 2 : start - first + size]
                h_tail[t, pl.ds(start // 2, size // 2), :] = jnp.concatenate(
                    [low, high], axis=1
                ).astype(jnp.bfloat16)

    def send_hidden(piece, subs):
        for d in (0, 1):

            @pl.when(has_next(d))
            def _():
                for sub in subs:
                    h_line(d, piece, t, sub).start()

    def forward(piece, subs, k):
        if k > tp_count - 2:
            return
        for d in (0, 1):
            block = t + k * (1 - 2 * d)
            block_safe = lax.rem(block + tp_count, tp_count)

            @pl.when((block >= 0) & (block < tp_count) & has_next(d))
            def _():
                for sub in subs:
                    h_line(d, piece, block_safe, sub).wait_recv()
                    h_line(d, piece, block_safe, sub).start()

    def forwards(piece, subs, low):
        for k in range(low, tp_count - 1):
            forward(piece, subs, k)

    down_n = 256 if features % 256 == 0 else 128

    def down(group_pieces, block, fresh):
        first, own_first, _ = pieces[group_pieces[0]]
        count = sum(pieces[piece][2] for piece in group_pieces)
        own = group_pieces[0] in own_pieces
        acc = own_acc.at[pl.ds(own_first, count)] if own else other_acc.at[pl.ds(0, count)]
        if rest:
            extra = []
            for piece in group_pieces:
                start, _, size = pieces[piece]
                packed = h_tail[block, pl.ds(start // 2, size // 2), :]
                extra += [packed[:, :rest], packed[:, rest:]]
            extra = jnp.concatenate(extra, axis=0)

        def one(i, carry):
            lanes = pl.ds(pl.multiple_of(i * down_n, down_n), down_n)
            term = jnp.dot(
                h_buf[block, pl.ds(first, count), :],
                down_w[pl.ds(pl.multiple_of(block * units, 16), main), lanes],
                preferred_element_type=jnp.float32,
            )
            if rest:
                term = term + jnp.dot(
                    extra,
                    down_w[pl.ds(pl.multiple_of(block * units + main, 16), rest), lanes],
                    preferred_element_type=jnp.float32,
                )
            if fresh:
                acc[:, lanes] = term
            else:
                acc[:, lanes] += term
            return carry

        lax.fori_loop(0, features // down_n, one, 0)

    def down_others(group_pieces, low, high):
        def one(index, carry):
            k = index // 2 + 1
            d = lax.rem(index, 2)
            block = t + k * (1 - 2 * d)
            block_safe = lax.rem(block + tp_count, tp_count)

            @pl.when((block >= 0) & (block < tp_count))
            def _():
                @pl.when(jnp.logical_not(has_next(d)))
                def _():
                    for piece in group_pieces:
                        for sub in subs_of(piece):
                            h_line(d, piece, block_safe, sub).wait_recv()

                down(group_pieces, block_safe, False)

            return carry

        lax.fori_loop(2 * (low - 1), 2 * (high - 1), one, 0)

    def wait_other_x(c):
        def one(block, carry):
            x_across(c, block).wait_recv()
            return carry

        lax.fori_loop(0, tp_count, one, 0)

    def part_copy(c):
        return remote(
            x_buf.at[1, 0, rows_of(c)],
            part_in.at[rows_of(c)],
            p_send.at[c],
            p_recv.at[c],
            {"seq": 1 - s},
        )

    def send_part(c):
        x_buf[1, 0, rows_of(c)] = other_acc[0 : parts[c], :].astype(jnp.bfloat16)
        part_copy(c).start()

    def stream_copy(q):
        _, first, count = pieces[own_pieces[q]]
        return remote(
            x_buf.at[1, 1, pl.ds(first, count)],
            stream_in.at[pl.ds(first, count)],
            r_send.at[q],
            r_recv.at[q],
            {"pp": lax.rem(p + 1, pp_count)},
        )

    def layer_copy(q):
        _, first, count = pieces[own_pieces[q]]
        return pltpu.make_async_copy(
            x_buf.at[1, 1, pl.ds(first, count)],
            layer_ref.at[0, pl.ds(first, count)],
            out_sem.at[kv_heads + q],
        )

    def finish_layer(q):
        _, first, count = pieces[own_pieces[q]]
        place = pl.ds(first, count)
        x_buf[1, 1, place] = (
            x_buf[0, t, place].astype(jnp.float32)
            + (own_acc[place, :] + part_in[place, :].astype(jnp.float32))
        ).astype(jnp.bfloat16)
        stream_copy(q).start()
        layer_copy(q).start()

    def hops(source, target):
        return lax.rem(target - source + tp_count, tp_count)

    def sum_sem(q, k):
        return xz_send.at[q, k] if q < 2 else xs_send.at[0, k]

    def square_sem(q, k):
        return sq_send.at[q, k]

    def own_place(q):
        _, first, count = pieces[own_pieces[q]]
        return pl.ds(first, count)

    def kv_copy(q, k, source, target):
        return remote(
            g_buf.at[own_place(q), pl.ds(pl.multiple_of(k * span, HEAD_SIZE), span)],
            kv_in.at[source, own_place(q)],
            sum_sem(q, k),
            kv_recv.at[q, hops(source, target)],
            {"tp": target},
        )

    def relay_copy(q, k, slot, target):
        return remote(
            g_buf.at[own_place(q), pl.ds(pl.multiple_of(k * span, HEAD_SIZE), span)],
            x_buf.at[1, 2, own_place(q), pl.ds(slot * span, span)],
            sum_sem(q, k),
            relay_recv.at[slot],
            {"tp": target},
        )

    def square_copy(q, k, source, target):
        ref = square_buf.at[q, source]
        return remote(ref, ref, square_sem(q, k), sq_recv.at[q, hops(source, target)], {"tp": target})

    def relays(q):
        return q < 1

    def partial_sum(q, target):
        return jnp.dot(
            y_buf[0 : pieces[own_pieces[q]][2], :],
            gate_w[0:features, pl.ds(pl.multiple_of(target * span, HEAD_SIZE), span)],
            preferred_element_type=jnp.float32,
        )

    def start_kv(q):
        _, first, count = pieces[own_pieces[q]]
        place = pl.ds(first, count)
        stream_copy(q).wait_recv()
        total = jnp.zeros((count, 128), jnp.float32)
        for j in range(lane_tiles):
            lanes = slice(j * 128, (j + 1) * 128)
            x = stream_in[place, lanes].astype(jnp.float32)
            total = total + x * x
            gain = kv_gain_ref[0:1, pl.ds(pl.multiple_of(t * features + j * 128, 128), 128)]
            y_buf[0:count, lanes] = (x * gain).astype(jnp.bfloat16)
        if count < 128:
            square_tmp[...] = jnp.zeros_like(square_tmp)
        square_tmp[0:count, :] = jnp.broadcast_to(
            jnp.sum(total, axis=1, keepdims=True), (count, 128)
        )
        square_buf[q, t] = jnp.transpose(square_tmp[...])[0:8]
        for k in range(1, tp_count):
            square_copy(q, k, t, lax.rem(t + k, tp_count)).start()
        for j in range(tp_count - 1):
            near = t >= tp_count // 2
            target = jnp.where(near, j, tp_count - 1 - j)
            target = jnp.where(near & (j >= t), j + 1, target)
            target = jnp.where(jnp.logical_not(near) & (tp_count - 1 - j <= t), tp_count - 2 - j, target)
            k = lax.rem(target - t + tp_count, tp_count)
            lanes = pl.ds(pl.multiple_of(k * span, HEAD_SIZE), span)
            term = partial_sum(q, target)
            if not relays(q):
                g_buf[place, lanes] = term.astype(jnp.bfloat16)
                kv_copy(q, k, t, target).start()
            else:
                low = (target == 0) & (t >= 1)
                high = (target == tp_count - 1) & (t <= tp_count - 2)
                at_relay = (low & (t == 1)) | (high & (t == tp_count - 2))

                @pl.when(at_relay)
                def _():
                    relay_sum[0:count, :] = term

                @pl.when(jnp.logical_not(at_relay))
                def _():
                    g_buf[place, lanes] = term.astype(jnp.bfloat16)

                @pl.when(low & (t >= 2))
                def _():
                    relay_copy(q, k, lax.rem(t - 2 + tp_count, tp_count), 1).start()

                @pl.when(high & (t <= tp_count - 3))
                def _():
                    slot = lax.rem(2 * tp_count - 3 - t, tp_count)
                    relay_copy(q, k, slot, tp_count - 2).start()

                @pl.when(jnp.logical_not(low) & jnp.logical_not(high))
                def _():
                    kv_copy(q, k, t, target).start()

        kv_own[place, :] = partial_sum(q, t)

    def relay_kv(q):
        _, first, count = pieces[own_pieces[q]]
        place = pl.ds(first, count)
        for end, relay in ((0, 1), (tp_count - 1, tp_count - 2)):
            k = (end - relay + tp_count) % tp_count

            @pl.when(t == relay)
            def _():
                total = relay_sum[0:count, :]
                for slot in range(tp_count - 2):
                    relay_copy(q, k, slot, relay).wait_recv()
                    total = total + x_buf[
                        1, 2, place, slot * span : (slot + 1) * span
                    ].astype(jnp.float32)
                g_buf[place, k * span : (k + 1) * span] = total.astype(jnp.bfloat16)
                kv_copy(q, k, t, end).start()

    def kv_out_copy(q):
        _, first, count = pieces[own_pieces[q]]
        return pltpu.make_async_copy(
            kv_out.at[pl.ds(first, count)],
            kv_next_ref.at[0, pl.ds(first, count)],
            out_sem.at[kv_heads + 3 + q],
        )

    def finish_kv(q):
        _, first, count = pieces[own_pieces[q]]
        place = pl.ds(first, count)
        square = square_buf[q, t]
        for k in range(1, tp_count):
            source = lax.rem(t + tp_count - k, tp_count)
            square_copy(q, k, source, t).wait_recv()
            square = square + square_buf[q, source]
        column = jnp.transpose(jnp.broadcast_to(square[0:1], (128, 128)))[0:count, 0:1]
        scale = lax.rsqrt(column / width + epsilon)
        for k in range(1, tp_count):
            source = lax.rem(t + tp_count - k, tp_count)
            through = ((t == 0) & (source > 1)) | (
                (t == tp_count - 1) & (source < tp_count - 2)
            )
            if relays(q):

                @pl.when(jnp.logical_not(through))
                def _():
                    kv_copy(q, k, source, t).wait_recv()
                    kv_own[place, :] += kv_in[source, place, :].astype(jnp.float32)

            else:
                kv_copy(q, k, source, t).wait_recv()
                kv_own[place, :] += kv_in[source, place, :].astype(jnp.float32)
        total = kv_own[place, :]
        total = total * scale
        heads_here = span // HEAD_SIZE
        for h in range(heads_here):
            lanes = slice(h * HEAD_SIZE, (h + 1) * HEAD_SIZE)
            x = total[:, lanes]
            mean_square = jnp.mean(x * x, axis=1, keepdims=True)
            after = x * lax.rsqrt(mean_square + epsilon) * k_gain_ref[0:1, :]
            head = jnp.zeros_like(x, jnp.int32) + (t * heads_here + h)
            kv_out[place, lanes] = jnp.where(head < KEY_VALUE_HEADS, after, x).astype(jnp.bfloat16)
        kv_out_copy(q).start()

    def x_left():
        for c in (0, 1):

            def one(block, carry):
                for d in (0, 1):
                    came = (block - t) * (1 - 2 * d) >= 0

                    @pl.when(has_next(d) & came)
                    def _():
                        x_line(d, c, block).wait_send()

                x_across(c, block).wait_send()
                return carry

            lax.fori_loop(0, tp_count, one, 0)

    def hidden_left(piece):
        def one(block, carry):
            for d in (0, 1):
                came = (block - t) * (1 - 2 * d) >= 0

                @pl.when(has_next(d) & came)
                def _():
                    for sub in subs_of(piece):
                        h_line(d, piece, block, sub).wait_send()

            return carry

        lax.fori_loop(0, tp_count, one, 0)

    def kv_left(q):
        stream_copy(q).wait_send()
        layer_copy(q).wait()
        for k in range(1, tp_count):
            kv_copy(q, k, t, lax.rem(t + k, tp_count)).wait_send()
            square_copy(q, k, t, lax.rem(t + k, tp_count)).wait_send()

    last = tp_count
    loads["gate"].wait()
    loads["up"].wait()
    normalise(0, 0, 0)
    x_events(1, 1)
    middle = full_tiles // 2 - 1

    def first_half_of_0():
        send_hidden(0, early)
        for k in range(2, tp_count - 1):
            x_events(1, k)

    hidden_group((0,), {middle: first_half_of_0})
    send_hidden(0, late)
    x_events(1, tp_count - 1)
    wait_other_x(0)
    forward(0, early, 1)
    normalise(1, 0, 0)
    normalise(0, 1, parts[0])

    hidden_group(
        (1, 3, 4),
        {
            middle - 1: functools.partial(forward, 0, late, 1),
            middle: functools.partial(send_hidden, 1, early),
            middle + 1: functools.partial(forwards, 0, early, 2),
            full_tiles - 1: functools.partial(forwards, 0, late, 2),
        },
    )
    send_hidden(1, late)
    wait_other_x(1)
    forward(1, early, 1)
    normalise(1, 1, 0)
    hidden_group(
        (2,),
        {
            middle: functools.partial(send_hidden, 2, early),
            middle + 1: functools.partial(forward, 1, late, 1),
            middle + 2: functools.partial(forwards, 1, early, 2),
        },
    )
    send_hidden(2, late)
    load(
        "kv",
        kv_weight_ref.at[0],
        gate_w.at[pl.ds(0, features), pl.ds(0, tp_count * span)],
    )
    forward(2, early, 1)
    loads["down0"].wait()
    loads["down1"].wait()
    down((0,), t, True)
    forwards(1, late, 2)
    down_others((0,), 1, last)
    forward(2, late, 1)
    hidden_left(0)
    send_hidden(3, subs_of(3))
    send_hidden(4, subs_of(4))
    down((1,), t, True)
    forwards(2, early, 2)
    down_others((1,), 1, last)
    send_part(0)
    forwards(2, late, 2)
    down((2,), t, True)
    down_others((2,), 1, 2)
    forward(3, subs_of(3), 1)
    x_left()
    down_others((2,), 2, last - 1)
    part_copy(0).wait_recv()
    finish_layer(0)
    forward(4, subs_of(4), 1)
    forwards(3, subs_of(3), 2)
    hidden_left(1)
    loads["kv"].wait()
    start_kv(0)
    down_others((2,), last - 1, last)
    send_part(1)
    forwards(4, subs_of(4), 2)
    down((3, 4), t, True)
    down_others((3, 4), 1, last - 1)
    down_others((3,), last - 1, last)
    part_copy(1).wait_recv()
    finish_layer(1)
    relay_kv(0)
    down_others((4,), last - 1, last)
    finish_layer(2)
    for piece in (2, 3, 4):
        hidden_left(piece)
    start_kv(1)
    finish_kv(0)
    for which in (0, 1):
        a_across(which).wait_send()
        part_copy(which).wait_send()
    start_kv(2)
    kv_left(0)
    finish_kv(1)
    kv_left(1)
    finish_kv(2)
    kv_left(2)
    for q in range(3):
        kv_out_copy(q).wait()


def settle_kernel(cuts, a_ref, b_ref, c_ref, a_out, b_out, c_out, a_buf, b_buf, c_buf, sem):
    into, out = [], []
    for src, buf, dst, cut in zip(
        (a_ref, b_ref, c_ref), (a_buf, b_buf, c_buf), (a_out, b_out, c_out), cuts
    ):
        count = src.shape[1] // cut
        for i in range(cut):
            place = pl.ds(i * count, count)
            n = len(into)
            into.append(
                pltpu.make_async_copy(src.at[:, place], buf.at[:, place], sem.at[0, n])
            )
            out.append(pltpu.make_async_copy(buf.at[:, place], dst.at[:, place], sem.at[1, n]))
    for copy in into:
        copy.start()
    for first, second in zip(into, out):
        first.wait()
        second.start()
    for copy in out:
        copy.wait()


def fits(shape, queries, keys, doc_lengths, resid, w_gate, w_down, key_value_weight):
    rows, features = resid.shape[1:]
    units = w_gate.shape[2]
    span = key_value_weight.shape[2] // shape["tp"]
    tp_span = key_value_weight.shape[2]
    group_span = HEAD_SIZE * queries.shape[2] // keys.shape[2]
    return (
        shape["seq"] == 2
        and shape["pp"] >= 3
        and shape["tp"] >= 3
        and rows % 64 == 0
        and features % 128 == 0
        and units % 128 in (0, 64)
        and units >= 512
        and 128 <= rows <= 192
        and part_rows(rows)[0] <= 128
        and (shape["tp"] - 2) * span <= features
        and span % HEAD_SIZE == 0
        and features <= units
        and tp_span <= resid.shape[2] * shape["tp"]
        and 2 * span <= features
        and group_span <= features
        and keys.shape[2] * 2 <= features
        and 2 * rows <= features
        and queries.shape[2] // group_span * rows + 2 * rows < w_down.shape[1]
    )


def body(
    shape,
    queries,
    keys,
    values,
    doc_lengths,
    resid,
    ffn_gain,
    w_gate,
    w_up,
    w_down,
    kv_gain,
    key_value_weight,
    k_gain,
):
    if not fits(shape, queries, keys, doc_lengths, resid, w_gate, w_down, key_value_weight):
        return plain_body(
            queries,
            keys,
            values,
            doc_lengths,
            resid,
            ffn_gain,
            w_gate,
            w_up,
            w_down,
            kv_gain,
            key_value_weight,
            k_gain,
        )
    sizes = (shape["seq"], shape["tp"], shape["pp"])
    tp_count = shape["tp"]
    rows, features = resid.shape[1:]
    width, units = w_gate.shape[1:]
    span = key_value_weight.shape[2] // tp_count
    half = part_rows(rows)[0]
    kv_heads = keys.shape[2] // HEAD_SIZE
    bf16, f32 = jnp.bfloat16, jnp.float32
    hbm = pl.BlockSpec(memory_space=pl.ANY)
    vmem = pl.BlockSpec(memory_space=pltpu.VMEM)
    smem = pl.BlockSpec(memory_space=pltpu.SMEM)
    dma = pltpu.SemaphoreType.DMA
    parts = pl.pallas_call(
            functools.partial(relay_kernel, sizes),
            out_shape=(
                jax.ShapeDtypeStruct(queries.shape, bf16),
                jax.ShapeDtypeStruct(resid.shape, bf16),
                jax.ShapeDtypeStruct((1, rows, span), bf16),
            ),
            in_specs=[smem, hbm, hbm, hbm, hbm, vmem, hbm, hbm, hbm, vmem, hbm, vmem],
            out_specs=(hbm, hbm, hbm),
            scratch_shapes=[
                pltpu.VMEM((units, width), bf16),
                pltpu.VMEM((units, width), bf16),
                pltpu.VMEM(w_down.shape[1:], bf16),
                pltpu.VMEM((2, tp_count, rows, features), bf16),
                pltpu.VMEM((tp_count, 2 * rows, units // 128 * 128), bf16),
                pltpu.VMEM((tp_count, rows, 128), bf16),
                pltpu.VMEM((rows, width), bf16),
                pltpu.VMEM((rows, features), f32),
                pltpu.VMEM((half, features), f32),
                pltpu.VMEM((rows, features), bf16),
                pltpu.VMEM((rows, features), bf16),
                pltpu.VMEM((half, features), bf16),
                pltpu.VMEM((tp_count, rows, span), bf16),
                pltpu.VMEM((rows, span), f32),
                pltpu.VMEM((3, tp_count, 8, 128), f32),
                pltpu.VMEM((128, 128), f32),
                pltpu.VMEM((rows, span), bf16),
                dma((kv_heads + 8,)),
                dma((kv_heads + 6,)),
                dma((2, tp_count + 1)),
                dma((2, tp_count - 1)),
                dma((2, tp_count)),
                dma((2, tp_count)),
                dma((2,)),
                dma((2,)),
                dma((10, tp_count + 1)),
                dma((13, tp_count - 1)),
                dma((2,)),
                dma((2,)),
                dma((3,)),
                dma((3,)),
                dma((3, tp_count)),
                dma((3, tp_count)),
                dma((3, tp_count)),
                dma((tp_count - 2,)),
                pltpu.VMEM((half, span), f32),
            ],
            compiler_params=pltpu.CompilerParams(
                collective_id=0, has_side_effects=True, vmem_limit_bytes=67043328
            ),
            name="relay_step",
        )(
            doc_lengths,
            queries,
            keys,
            values,
            resid,
            ffn_gain,
            jnp.swapaxes(w_gate, 1, 2),
            jnp.swapaxes(w_up, 1, 2),
            w_down,
            kv_gain,
            key_value_weight,
            k_gain,
        )
    hbm_shapes = [jax.ShapeDtypeStruct(part.shape, part.dtype) for part in parts]
    return tuple(
        pl.pallas_call(
            functools.partial(settle_kernel, (4, 2, 1)),
            out_shape=tuple(hbm_shapes),
            in_specs=[hbm] * 3,
            out_specs=(hbm,) * 3,
            scratch_shapes=[pltpu.VMEM(part.shape, part.dtype) for part in parts] + [dma((2, 7))],
            name="settle",
        )(*parts)
    )


def solution(mesh):
    placed = (
        P("pp", "seq", "tp"),
        P("pp", "seq", "tp"),
        P("pp", "seq", "tp"),
        P("pp", None),
        P("pp", "seq", "tp"),
        P("pp", None),
        P("pp", None, ("seq", "tp")),
        P("pp", None, ("seq", "tp")),
        P("pp", "seq", "tp"),
        P("pp", None),
        P("pp", "tp", None),
        P("pp", None),
    )
    return jax.shard_map(
        functools.partial(body, dict(mesh.shape)),
        mesh=mesh,
        in_specs=placed,
        out_specs=(P("pp", "seq", "tp"), P("pp", "seq", "tp"), P("pp", "seq", "tp")),
        check_vma=False,
    )
```

```python
import functools
import math

import jax
import jax.numpy as jnp
from jax import lax
from jax.experimental import pallas as pl
from jax.experimental.pallas import tpu as pltpu
from jax.sharding import PartitionSpec as P

MODEL_WIDTH = 5120
QUERY_HEADS = 64
KEY_VALUE_HEADS = 8
HEAD_SIZE = 128


epsilon = 1e-06
negative = -1e30


def passed_along(block, axis, distance):
    count = lax.axis_size(axis)
    return lax.ppermute(block, axis, [(i, (i + distance) % count) for i in range(count)])


def passed_where(block, distance, places):
    seq_count = lax.axis_size("seq")
    tp_count = lax.axis_size("tp")
    route = [
        (s * tp_count + t, ((s + distance) % seq_count) * tp_count + t)
        for s in range(seq_count)
        for t in places
    ]
    return lax.ppermute(block, ("seq", "tp"), route)


def line_gather(block):
    count = lax.axis_size("tp")
    slots = {0: block}
    for k in range(1, count):
        slots[-k] = lax.ppermute(
            slots[1 - k], "tp", [(i, i + 1) for i in range(k - 1, count - 1)]
        )
        slots[k] = lax.ppermute(
            slots[k - 1], "tp", [(i, i - 1) for i in range(1, count - k + 1)]
        )
    return slots


def valid_places(offset, count):
    return [t for t in range(count) if 0 <= t + offset < count]


def pick(slots, offsets, tp_rank):
    picked = slots[offsets[0]]
    for t in range(1, len(offsets)):
        if offsets[t] != offsets[t - 1] or len(set(offsets)) > 1:
            picked = jnp.where(tp_rank == t, slots[offsets[t]], picked)
    return picked


def arrival_order(count):
    table = []
    for t in range(count):
        order = [0]
        for k in range(1, count):
            order += [d for d in (-k, k) if 0 <= t + d < count]
        table.append(order)
    return table


def document_ids(places, bounds):
    return jnp.sum((places[:, None] >= bounds[None, :]).astype(jnp.int32), axis=1)


def seq_gather(block):
    count = lax.axis_size("seq")
    rank = lax.axis_index("seq")
    rows = block.shape[0]
    whole = jnp.zeros((count * rows, block.shape[1]), block.dtype)
    for k in range(count):
        part = block if k == 0 else passed_along(block, "seq", k)
        whole = lax.dynamic_update_slice_in_dim(whole, part, lax.rem(rank - k + count, count) * rows, 0)
    return whole


def attend_rows(query_rows, query_places, keys_local, values_local, lengths):
    bounds = jnp.cumsum(lengths)
    query_docs = document_ids(query_places, bounds)
    row_count = query_rows.shape[0]
    kv_heads = keys_local.shape[1] // HEAD_SIZE
    group_width = QUERY_HEADS // KEY_VALUE_HEADS
    query_four = query_rows.reshape(row_count, kv_heads, group_width, HEAD_SIZE)
    inv_root = 1.0 / math.sqrt(HEAD_SIZE)
    key_piece = seq_gather(keys_local)
    value_piece = seq_gather(values_local)
    key_count = key_piece.shape[0]

    key_places = jnp.arange(key_count, dtype=jnp.int32)
    key_docs = document_ids(key_places, bounds)
    visible = (query_docs[:, None] == key_docs[None, :]) & (
        key_places[None, :] <= query_places[:, None]
    )
    scores = (
        jnp.einsum(
            "rkgd,nkd->kgrn",
            query_four,
            key_piece.reshape(key_count, kv_heads, HEAD_SIZE),
            preferred_element_type=jnp.float32,
        )
        * inv_root
    )
    masked = jnp.where(visible, scores, negative)
    row_max = jnp.max(masked, axis=3)
    exponent = jnp.where(visible, jnp.exp(masked - row_max[..., None]), 0.0)
    running_sum = jnp.sum(exponent, axis=3)
    weighted = jnp.einsum(
        "kgrn,nkd->kgrd",
        exponent.astype(jnp.bfloat16),
        value_piece.reshape(key_count, kv_heads, HEAD_SIZE),
        preferred_element_type=jnp.float32,
    )
    mixed = weighted / running_sum[..., None]
    return (
        jnp.transpose(mixed, (2, 0, 1, 3))
        .reshape(row_count, kv_heads * group_width * HEAD_SIZE)
        .astype(jnp.bfloat16)
    )


def plain_body(
    queries,
    keys,
    values,
    doc_lengths,
    resid,
    ffn_gain,
    w_gate,
    w_up,
    w_down,
    kv_gain,
    key_value_weight,
    k_gain,
):
    seq_count = lax.axis_size("seq")
    seq_rank = lax.axis_index("seq")
    tp_count = lax.axis_size("tp")
    tp_rank = lax.axis_index("tp")
    tok_rows = queries.shape[1]
    lengths = doc_lengths[0]
    query_local = queries[0]
    query_places = seq_rank * tok_rows + jnp.arange(tok_rows, dtype=jnp.int32)
    attended = attend_rows(query_local, query_places, keys[0], values[0], lengths)
    resid_local = resid[0]
    wide = resid_local.astype(jnp.float32)
    features = resid_local.shape[1]
    hidden_local = w_gate.shape[2]
    slots = line_gather(resid_local)
    groups = [slots]
    for k in range(1, seq_count):
        groups.append(
            {d: passed_where(slots[d], k, valid_places(d, tp_count)) for d in sorted(slots, key=abs)}
        )
    gain = ffn_gain[0]
    table = arrival_order(tp_count)
    down_weight = w_down[0]
    totals = []
    ready = None
    for group in groups:
        if ready is not None:
            offsets_here = sorted(group)
            tied = lax.optimization_barrier(tuple(group[d] for d in offsets_here) + (ready,))
            group = dict(zip(offsets_here, tied[:-1]))
        pieces = [
            pick(group, [j - t for t in range(tp_count)], tp_rank).astype(jnp.float32)
            for j in range(tp_count)
        ]
        squares = sum(jnp.sum(piece * piece, axis=1) for piece in pieces)
        inverse = lax.rsqrt(squares / MODEL_WIDTH + epsilon)
        normed = jnp.concatenate(
            [
                (
                    pieces[j] * inverse[:, None] * gain[None, j * features : (j + 1) * features]
                ).astype(jnp.bfloat16)
                for j in range(tp_count)
            ],
            axis=1,
        )
        gate_total = jnp.dot(normed, w_gate[0], preferred_element_type=jnp.float32)
        up_total = jnp.dot(normed, w_up[0], preferred_element_type=jnp.float32)
        hidden = (jax.nn.silu(gate_total) * up_total).astype(jnp.bfloat16)
        ready = hidden
        hidden_slots = line_gather(hidden)
        total = None
        for m in range(tp_count):
            offsets = [table[t][m] for t in range(tp_count)]
            block = pick(hidden_slots, offsets, tp_rank)
            place = tp_rank + jnp.asarray(offsets, jnp.int32)[tp_rank]
            rows = lax.dynamic_slice_in_dim(down_weight, place * hidden_local, hidden_local)
            term = jnp.dot(block, rows, preferred_element_type=jnp.float32)
            total = term if total is None else total + term
        totals.append(total)
    update_rows = totals[0]
    for k in range(1, seq_count):
        update_rows = update_rows + passed_along(
            totals[k].astype(jnp.bfloat16), "seq", -k
        ).astype(jnp.float32)
    layer_local = (wide + update_rows).astype(jnp.bfloat16)
    incoming = passed_along(layer_local, "pp", 1)
    incoming_wide = incoming.astype(jnp.float32)
    own_square = jnp.sum(incoming_wide * incoming_wide, axis=1)
    incoming_total = own_square
    for k in range(1, tp_count):
        incoming_total = incoming_total + passed_along(own_square, "tp", k)
    scale_rows = lax.rsqrt(incoming_total / MODEL_WIDTH + epsilon)
    kv_gain_part = lax.dynamic_slice_in_dim(kv_gain[0], tp_rank * features, features)
    kv_input = (incoming_wide * kv_gain_part[None, :]).astype(jnp.bfloat16)
    kv_weight = key_value_weight[0]
    span = kv_weight.shape[1] // tp_count
    mapped_rows = jnp.dot(kv_input, kv_weight, preferred_element_type=jnp.float32)
    kv_span = lax.dynamic_slice_in_dim(mapped_rows, tp_rank * span, span, 1)
    mapped_bits = mapped_rows.astype(jnp.bfloat16)
    for k in range(1, tp_count):
        part = lax.dynamic_slice_in_dim(mapped_bits, lax.rem(tp_rank + k, tp_count) * span, span, 1)
        kv_span = kv_span + passed_along(part, "tp", k).astype(jnp.float32)
    kv_span = kv_span * scale_rows[:, None]
    span_width = kv_span.shape[1]
    heads_here = span_width // HEAD_SIZE
    divide_heads = kv_span.reshape(tok_rows, heads_here, HEAD_SIZE)
    mean_square = jnp.mean(divide_heads * divide_heads, axis=2, keepdims=True)
    norm_applied = divide_heads * lax.rsqrt(mean_square + epsilon) * k_gain[0][None, None, :]
    head_index_list = tp_rank * heads_here + jnp.arange(heads_here, dtype=jnp.int32)
    kv_result = (
        jnp.where((head_index_list < KEY_VALUE_HEADS)[None, :, None], norm_applied, divide_heads)
        .reshape(tok_rows, span_width)
        .astype(jnp.bfloat16)
    )
    return (attended[None], layer_local[None], kv_result[None])


MESH = pl.DeviceIdType.MESH


def part_rows(rows):
    second = max(rows // 3 // 64 * 64, 64)
    return rows - second, second


def relay_kernel(
    sizes,
    lengths_ref,
    queries_ref,
    keys_ref,
    values_ref,
    resid_ref,
    ffn_gain_ref,
    w_gate_ref,
    w_up_ref,
    w_down_ref,
    kv_gain_ref,
    kv_weight_ref,
    k_gain_ref,
    attn_ref,
    layer_ref,
    kv_next_ref,
    gate_w,
    up_w,
    down_w,
    x_buf,
    h_buf,
    h_tail,
    g_buf,
    own_acc,
    other_acc,
    part_in,
    stream_in,
    y_buf,
    kv_in,
    kv_own,
    square_buf,
    square_tmp,
    kv_out,
    local_sem,
    out_sem,
    xz_send,
    xz_recv,
    xs_send,
    xs_recv,
    a_send,
    a_recv,
    h_send,
    h_recv,
    p_send,
    p_recv,
    r_send,
    r_recv,
    kv_recv,
    sq_send,
    sq_recv,
    relay_recv,
    relay_sum,
):
    seq_count, tp_count, pp_count = sizes
    s = lax.axis_index("seq")
    t = lax.axis_index("tp")
    p = lax.axis_index("pp")
    barrier = pltpu.get_barrier_semaphore()
    for k in range(1, tp_count):
        pl.semaphore_signal(
            barrier, inc=1, device_id={"tp": lax.rem(t + k, tp_count)}, device_id_type=MESH
        )
    pl.semaphore_signal(barrier, inc=1, device_id={"seq": 1 - s}, device_id_type=MESH)
    for k in (1, pp_count - 1):
        pl.semaphore_signal(
            barrier, inc=1, device_id={"pp": lax.rem(p + k, pp_count)}, device_id_type=MESH
        )
    rows = resid_ref.shape[1]
    features = resid_ref.shape[2]
    units = w_gate_ref.shape[1]
    width = w_gate_ref.shape[2]
    span = kv_next_ref.shape[2]
    parts = part_rows(rows)
    tail = parts[1] // 2
    kv_heads = keys_ref.shape[2] // HEAD_SIZE
    group = queries_ref.shape[2] // keys_ref.shape[2]
    group_span = group * HEAD_SIZE

    pieces = (
        (0, 0, parts[0]),
        (parts[0], 0, parts[0]),
        (2 * parts[0] + parts[1], parts[0], parts[1]),
        (2 * parts[0], parts[0], parts[1] - tail),
        (2 * parts[0] + parts[1] - tail, rows - tail, tail),
    )
    main = units // 128 * 128
    rest = units - main
    block_n = 256 if main % 256 == 0 else 128
    full_tiles = main // block_n
    split = full_tiles // 2 * block_n
    early, late = (0,), (1, 2) if rest else (1,)
    whole = early + late
    own_pieces = (0, 3, 4)

    def rows_of(c):
        return pl.ds(c * parts[0], parts[c])

    def remote(src, dst, send, recv, where):
        return pltpu.make_async_remote_copy(
            src_ref=src,
            dst_ref=dst,
            send_sem=send,
            recv_sem=recv,
            device_id=where,
            device_id_type=MESH,
        )

    def next_on_line(d):
        return lax.rem(t + 2 * d - 1 + tp_count, tp_count)

    def has_next(d):
        place = t + 2 * d - 1
        return (place >= 0) & (place < tp_count)

    def recv_slot(d, block):
        return lax.rem(block + d + tp_count - 2, tp_count - 1)

    def x_line(d, c, block, own=False):
        dst = x_buf.at[0, block, rows_of(c)]
        src = resid_ref.at[0, rows_of(c)] if own else dst
        return remote(
            src,
            dst,
            xz_send.at[c, block + 1 - d],
            xz_recv.at[c, recv_slot(d, block)],
            {"tp": next_on_line(d)},
        )

    def x_across(c, block, own=False):
        src = resid_ref.at[0, rows_of(c)] if own else x_buf.at[0, block, rows_of(c)]
        return remote(
            src,
            x_buf.at[1, block, rows_of(c)],
            xs_send.at[c, block],
            xs_recv.at[c, block],
            {"seq": 1 - s},
        )

    def subs_of(piece):
        return whole if piece < 3 else (3,) + ((2,) if rest else ())

    def h_line(d, piece, block, sub):
        first, _, count = pieces[piece]
        if sub == 2:
            ref = h_tail.at[block, pl.ds(first // 2, count // 2)]
        else:
            lanes = (pl.ds(0, split), pl.ds(split, main - split), None, pl.ds(0, main))[sub]
            ref = h_buf.at[block, pl.ds(first, count), lanes]
        slot = sub if piece < 3 else (0, 1)[sub == 2]
        recv = 3 * piece + slot if piece < 3 else 9 + 2 * (piece - 3) + slot
        sent = recv if piece < 3 else (recv - 9 if recv < 12 else 9)
        return remote(
            ref,
            ref,
            h_send.at[sent, block + 1 - d],
            h_recv.at[recv, recv_slot(d, block)],
            {"tp": next_on_line(d)},
        )

    key_row = kv_heads * rows
    kv_width = kv_heads * HEAD_SIZE

    def query_place(i):
        return down_w.at[pl.ds(i * rows, rows), pl.ds(0, group_span)]

    def key_place(side, which):
        return down_w.at[
            pl.ds(key_row + side * rows, rows), pl.ds(which * kv_width, kv_width)
        ]

    attn_rows = key_row + seq_count * rows

    def a_across(which):
        src = keys_ref if which == 0 else values_ref
        return remote(
            src.at[0],
            key_place(s, which),
            a_send.at[which],
            a_recv.at[which],
            {"seq": 1 - s},
        )

    def a_arrived(which):
        src = keys_ref if which == 0 else values_ref
        return remote(
            src.at[0],
            key_place(1 - s, which),
            a_send.at[which],
            a_recv.at[which],
            {"seq": 1 - s},
        )

    loads = {}

    def load(name, src, dst):
        loads[name] = pltpu.make_async_copy(src, dst, local_sem.at[len(loads)])
        loads[name].start()

    for i in range(kv_heads):
        load(
            ("q", i),
            queries_ref.at[0, :, pl.ds(i * group_span, group_span)],
            query_place(i),
        )
    load("k", keys_ref.at[0], key_place(s, 0))
    load("v", values_ref.at[0], key_place(s, 1))
    load("x", resid_ref.at[0], x_buf.at[0, t])
    load("gate", w_gate_ref.at[0], gate_w)
    load("up", w_up_ref.at[0], up_w)
    down_rows = w_down_ref.shape[1]
    load(
        "down1",
        w_down_ref.at[0, pl.ds(attn_rows, down_rows - attn_rows)],
        down_w.at[pl.ds(attn_rows, down_rows - attn_rows)],
    )

    pl.semaphore_wait(barrier, tp_count - 1 + 1 + 2)

    def send_own_x(d, c, when):
        @pl.when(has_next(d) & when)
        def _():
            x_line(d, c, t, True).start()

    late_low = (t >= 2) & (t <= tp_count - 2)
    late_high = (t >= 1) & (t <= tp_count - 3)
    always = t >= 0
    for d in (0, 1):
        send_own_x(d, 0, always)
    a_across(0).start()
    a_across(1).start()
    send_own_x(0, 1, jnp.logical_not(late_low))
    send_own_x(1, 1, jnp.logical_not(late_high))
    x_across(0, t, True).start()

    def x_events(c, k):
        for d in (0, 1):
            block = t + k * (1 - 2 * d)
            block_safe = lax.rem(block + tp_count, tp_count)

            @pl.when((block >= 0) & (block < tp_count))
            def _():
                x_line(d, c, block_safe).wait_recv()

                @pl.when(has_next(d))
                def _():
                    x_line(d, c, block_safe).start()

                x_across(c, block_safe).start()

    bias = own_acc.at[:, pl.ds(0, seq_count * rows)]
    row_id = lax.broadcasted_iota(jnp.int32, (rows, seq_count * rows), 0) + s * rows
    col_id = lax.broadcasted_iota(jnp.int32, (rows, seq_count * rows), 1)
    bound = lengths_ref[0, 0]
    begin = jnp.zeros_like(row_id)
    for k in range(1, lengths_ref.shape[1]):
        begin = jnp.where(row_id >= bound, bound, begin)
        bound = bound + lengths_ref[0, k]
    own_acc[:, : seq_count * rows] = jnp.where(
        (col_id <= row_id) & (col_id >= begin), 0.0, negative
    )
    inv_root = 1.0 / math.sqrt(HEAD_SIZE)

    def attend(first, last):
        def one(index, carry):
            i = index // group
            j = lax.rem(index, group)
            place = pl.ds(pl.multiple_of(i * rows, 16), rows)
            lanes = pl.ds(pl.multiple_of(j * HEAD_SIZE, HEAD_SIZE), HEAD_SIZE)
            query = down_w[place, lanes]
            key = down_w[
                key_row : key_row + seq_count * rows,
                pl.ds(pl.multiple_of(i * HEAD_SIZE, HEAD_SIZE), HEAD_SIZE),
            ]
            value = down_w[
                key_row : key_row + seq_count * rows,
                pl.ds(pl.multiple_of(kv_width + i * HEAD_SIZE, HEAD_SIZE), HEAD_SIZE),
            ]
            scores = lax.dot_general(
                query, key, (((1,), (1,)), ((), ())), preferred_element_type=jnp.float32
            )
            masked = scores * inv_root + bias[...]
            peak = jnp.max(masked, axis=1, keepdims=True)
            expo = jnp.exp(masked - peak)
            total = jnp.sum(expo, axis=1, keepdims=True)
            mixed = jnp.dot(
                expo.astype(jnp.bfloat16), value, preferred_element_type=jnp.float32
            )
            down_w[place, lanes] = (mixed / total).astype(jnp.bfloat16)
            return carry

        lax.fori_loop(first, last, one, 0)

    heads = kv_heads * group
    middle_head = heads // 2
    x_events(0, 1)
    send_own_x(0, 1, late_low)
    send_own_x(1, 1, late_high)
    for i in range(kv_heads):
        loads[("q", i)].wait()
    loads["k"].wait()
    loads["v"].wait()
    a_arrived(0).wait_recv()
    a_arrived(1).wait_recv()
    attend(0, middle_head)
    for k in range(2, tp_count - 1):
        x_events(0, k)
    x_across(1, t, True).start()
    attend(middle_head, heads)
    x_events(1, 1)
    attn_copies = [
        pltpu.make_async_copy(
            query_place(i),
            attn_ref.at[0, :, pl.ds(i * group_span, group_span)],
            out_sem.at[i],
        )
        for i in range(kv_heads)
    ]
    for copy in attn_copies:
        copy.start()
    x_events(0, tp_count - 1)
    loads["x"].wait()
    for copy in attn_copies:
        copy.wait()
    load("down0", w_down_ref.at[0, pl.ds(0, attn_rows)], down_w.at[pl.ds(0, attn_rows)])

    lane_tiles = features // 128

    def normalise(side, c, first):
        def squares(block, acc):
            for j in range(lane_tiles):
                x = x_buf[side, block, rows_of(c), j * 128 : (j + 1) * 128].astype(jnp.float32)
                acc = acc + x * x
            return acc

        total = lax.fori_loop(0, tp_count, squares, jnp.zeros((parts[c], 128), jnp.float32))
        inverse = lax.rsqrt(jnp.sum(total, axis=1, keepdims=True) / width + epsilon)

        def write(block, carry):
            for j in range(lane_tiles):
                x = x_buf[side, block, rows_of(c), j * 128 : (j + 1) * 128].astype(jnp.float32)
                lanes = pl.ds(pl.multiple_of(block * features + j * 128, 128), 128)
                g_buf[first : first + parts[c], lanes] = (
                    x * inverse * ffn_gain_ref[0:1, lanes]
                ).astype(jnp.bfloat16)
            return carry

        lax.fori_loop(0, tp_count, write, 0)

    def gated(count, place):
        both = (((1,), (1,)), ((), ()))
        x = g_buf[0:count, :]
        g = lax.dot_general(x, gate_w[place, :], both, preferred_element_type=jnp.float32)
        u = lax.dot_general(x, up_w[place, :], both, preferred_element_type=jnp.float32)
        return g / (1.0 + jnp.exp(-g)) * u

    def hidden_group(group_pieces, hooks):
        first = pieces[group_pieces[0]][0]
        count = sum(pieces[piece][2] for piece in group_pieces)

        def one(i, carry):
            place = pl.ds(pl.multiple_of(i * block_n, block_n), block_n)
            h_buf[t, pl.ds(first, count), place] = gated(count, place).astype(jnp.bfloat16)
            for index, hook in hooks.items():
                pl.when(i == index)(hook)
            return carry

        lax.fori_loop(0, full_tiles, one, 0)
        if rest:
            hidden = gated(count, pl.ds(main, rest))
            for piece in group_pieces:
                start, _, size = pieces[piece]
                low = hidden[start - first : start - first + size // 2]
                high = hidden[start - first + size // 2 : start - first + size]
                h_tail[t, pl.ds(start // 2, size // 2), :] = jnp.concatenate(
                    [low, high], axis=1
                ).astype(jnp.bfloat16)

    def send_hidden(piece, subs, inward=None):
        for d in (0, 1):
            place = t + 2 * d - 1
            ending = (place == 0) | (place == tp_count - 1)
            turn = has_next(d)
            if inward is not None:
                turn = turn & (ending if inward else jnp.logical_not(ending))

            @pl.when(turn)
            def _():
                for sub in subs:
                    h_line(d, piece, t, sub).start()

    def forward(piece, subs, k):
        if k > tp_count - 2:
            return
        for d in (0, 1):
            block = t + k * (1 - 2 * d)
            block_safe = lax.rem(block + tp_count, tp_count)

            @pl.when((block >= 0) & (block < tp_count) & has_next(d))
            def _():
                for sub in subs:
                    h_line(d, piece, block_safe, sub).wait_recv()
                    h_line(d, piece, block_safe, sub).start()

    def forwards(piece, subs, low):
        for k in range(low, tp_count - 1):
            forward(piece, subs, k)

    down_n = 256 if features % 256 == 0 else 128

    def down(group_pieces, block, fresh):
        first, own_first, _ = pieces[group_pieces[0]]
        count = sum(pieces[piece][2] for piece in group_pieces)
        own = group_pieces[0] in own_pieces
        acc = own_acc.at[pl.ds(own_first, count)] if own else other_acc.at[pl.ds(0, count)]
        if rest:
            extra = []
            for piece in group_pieces:
                start, _, size = pieces[piece]
                packed = h_tail[block, pl.ds(start // 2, size // 2), :]
                extra += [packed[:, :rest], packed[:, rest:]]
            extra = jnp.concatenate(extra, axis=0)

        def one(i, carry):
            lanes = pl.ds(pl.multiple_of(i * down_n, down_n), down_n)
            term = jnp.dot(
                h_buf[block, pl.ds(first, count), :],
                down_w[pl.ds(pl.multiple_of(block * units, 16), main), lanes],
                preferred_element_type=jnp.float32,
            )
            if rest:
                term = term + jnp.dot(
                    extra,
                    down_w[pl.ds(pl.multiple_of(block * units + main, 16), rest), lanes],
                    preferred_element_type=jnp.float32,
                )
            if fresh:
                acc[:, lanes] = term
            else:
                acc[:, lanes] += term
            return carry

        lax.fori_loop(0, features // down_n, one, 0)

    def down_others(group_pieces, low, high):
        def one(index, carry):
            k = index // 2 + 1
            d = lax.rem(index, 2)
            block = t + k * (1 - 2 * d)
            block_safe = lax.rem(block + tp_count, tp_count)

            @pl.when((block >= 0) & (block < tp_count))
            def _():
                @pl.when(jnp.logical_not(has_next(d)))
                def _():
                    for piece in group_pieces:
                        for sub in subs_of(piece):
                            h_line(d, piece, block_safe, sub).wait_recv()

                down(group_pieces, block_safe, False)

            return carry

        lax.fori_loop(2 * (low - 1), 2 * (high - 1), one, 0)

    def wait_other_x(c):
        def one(block, carry):
            x_across(c, block).wait_recv()
            return carry

        lax.fori_loop(0, tp_count, one, 0)

    def part_copy(c):
        return remote(
            x_buf.at[1, 0, rows_of(c)],
            part_in.at[rows_of(c)],
            p_send.at[c],
            p_recv.at[c],
            {"seq": 1 - s},
        )

    def send_part(c):
        x_buf[1, 0, rows_of(c)] = other_acc[0 : parts[c], :].astype(jnp.bfloat16)
        part_copy(c).start()

    def stream_copy(q):
        _, first, count = pieces[own_pieces[q]]
        return remote(
            x_buf.at[1, 1, pl.ds(first, count)],
            stream_in.at[pl.ds(first, count)],
            r_send.at[q],
            r_recv.at[q],
            {"pp": lax.rem(p + 1, pp_count)},
        )

    def layer_copy(q):
        _, first, count = pieces[own_pieces[q]]
        return pltpu.make_async_copy(
            x_buf.at[1, 1, pl.ds(first, count)],
            layer_ref.at[0, pl.ds(first, count)],
            out_sem.at[kv_heads + q],
        )

    def finish_layer(q):
        _, first, count = pieces[own_pieces[q]]
        place = pl.ds(first, count)
        x_buf[1, 1, place] = (
            x_buf[0, t, place].astype(jnp.float32)
            + (own_acc[place, :] + part_in[place, :].astype(jnp.float32))
        ).astype(jnp.bfloat16)
        stream_copy(q).start()
        layer_copy(q).start()

    def hops(source, target):
        return lax.rem(target - source + tp_count, tp_count)

    def sum_sem(q, k):
        return xz_send.at[q, k] if q < 2 else xs_send.at[0, k]

    def square_sem(q, k):
        return sq_send.at[q, k]

    def own_place(q):
        _, first, count = pieces[own_pieces[q]]
        return pl.ds(first, count)

    def kv_copy(q, k, source, target):
        return remote(
            g_buf.at[own_place(q), pl.ds(pl.multiple_of(k * span, HEAD_SIZE), span)],
            kv_in.at[source, own_place(q)],
            sum_sem(q, k),
            kv_recv.at[q, hops(source, target)],
            {"tp": target},
        )

    def relay_copy(q, k, slot, target):
        return remote(
            g_buf.at[own_place(q), pl.ds(pl.multiple_of(k * span, HEAD_SIZE), span)],
            x_buf.at[1, 2, own_place(q), pl.ds(slot * span, span)],
            sum_sem(q, k),
            relay_recv.at[slot],
            {"tp": target},
        )

    def square_copy(q, k, source, target):
        ref = square_buf.at[q, source]
        return remote(ref, ref, square_sem(q, k), sq_recv.at[q, hops(source, target)], {"tp": target})

    def relays(q):
        return q < 1

    def partial_sum(q, target):
        return jnp.dot(
            y_buf[0 : pieces[own_pieces[q]][2], :],
            gate_w[0:features, pl.ds(pl.multiple_of(target * span, HEAD_SIZE), span)],
            preferred_element_type=jnp.float32,
        )

    def start_kv(q):
        _, first, count = pieces[own_pieces[q]]
        place = pl.ds(first, count)
        stream_copy(q).wait_recv()
        total = jnp.zeros((count, 128), jnp.float32)
        for j in range(lane_tiles):
            lanes = slice(j * 128, (j + 1) * 128)
            x = stream_in[place, lanes].astype(jnp.float32)
            total = total + x * x
            gain = kv_gain_ref[0:1, pl.ds(pl.multiple_of(t * features + j * 128, 128), 128)]
            y_buf[0:count, lanes] = (x * gain).astype(jnp.bfloat16)
        if count < 128:
            square_tmp[...] = jnp.zeros_like(square_tmp)
        square_tmp[0:count, :] = jnp.broadcast_to(
            jnp.sum(total, axis=1, keepdims=True), (count, 128)
        )
        square_buf[q, t] = jnp.transpose(square_tmp[...])[0:8]
        for k in range(1, tp_count):
            square_copy(q, k, t, lax.rem(t + k, tp_count)).start()
        for j in range(tp_count - 1):
            near = t >= tp_count // 2
            target = jnp.where(near, j, tp_count - 1 - j)
            target = jnp.where(near & (j >= t), j + 1, target)
            target = jnp.where(jnp.logical_not(near) & (tp_count - 1 - j <= t), tp_count - 2 - j, target)
            k = lax.rem(target - t + tp_count, tp_count)
            lanes = pl.ds(pl.multiple_of(k * span, HEAD_SIZE), span)
            term = partial_sum(q, target)
            if not relays(q):
                g_buf[place, lanes] = term.astype(jnp.bfloat16)
                kv_copy(q, k, t, target).start()
            else:
                low = (target == 0) & (t >= 1)
                high = (target == tp_count - 1) & (t <= tp_count - 2)
                at_relay = (low & (t == 1)) | (high & (t == tp_count - 2))

                @pl.when(at_relay)
                def _():
                    relay_sum[0:count, :] = term

                @pl.when(jnp.logical_not(at_relay))
                def _():
                    g_buf[place, lanes] = term.astype(jnp.bfloat16)

                @pl.when(low & (t >= 2))
                def _():
                    relay_copy(q, k, lax.rem(t - 2 + tp_count, tp_count), 1).start()

                @pl.when(high & (t <= tp_count - 3))
                def _():
                    slot = lax.rem(2 * tp_count - 3 - t, tp_count)
                    relay_copy(q, k, slot, tp_count - 2).start()

                @pl.when(jnp.logical_not(low) & jnp.logical_not(high))
                def _():
                    kv_copy(q, k, t, target).start()

        kv_own[place, :] = partial_sum(q, t)

    def relay_kv(q):
        _, first, count = pieces[own_pieces[q]]
        place = pl.ds(first, count)
        for end, relay in ((0, 1), (tp_count - 1, tp_count - 2)):
            k = (end - relay + tp_count) % tp_count

            @pl.when(t == relay)
            def _():
                total = relay_sum[0:count, :]
                for slot in range(tp_count - 2):
                    relay_copy(q, k, slot, relay).wait_recv()
                    total = total + x_buf[
                        1, 2, place, slot * span : (slot + 1) * span
                    ].astype(jnp.float32)
                g_buf[place, k * span : (k + 1) * span] = total.astype(jnp.bfloat16)
                kv_copy(q, k, t, end).start()

    def kv_out_copy(q):
        _, first, count = pieces[own_pieces[q]]
        return pltpu.make_async_copy(
            kv_out.at[pl.ds(first, count)],
            kv_next_ref.at[0, pl.ds(first, count)],
            out_sem.at[kv_heads + 3 + q],
        )

    def finish_kv(q):
        _, first, count = pieces[own_pieces[q]]
        place = pl.ds(first, count)
        square = square_buf[q, t]
        for k in range(1, tp_count):
            source = lax.rem(t + tp_count - k, tp_count)
            square_copy(q, k, source, t).wait_recv()
            square = square + square_buf[q, source]
        column = jnp.transpose(jnp.broadcast_to(square[0:1], (128, 128)))[0:count, 0:1]
        scale = lax.rsqrt(column / width + epsilon)
        for k in range(1, tp_count):
            source = lax.rem(t + tp_count - k, tp_count)
            through = ((t == 0) & (source > 1)) | (
                (t == tp_count - 1) & (source < tp_count - 2)
            )
            if relays(q):

                @pl.when(jnp.logical_not(through))
                def _():
                    kv_copy(q, k, source, t).wait_recv()
                    kv_own[place, :] += kv_in[source, place, :].astype(jnp.float32)

            else:
                kv_copy(q, k, source, t).wait_recv()
                kv_own[place, :] += kv_in[source, place, :].astype(jnp.float32)
        total = kv_own[place, :]
        total = total * scale
        heads_here = span // HEAD_SIZE
        for h in range(heads_here):
            lanes = slice(h * HEAD_SIZE, (h + 1) * HEAD_SIZE)
            x = total[:, lanes]
            mean_square = jnp.mean(x * x, axis=1, keepdims=True)
            after = x * lax.rsqrt(mean_square + epsilon) * k_gain_ref[0:1, :]
            head = jnp.zeros_like(x, jnp.int32) + (t * heads_here + h)
            kv_out[place, lanes] = jnp.where(head < KEY_VALUE_HEADS, after, x).astype(jnp.bfloat16)
        kv_out_copy(q).start()

    def x_left():
        for c in (0, 1):

            def one(block, carry):
                for d in (0, 1):
                    came = (block - t) * (1 - 2 * d) >= 0

                    @pl.when(has_next(d) & came)
                    def _():
                        x_line(d, c, block).wait_send()

                x_across(c, block).wait_send()
                return carry

            lax.fori_loop(0, tp_count, one, 0)

    def hidden_left(piece):
        def one(block, carry):
            for d in (0, 1):
                came = (block - t) * (1 - 2 * d) >= 0

                @pl.when(has_next(d) & came)
                def _():
                    for sub in subs_of(piece):
                        h_line(d, piece, block, sub).wait_send()

            return carry

        lax.fori_loop(0, tp_count, one, 0)

    def kv_left(q):
        stream_copy(q).wait_send()
        layer_copy(q).wait()
        for k in range(1, tp_count):
            kv_copy(q, k, t, lax.rem(t + k, tp_count)).wait_send()
            square_copy(q, k, t, lax.rem(t + k, tp_count)).wait_send()

    last = tp_count
    loads["gate"].wait()
    loads["up"].wait()
    normalise(0, 0, 0)
    middle = full_tiles // 2 - 1

    def inner_x():
        for k in range(2, tp_count - 1):
            x_events(1, k)

    hidden_group(
        (0,), {middle - 1: inner_x, middle: functools.partial(send_hidden, 0, early)}
    )
    send_hidden(0, late)
    x_events(1, tp_count - 1)
    wait_other_x(0)
    forward(0, early, 1)
    normalise(1, 0, 0)
    normalise(0, 1, parts[0])

    hidden_group(
        (1, 3, 4),
        {
            middle - 1: functools.partial(forward, 0, late, 1),
            middle: functools.partial(send_hidden, 1, early),
            middle + 1: functools.partial(forwards, 0, early, 2),
            full_tiles - 1: functools.partial(forwards, 0, late, 2),
        },
    )
    send_hidden(1, late)
    wait_other_x(1)
    forward(1, early, 1)
    normalise(1, 1, 0)
    hidden_group(
        (2,),
        {
            middle: functools.partial(send_hidden, 2, early, False),
            middle + 1: functools.partial(forward, 1, late, 1),
            middle + 2: functools.partial(forwards, 1, early, 2),
        },
    )
    send_hidden(2, late, False)
    hidden_left(0)
    send_hidden(3, subs_of(3), False)
    send_hidden(4, subs_of(4), False)
    load(
        "kv",
        kv_weight_ref.at[0],
        gate_w.at[pl.ds(0, features), pl.ds(0, tp_count * span)],
    )
    loads["down0"].wait()
    loads["down1"].wait()
    down((0,), t, True)
    forwards(1, late, 2)
    send_hidden(2, whole, True)
    down_others((0,), 1, last)
    down((1,), t, True)
    forward(2, whole, 1)
    down_others((1,), 1, last)
    send_part(0)
    down((2,), t, True)
    forwards(2, whole, 2)
    send_hidden(3, subs_of(3), True)
    send_hidden(4, subs_of(4), True)
    down_others((2,), 1, last)
    send_part(1)
    x_left()
    forward(3, subs_of(3), 1)
    forward(4, subs_of(4), 1)
    part_copy(0).wait_recv()
    finish_layer(0)
    down((3, 4), t, True)
    down_others((3, 4), 1, 2)
    hidden_left(1)
    loads["kv"].wait()
    forwards(3, subs_of(3), 2)
    start_kv(0)
    forwards(4, subs_of(4), 2)
    down_others((3, 4), 2, last - 1)
    down_others((3,), last - 1, last)
    part_copy(1).wait_recv()
    finish_layer(1)
    relay_kv(0)
    down_others((4,), last - 1, last)
    finish_layer(2)
    for piece in (2, 3, 4):
        hidden_left(piece)
    start_kv(1)
    for which in (0, 1):
        a_across(which).wait_send()
        part_copy(which).wait_send()
    start_kv(2)
    finish_kv(0)
    kv_left(0)
    finish_kv(1)
    kv_left(1)
    finish_kv(2)
    kv_left(2)
    for q in range(3):
        kv_out_copy(q).wait()


def settle_kernel(cuts, a_ref, b_ref, c_ref, a_out, b_out, c_out, a_buf, b_buf, c_buf, sem):
    into, out = [], []
    for src, buf, dst, cut in zip(
        (a_ref, b_ref, c_ref), (a_buf, b_buf, c_buf), (a_out, b_out, c_out), cuts
    ):
        count = src.shape[1] // cut
        for i in range(cut):
            place = pl.ds(i * count, count)
            n = len(into)
            into.append(
                pltpu.make_async_copy(src.at[:, place], buf.at[:, place], sem.at[0, n])
            )
            out.append(pltpu.make_async_copy(buf.at[:, place], dst.at[:, place], sem.at[1, n]))
    for copy in into:
        copy.start()
    for first, second in zip(into, out):
        first.wait()
        second.start()
    for copy in out:
        copy.wait()


def fits(shape, queries, keys, doc_lengths, resid, w_gate, w_down, key_value_weight):
    rows, features = resid.shape[1:]
    units = w_gate.shape[2]
    span = key_value_weight.shape[2] // shape["tp"]
    tp_span = key_value_weight.shape[2]
    group_span = HEAD_SIZE * queries.shape[2] // keys.shape[2]
    return (
        shape["seq"] == 2
        and shape["pp"] >= 3
        and shape["tp"] >= 3
        and rows % 64 == 0
        and features % 128 == 0
        and units % 128 in (0, 64)
        and units >= 512
        and 128 <= rows <= 192
        and part_rows(rows)[0] <= 128
        and (shape["tp"] - 2) * span <= features
        and span % HEAD_SIZE == 0
        and features <= units
        and tp_span <= resid.shape[2] * shape["tp"]
        and 2 * span <= features
        and group_span <= features
        and keys.shape[2] * 2 <= features
        and 2 * rows <= features
        and queries.shape[2] // group_span * rows + 2 * rows < w_down.shape[1]
    )


def body(
    shape,
    queries,
    keys,
    values,
    doc_lengths,
    resid,
    ffn_gain,
    w_gate,
    w_up,
    w_down,
    kv_gain,
    key_value_weight,
    k_gain,
):
    if not fits(shape, queries, keys, doc_lengths, resid, w_gate, w_down, key_value_weight):
        return plain_body(
            queries,
            keys,
            values,
            doc_lengths,
            resid,
            ffn_gain,
            w_gate,
            w_up,
            w_down,
            kv_gain,
            key_value_weight,
            k_gain,
        )
    sizes = (shape["seq"], shape["tp"], shape["pp"])
    tp_count = shape["tp"]
    rows, features = resid.shape[1:]
    width, units = w_gate.shape[1:]
    span = key_value_weight.shape[2] // tp_count
    half = part_rows(rows)[0]
    kv_heads = keys.shape[2] // HEAD_SIZE
    bf16, f32 = jnp.bfloat16, jnp.float32
    hbm = pl.BlockSpec(memory_space=pl.ANY)
    vmem = pl.BlockSpec(memory_space=pltpu.VMEM)
    smem = pl.BlockSpec(memory_space=pltpu.SMEM)
    dma = pltpu.SemaphoreType.DMA
    parts = pl.pallas_call(
            functools.partial(relay_kernel, sizes),
            out_shape=(
                jax.ShapeDtypeStruct(queries.shape, bf16),
                jax.ShapeDtypeStruct(resid.shape, bf16),
                jax.ShapeDtypeStruct((1, rows, span), bf16),
            ),
            in_specs=[smem, hbm, hbm, hbm, hbm, vmem, hbm, hbm, hbm, vmem, hbm, vmem],
            out_specs=(hbm, hbm, hbm),
            scratch_shapes=[
                pltpu.VMEM((units, width), bf16),
                pltpu.VMEM((units, width), bf16),
                pltpu.VMEM(w_down.shape[1:], bf16),
                pltpu.VMEM((2, tp_count, rows, features), bf16),
                pltpu.VMEM((tp_count, 2 * rows, units // 128 * 128), bf16),
                pltpu.VMEM((tp_count, rows, 128), bf16),
                pltpu.VMEM((rows, width), bf16),
                pltpu.VMEM((rows, features), f32),
                pltpu.VMEM((half, features), f32),
                pltpu.VMEM((rows, features), bf16),
                pltpu.VMEM((rows, features), bf16),
                pltpu.VMEM((half, features), bf16),
                pltpu.VMEM((tp_count, rows, span), bf16),
                pltpu.VMEM((rows, span), f32),
                pltpu.VMEM((3, tp_count, 8, 128), f32),
                pltpu.VMEM((128, 128), f32),
                pltpu.VMEM((rows, span), bf16),
                dma((kv_heads + 8,)),
                dma((kv_heads + 6,)),
                dma((2, tp_count + 1)),
                dma((2, tp_count - 1)),
                dma((2, tp_count)),
                dma((2, tp_count)),
                dma((2,)),
                dma((2,)),
                dma((10, tp_count + 1)),
                dma((13, tp_count - 1)),
                dma((2,)),
                dma((2,)),
                dma((3,)),
                dma((3,)),
                dma((3, tp_count)),
                dma((3, tp_count)),
                dma((3, tp_count)),
                dma((tp_count - 2,)),
                pltpu.VMEM((half, span), f32),
            ],
            compiler_params=pltpu.CompilerParams(
                collective_id=0, has_side_effects=True, vmem_limit_bytes=67043328
            ),
            name="relay_step",
        )(
            doc_lengths,
            queries,
            keys,
            values,
            resid,
            ffn_gain,
            jnp.swapaxes(w_gate, 1, 2),
            jnp.swapaxes(w_up, 1, 2),
            w_down,
            kv_gain,
            key_value_weight,
            k_gain,
        )
    hbm_shapes = [jax.ShapeDtypeStruct(part.shape, part.dtype) for part in parts]
    return tuple(
        pl.pallas_call(
            functools.partial(settle_kernel, (4, 2, 1)),
            out_shape=tuple(hbm_shapes),
            in_specs=[hbm] * 3,
            out_specs=(hbm,) * 3,
            scratch_shapes=[pltpu.VMEM(part.shape, part.dtype) for part in parts] + [dma((2, 7))],
            name="settle",
        )(*parts)
    )


def solution(mesh):
    placed = (
        P("pp", "seq", "tp"),
        P("pp", "seq", "tp"),
        P("pp", "seq", "tp"),
        P("pp", None),
        P("pp", "seq", "tp"),
        P("pp", None),
        P("pp", None, ("seq", "tp")),
        P("pp", None, ("seq", "tp")),
        P("pp", "seq", "tp"),
        P("pp", None),
        P("pp", "tp", None),
        P("pp", None),
    )
    return jax.shard_map(
        functools.partial(body, dict(mesh.shape)),
        mesh=mesh,
        in_specs=placed,
        out_specs=(P("pp", "seq", "tp"), P("pp", "seq", "tp"), P("pp", "seq", "tp")),
        check_vma=False,
    )
```

```python
import functools
import math

import jax
import jax.numpy as jnp
from jax import lax
from jax.experimental import pallas as pl
from jax.experimental.pallas import tpu as pltpu
from jax.sharding import PartitionSpec as P

MODEL_WIDTH = 5120
QUERY_HEADS = 64
KEY_VALUE_HEADS = 8
HEAD_SIZE = 128


epsilon = 1e-06
negative = -1e30


def passed_along(block, axis, distance):
    count = lax.axis_size(axis)
    return lax.ppermute(block, axis, [(i, (i + distance) % count) for i in range(count)])


def passed_where(block, distance, places):
    seq_count = lax.axis_size("seq")
    tp_count = lax.axis_size("tp")
    route = [
        (s * tp_count + t, ((s + distance) % seq_count) * tp_count + t)
        for s in range(seq_count)
        for t in places
    ]
    return lax.ppermute(block, ("seq", "tp"), route)


def line_gather(block):
    count = lax.axis_size("tp")
    slots = {0: block}
    for k in range(1, count):
        slots[-k] = lax.ppermute(
            slots[1 - k], "tp", [(i, i + 1) for i in range(k - 1, count - 1)]
        )
        slots[k] = lax.ppermute(
            slots[k - 1], "tp", [(i, i - 1) for i in range(1, count - k + 1)]
        )
    return slots


def valid_places(offset, count):
    return [t for t in range(count) if 0 <= t + offset < count]


def pick(slots, offsets, tp_rank):
    picked = slots[offsets[0]]
    for t in range(1, len(offsets)):
        if offsets[t] != offsets[t - 1] or len(set(offsets)) > 1:
            picked = jnp.where(tp_rank == t, slots[offsets[t]], picked)
    return picked


def arrival_order(count):
    table = []
    for t in range(count):
        order = [0]
        for k in range(1, count):
            order += [d for d in (-k, k) if 0 <= t + d < count]
        table.append(order)
    return table


def document_ids(places, bounds):
    return jnp.sum((places[:, None] >= bounds[None, :]).astype(jnp.int32), axis=1)


def seq_gather(block):
    count = lax.axis_size("seq")
    rank = lax.axis_index("seq")
    rows = block.shape[0]
    whole = jnp.zeros((count * rows, block.shape[1]), block.dtype)
    for k in range(count):
        part = block if k == 0 else passed_along(block, "seq", k)
        whole = lax.dynamic_update_slice_in_dim(whole, part, lax.rem(rank - k + count, count) * rows, 0)
    return whole


def attend_rows(query_rows, query_places, keys_local, values_local, lengths):
    bounds = jnp.cumsum(lengths)
    query_docs = document_ids(query_places, bounds)
    row_count = query_rows.shape[0]
    kv_heads = keys_local.shape[1] // HEAD_SIZE
    group_width = QUERY_HEADS // KEY_VALUE_HEADS
    query_four = query_rows.reshape(row_count, kv_heads, group_width, HEAD_SIZE)
    inv_root = 1.0 / math.sqrt(HEAD_SIZE)
    key_piece = seq_gather(keys_local)
    value_piece = seq_gather(values_local)
    key_count = key_piece.shape[0]

    key_places = jnp.arange(key_count, dtype=jnp.int32)
    key_docs = document_ids(key_places, bounds)
    visible = (query_docs[:, None] == key_docs[None, :]) & (
        key_places[None, :] <= query_places[:, None]
    )
    scores = (
        jnp.einsum(
            "rkgd,nkd->kgrn",
            query_four,
            key_piece.reshape(key_count, kv_heads, HEAD_SIZE),
            preferred_element_type=jnp.float32,
        )
        * inv_root
    )
    masked = jnp.where(visible, scores, negative)
    row_max = jnp.max(masked, axis=3)
    exponent = jnp.where(visible, jnp.exp(masked - row_max[..., None]), 0.0)
    running_sum = jnp.sum(exponent, axis=3)
    weighted = jnp.einsum(
        "kgrn,nkd->kgrd",
        exponent.astype(jnp.bfloat16),
        value_piece.reshape(key_count, kv_heads, HEAD_SIZE),
        preferred_element_type=jnp.float32,
    )
    mixed = weighted / running_sum[..., None]
    return (
        jnp.transpose(mixed, (2, 0, 1, 3))
        .reshape(row_count, kv_heads * group_width * HEAD_SIZE)
        .astype(jnp.bfloat16)
    )


def plain_body(
    queries,
    keys,
    values,
    doc_lengths,
    resid,
    ffn_gain,
    w_gate,
    w_up,
    w_down,
    kv_gain,
    key_value_weight,
    k_gain,
):
    seq_count = lax.axis_size("seq")
    seq_rank = lax.axis_index("seq")
    tp_count = lax.axis_size("tp")
    tp_rank = lax.axis_index("tp")
    tok_rows = queries.shape[1]
    lengths = doc_lengths[0]
    query_local = queries[0]
    query_places = seq_rank * tok_rows + jnp.arange(tok_rows, dtype=jnp.int32)
    attended = attend_rows(query_local, query_places, keys[0], values[0], lengths)
    resid_local = resid[0]
    wide = resid_local.astype(jnp.float32)
    features = resid_local.shape[1]
    hidden_local = w_gate.shape[2]
    slots = line_gather(resid_local)
    groups = [slots]
    for k in range(1, seq_count):
        groups.append(
            {d: passed_where(slots[d], k, valid_places(d, tp_count)) for d in sorted(slots, key=abs)}
        )
    gain = ffn_gain[0]
    table = arrival_order(tp_count)
    down_weight = w_down[0]
    totals = []
    ready = None
    for group in groups:
        if ready is not None:
            offsets_here = sorted(group)
            tied = lax.optimization_barrier(tuple(group[d] for d in offsets_here) + (ready,))
            group = dict(zip(offsets_here, tied[:-1]))
        pieces = [
            pick(group, [j - t for t in range(tp_count)], tp_rank).astype(jnp.float32)
            for j in range(tp_count)
        ]
        squares = sum(jnp.sum(piece * piece, axis=1) for piece in pieces)
        inverse = lax.rsqrt(squares / MODEL_WIDTH + epsilon)
        normed = jnp.concatenate(
            [
                (
                    pieces[j] * inverse[:, None] * gain[None, j * features : (j + 1) * features]
                ).astype(jnp.bfloat16)
                for j in range(tp_count)
            ],
            axis=1,
        )
        gate_total = jnp.dot(normed, w_gate[0], preferred_element_type=jnp.float32)
        up_total = jnp.dot(normed, w_up[0], preferred_element_type=jnp.float32)
        hidden = (jax.nn.silu(gate_total) * up_total).astype(jnp.bfloat16)
        ready = hidden
        hidden_slots = line_gather(hidden)
        total = None
        for m in range(tp_count):
            offsets = [table[t][m] for t in range(tp_count)]
            block = pick(hidden_slots, offsets, tp_rank)
            place = tp_rank + jnp.asarray(offsets, jnp.int32)[tp_rank]
            rows = lax.dynamic_slice_in_dim(down_weight, place * hidden_local, hidden_local)
            term = jnp.dot(block, rows, preferred_element_type=jnp.float32)
            total = term if total is None else total + term
        totals.append(total)
    update_rows = totals[0]
    for k in range(1, seq_count):
        update_rows = update_rows + passed_along(
            totals[k].astype(jnp.bfloat16), "seq", -k
        ).astype(jnp.float32)
    layer_local = (wide + update_rows).astype(jnp.bfloat16)
    incoming = passed_along(layer_local, "pp", 1)
    incoming_wide = incoming.astype(jnp.float32)
    own_square = jnp.sum(incoming_wide * incoming_wide, axis=1)
    incoming_total = own_square
    for k in range(1, tp_count):
        incoming_total = incoming_total + passed_along(own_square, "tp", k)
    scale_rows = lax.rsqrt(incoming_total / MODEL_WIDTH + epsilon)
    kv_gain_part = lax.dynamic_slice_in_dim(kv_gain[0], tp_rank * features, features)
    kv_input = (incoming_wide * kv_gain_part[None, :]).astype(jnp.bfloat16)
    kv_weight = key_value_weight[0]
    span = kv_weight.shape[1] // tp_count
    mapped_rows = jnp.dot(kv_input, kv_weight, preferred_element_type=jnp.float32)
    kv_span = lax.dynamic_slice_in_dim(mapped_rows, tp_rank * span, span, 1)
    mapped_bits = mapped_rows.astype(jnp.bfloat16)
    for k in range(1, tp_count):
        part = lax.dynamic_slice_in_dim(mapped_bits, lax.rem(tp_rank + k, tp_count) * span, span, 1)
        kv_span = kv_span + passed_along(part, "tp", k).astype(jnp.float32)
    kv_span = kv_span * scale_rows[:, None]
    span_width = kv_span.shape[1]
    heads_here = span_width // HEAD_SIZE
    divide_heads = kv_span.reshape(tok_rows, heads_here, HEAD_SIZE)
    mean_square = jnp.mean(divide_heads * divide_heads, axis=2, keepdims=True)
    norm_applied = divide_heads * lax.rsqrt(mean_square + epsilon) * k_gain[0][None, None, :]
    head_index_list = tp_rank * heads_here + jnp.arange(heads_here, dtype=jnp.int32)
    kv_result = (
        jnp.where((head_index_list < KEY_VALUE_HEADS)[None, :, None], norm_applied, divide_heads)
        .reshape(tok_rows, span_width)
        .astype(jnp.bfloat16)
    )
    return (attended[None], layer_local[None], kv_result[None])


MESH = pl.DeviceIdType.MESH


def part_rows(rows):
    second = max(rows // 3 // 64 * 64, 64)
    return rows - second, second


def relay_kernel(
    sizes,
    lengths_in,
    queries_ref,
    keys_ref,
    values_ref,
    resid_ref,
    ffn_gain_in,
    w_gate_ref,
    w_up_ref,
    w_down_ref,
    kv_gain_in,
    kv_weight_ref,
    k_gain_in,
    attn_ref,
    layer_ref,
    kv_next_ref,
    gate_w,
    up_w,
    down_w,
    x_buf,
    h_buf,
    h_tail,
    g_buf,
    own_acc,
    other_acc,
    part_in,
    stream_in,
    y_buf,
    kv_in,
    kv_own,
    square_buf,
    square_tmp,
    kv_out,
    local_sem,
    out_sem,
    xz_send,
    xz_recv,
    xs_send,
    xs_recv,
    a_send,
    a_recv,
    h_send,
    h_recv,
    p_send,
    p_recv,
    r_send,
    r_recv,
    kv_recv,
    sq_send,
    sq_recv,
    relay_recv,
    relay_sum,
    lengths_ref,
    ffn_gain_ref,
    kv_gain_ref,
    k_gain_ref,
):
    seq_count, tp_count, pp_count = sizes
    s = lax.axis_index("seq")
    t = lax.axis_index("tp")
    p = lax.axis_index("pp")
    barrier = pltpu.get_barrier_semaphore()
    for k in range(1, tp_count):
        pl.semaphore_signal(
            barrier, inc=1, device_id={"tp": lax.rem(t + k, tp_count)}, device_id_type=MESH
        )
    pl.semaphore_signal(barrier, inc=1, device_id={"seq": 1 - s}, device_id_type=MESH)
    for k in (1, pp_count - 1):
        pl.semaphore_signal(
            barrier, inc=1, device_id={"pp": lax.rem(p + k, pp_count)}, device_id_type=MESH
        )
    rows = resid_ref.shape[1]
    features = resid_ref.shape[2]
    units = w_gate_ref.shape[1]
    width = w_gate_ref.shape[2]
    span = kv_next_ref.shape[2]
    parts = part_rows(rows)
    tail = parts[1] // 2
    kv_heads = keys_ref.shape[2] // HEAD_SIZE
    group = queries_ref.shape[2] // keys_ref.shape[2]
    group_span = group * HEAD_SIZE

    pieces = (
        (0, 0, parts[0]),
        (parts[0], 0, parts[0]),
        (2 * parts[0] + parts[1], parts[0], parts[1]),
        (2 * parts[0], parts[0], parts[1] - tail),
        (2 * parts[0] + parts[1] - tail, rows - tail, tail),
    )
    main = units // 128 * 128
    rest = units - main
    block_n = 256 if main % 256 == 0 else 128
    full_tiles = main // block_n
    split = full_tiles // 2 * block_n
    early, late = (0,), (1, 2) if rest else (1,)
    whole = early + late
    own_pieces = (0, 3, 4)

    def rows_of(c):
        return pl.ds(c * parts[0], parts[c])

    def remote(src, dst, send, recv, where):
        return pltpu.make_async_remote_copy(
            src_ref=src,
            dst_ref=dst,
            send_sem=send,
            recv_sem=recv,
            device_id=where,
            device_id_type=MESH,
        )

    def next_on_line(d):
        return lax.rem(t + 2 * d - 1 + tp_count, tp_count)

    def has_next(d):
        place = t + 2 * d - 1
        return (place >= 0) & (place < tp_count)

    def recv_slot(d, block):
        return lax.rem(block + d + tp_count - 2, tp_count - 1)

    def x_halves(c):
        return (0, 1) if c == 0 else (2,)

    def x_line(d, half, block, own=False):
        size = parts[0] // 2
        place = pl.ds(half * size, size) if half < 2 else rows_of(1)
        dst = x_buf.at[0, block, place]
        src = resid_ref.at[0, place] if own else dst
        return remote(
            src,
            dst,
            xz_send.at[half, block + 1 - d],
            xz_recv.at[half, recv_slot(d, block)],
            {"tp": next_on_line(d)},
        )

    def x_across(c, block, own=False):
        src = resid_ref.at[0, rows_of(c)] if own else x_buf.at[0, block, rows_of(c)]
        return remote(
            src,
            x_buf.at[1, block, rows_of(c)],
            xs_send.at[c, block],
            xs_recv.at[c, block],
            {"seq": 1 - s},
        )

    def subs_of(piece):
        return whole if piece < 3 else (3,) + ((2,) if rest else ())

    def h_line(d, piece, block, sub):
        first, _, count = pieces[piece]
        if sub == 2:
            ref = h_tail.at[block, pl.ds(first // 2, count // 2)]
        else:
            lanes = (pl.ds(0, split), pl.ds(split, main - split), None, pl.ds(0, main))[sub]
            ref = h_buf.at[block, pl.ds(first, count), lanes]
        slot = sub if piece < 3 else (0, 1)[sub == 2]
        recv = 3 * piece + slot if piece < 3 else 9 + 2 * (piece - 3) + slot
        sent = recv if piece < 3 else (recv - 9 if recv < 12 else 9)
        return remote(
            ref,
            ref,
            h_send.at[sent, block + 1 - d],
            h_recv.at[recv, recv_slot(d, block)],
            {"tp": next_on_line(d)},
        )

    key_row = kv_heads * rows
    kv_width = kv_heads * HEAD_SIZE

    def query_place(i):
        return down_w.at[pl.ds(i * rows, rows), pl.ds(0, group_span)]

    def key_place(side, which):
        return down_w.at[
            pl.ds(key_row + side * rows, rows), pl.ds(which * kv_width, kv_width)
        ]

    attn_rows = key_row + seq_count * rows

    def a_across(which):
        src = keys_ref if which == 0 else values_ref
        return remote(
            src.at[0],
            key_place(s, which),
            a_send.at[which],
            a_recv.at[which],
            {"seq": 1 - s},
        )

    def a_arrived(which):
        src = keys_ref if which == 0 else values_ref
        return remote(
            src.at[0],
            key_place(1 - s, which),
            a_send.at[which],
            a_recv.at[which],
            {"seq": 1 - s},
        )

    loads = {}

    def load(name, src, dst):
        loads[name] = pltpu.make_async_copy(src, dst, local_sem.at[len(loads)])
        loads[name].start()

    for i in range(kv_heads):
        load(
            ("q", i),
            queries_ref.at[0, :, pl.ds(i * group_span, group_span)],
            query_place(i),
        )
    load("lengths", lengths_in, lengths_ref)
    load("k", keys_ref.at[0], key_place(s, 0))
    load("v", values_ref.at[0], key_place(s, 1))
    load("x", resid_ref.at[0], x_buf.at[0, t])
    load("ffn_gain", ffn_gain_in, ffn_gain_ref)
    load("kv_gain", kv_gain_in, kv_gain_ref)
    load("k_gain", k_gain_in, k_gain_ref)
    load("gate", w_gate_ref.at[0], gate_w)
    load("up", w_up_ref.at[0], up_w)
    down_rows = w_down_ref.shape[1]
    load(
        "down1",
        w_down_ref.at[0, pl.ds(attn_rows, down_rows - attn_rows)],
        down_w.at[pl.ds(attn_rows, down_rows - attn_rows)],
    )

    pl.semaphore_wait(barrier, tp_count - 1 + 1 + 2)

    def send_own_x(d, c, when):
        @pl.when(has_next(d) & when)
        def _():
            for half in x_halves(c):
                x_line(d, half, t, True).start()

    late_low = (t >= 2) & (t <= tp_count - 2)
    late_high = (t >= 1) & (t <= tp_count - 3)
    always = t >= 0
    for d in (0, 1):
        send_own_x(d, 0, always)
    a_across(0).start()
    a_across(1).start()
    send_own_x(0, 1, jnp.logical_not(late_low))
    send_own_x(1, 1, jnp.logical_not(late_high))
    x_across(0, t, True).start()

    def x_events(c, k):
        def from_side(d):
            block = t + k * (1 - 2 * d)
            return lax.rem(block + tp_count, tp_count), (block >= 0) & (block < tp_count)

        for half in x_halves(c):
            for d in (0, 1):
                block, there = from_side(d)

                @pl.when(there)
                def _():
                    x_line(d, half, block).wait_recv()

                    @pl.when(has_next(d))
                    def _():
                        x_line(d, half, block).start()

        for d in (0, 1):
            block, there = from_side(d)

            @pl.when(there)
            def _():
                x_across(c, block).start()

    loads["lengths"].wait()
    bias = own_acc.at[:, pl.ds(0, seq_count * rows)]
    row_id = lax.broadcasted_iota(jnp.int32, (rows, seq_count * rows), 0) + s * rows
    col_id = lax.broadcasted_iota(jnp.int32, (rows, seq_count * rows), 1)
    bound = lengths_ref[0, 0]
    begin = jnp.zeros_like(row_id)
    for k in range(1, lengths_ref.shape[1]):
        begin = jnp.where(row_id >= bound, bound, begin)
        bound = bound + lengths_ref[0, k]
    own_acc[:, : seq_count * rows] = jnp.where(
        (col_id <= row_id) & (col_id >= begin), 0.0, negative
    )
    inv_root = 1.0 / math.sqrt(HEAD_SIZE)

    def attend(first, last):
        def one(index, carry):
            i = index // group
            j = lax.rem(index, group)
            place = pl.ds(pl.multiple_of(i * rows, 16), rows)
            lanes = pl.ds(pl.multiple_of(j * HEAD_SIZE, HEAD_SIZE), HEAD_SIZE)
            query = down_w[place, lanes]
            key = down_w[
                key_row : key_row + seq_count * rows,
                pl.ds(pl.multiple_of(i * HEAD_SIZE, HEAD_SIZE), HEAD_SIZE),
            ]
            value = down_w[
                key_row : key_row + seq_count * rows,
                pl.ds(pl.multiple_of(kv_width + i * HEAD_SIZE, HEAD_SIZE), HEAD_SIZE),
            ]
            scores = lax.dot_general(
                query, key, (((1,), (1,)), ((), ())), preferred_element_type=jnp.float32
            )
            masked = scores * inv_root + bias[...]
            peak = jnp.max(masked, axis=1, keepdims=True)
            expo = jnp.exp(masked - peak)
            total = jnp.sum(expo, axis=1, keepdims=True)
            mixed = jnp.dot(
                expo.astype(jnp.bfloat16), value, preferred_element_type=jnp.float32
            )
            down_w[place, lanes] = (mixed / total).astype(jnp.bfloat16)
            return carry

        lax.fori_loop(first, last, one, 0)

    heads = kv_heads * group
    middle_head = heads // 2
    x_events(0, 1)
    send_own_x(0, 1, late_low)
    send_own_x(1, 1, late_high)
    for i in range(kv_heads):
        loads[("q", i)].wait()
    loads["k"].wait()
    loads["v"].wait()
    a_arrived(0).wait_recv()
    a_arrived(1).wait_recv()
    attend(0, middle_head)
    for k in range(2, tp_count - 1):
        x_events(0, k)
    x_across(1, t, True).start()
    attend(middle_head, heads)
    x_events(1, 1)
    attn_copies = [
        pltpu.make_async_copy(
            query_place(i),
            attn_ref.at[0, :, pl.ds(i * group_span, group_span)],
            out_sem.at[i],
        )
        for i in range(kv_heads)
    ]
    for copy in attn_copies:
        copy.start()
    x_events(0, tp_count - 1)
    loads["x"].wait()
    for copy in attn_copies:
        copy.wait()
    load("down0", w_down_ref.at[0, pl.ds(0, attn_rows)], down_w.at[pl.ds(0, attn_rows)])

    lane_tiles = features // 128

    def normalise(side, c, first):
        def squares(block, acc):
            for j in range(lane_tiles):
                x = x_buf[side, block, rows_of(c), j * 128 : (j + 1) * 128].astype(jnp.float32)
                acc = acc + x * x
            return acc

        total = lax.fori_loop(0, tp_count, squares, jnp.zeros((parts[c], 128), jnp.float32))
        inverse = lax.rsqrt(jnp.sum(total, axis=1, keepdims=True) / width + epsilon)

        def write(block, carry):
            for j in range(lane_tiles):
                x = x_buf[side, block, rows_of(c), j * 128 : (j + 1) * 128].astype(jnp.float32)
                lanes = pl.ds(pl.multiple_of(block * features + j * 128, 128), 128)
                g_buf[first : first + parts[c], lanes] = (
                    x * inverse * ffn_gain_ref[0:1, lanes]
                ).astype(jnp.bfloat16)
            return carry

        lax.fori_loop(0, tp_count, write, 0)

    def gated(count, place):
        both = (((1,), (1,)), ((), ()))
        x = g_buf[0:count, :]
        g = lax.dot_general(x, gate_w[place, :], both, preferred_element_type=jnp.float32)
        u = lax.dot_general(x, up_w[place, :], both, preferred_element_type=jnp.float32)
        return g / (1.0 + jnp.exp(-g)) * u

    def hidden_group(group_pieces, hooks):
        first = pieces[group_pieces[0]][0]
        count = sum(pieces[piece][2] for piece in group_pieces)

        def one(i, carry):
            place = pl.ds(pl.multiple_of(i * block_n, block_n), block_n)
            h_buf[t, pl.ds(first, count), place] = gated(count, place).astype(jnp.bfloat16)
            for index, hook in hooks.items():
                pl.when(i == index)(hook)
            return carry

        lax.fori_loop(0, full_tiles, one, 0)
        if rest:
            hidden = gated(count, pl.ds(main, rest))
            for piece in group_pieces:
                start, _, size = pieces[piece]
                low = hidden[start - first : start - first + size // 2]
                high = hidden[start - first + size // 2 : start - first + size]
                h_tail[t, pl.ds(start // 2, size // 2), :] = jnp.concatenate(
                    [low, high], axis=1
                ).astype(jnp.bfloat16)

    def send_hidden(piece, subs, inward=None):
        for d in (0, 1):
            place = t + 2 * d - 1
            ending = (place == 0) | (place == tp_count - 1)
            turn = has_next(d)
            if inward is not None:
                turn = turn & (ending if inward else jnp.logical_not(ending))

            @pl.when(turn)
            def _():
                for sub in subs:
                    h_line(d, piece, t, sub).start()

    def forward(piece, subs, k):
        if k > tp_count - 2:
            return
        for d in (0, 1):
            block = t + k * (1 - 2 * d)
            block_safe = lax.rem(block + tp_count, tp_count)

            @pl.when((block >= 0) & (block < tp_count) & has_next(d))
            def _():
                for sub in subs:
                    h_line(d, piece, block_safe, sub).wait_recv()
                    h_line(d, piece, block_safe, sub).start()

    def forwards(piece, subs, low):
        for k in range(low, tp_count - 1):
            forward(piece, subs, k)

    down_n = 256 if features % 256 == 0 else 128

    def down(group_pieces, block, fresh):
        first, own_first, _ = pieces[group_pieces[0]]
        count = sum(pieces[piece][2] for piece in group_pieces)
        own = group_pieces[0] in own_pieces
        acc = own_acc.at[pl.ds(own_first, count)] if own else other_acc.at[pl.ds(0, count)]
        if rest:
            extra = []
            for piece in group_pieces:
                start, _, size = pieces[piece]
                packed = h_tail[block, pl.ds(start // 2, size // 2), :]
                extra += [packed[:, :rest], packed[:, rest:]]
            extra = jnp.concatenate(extra, axis=0)

        def one(i, carry):
            lanes = pl.ds(pl.multiple_of(i * down_n, down_n), down_n)
            term = jnp.dot(
                h_buf[block, pl.ds(first, count), :],
                down_w[pl.ds(pl.multiple_of(block * units, 16), main), lanes],
                preferred_element_type=jnp.float32,
            )
            if rest:
                term = term + jnp.dot(
                    extra,
                    down_w[pl.ds(pl.multiple_of(block * units + main, 16), rest), lanes],
                    preferred_element_type=jnp.float32,
                )
            if fresh:
                acc[:, lanes] = term
            else:
                acc[:, lanes] += term
            return carry

        lax.fori_loop(0, features // down_n, one, 0)

    def down_others(group_pieces, low, high):
        def one(index, carry):
            k = index // 2 + 1
            d = lax.rem(index, 2)
            block = t + k * (1 - 2 * d)
            block_safe = lax.rem(block + tp_count, tp_count)

            @pl.when((block >= 0) & (block < tp_count))
            def _():
                @pl.when(jnp.logical_not(has_next(d)))
                def _():
                    for piece in group_pieces:
                        for sub in subs_of(piece):
                            h_line(d, piece, block_safe, sub).wait_recv()

                down(group_pieces, block_safe, False)

            return carry

        lax.fori_loop(2 * (low - 1), 2 * (high - 1), one, 0)

    def wait_other_x(c):
        def one(block, carry):
            x_across(c, block).wait_recv()
            return carry

        lax.fori_loop(0, tp_count, one, 0)

    def part_copy(c):
        return remote(
            x_buf.at[1, 0, rows_of(c)],
            part_in.at[rows_of(c)],
            p_send.at[c],
            p_recv.at[c],
            {"seq": 1 - s},
        )

    def send_part(c):
        x_buf[1, 0, rows_of(c)] = other_acc[0 : parts[c], :].astype(jnp.bfloat16)
        part_copy(c).start()

    def stream_copy(q):
        _, first, count = pieces[own_pieces[q]]
        return remote(
            x_buf.at[1, 1, pl.ds(first, count)],
            stream_in.at[pl.ds(first, count)],
            r_send.at[q],
            r_recv.at[q],
            {"pp": lax.rem(p + 1, pp_count)},
        )

    def layer_copy(q):
        _, first, count = pieces[own_pieces[q]]
        return pltpu.make_async_copy(
            x_buf.at[1, 1, pl.ds(first, count)],
            layer_ref.at[0, pl.ds(first, count)],
            out_sem.at[kv_heads + q],
        )

    def finish_layer(q):
        _, first, count = pieces[own_pieces[q]]
        place = pl.ds(first, count)
        x_buf[1, 1, place] = (
            x_buf[0, t, place].astype(jnp.float32)
            + (own_acc[place, :] + part_in[place, :].astype(jnp.float32))
        ).astype(jnp.bfloat16)
        stream_copy(q).start()
        layer_copy(q).start()

    def hops(source, target):
        return lax.rem(target - source + tp_count, tp_count)

    def sum_sem(q, k):
        return xz_send.at[q, k] if q < 2 else xs_send.at[0, k]

    def square_sem(q, k):
        return sq_send.at[q, k]

    def own_place(q):
        _, first, count = pieces[own_pieces[q]]
        return pl.ds(first, count)

    def kv_copy(q, k, source, target):
        return remote(
            g_buf.at[own_place(q), pl.ds(pl.multiple_of(k * span, HEAD_SIZE), span)],
            kv_in.at[source, own_place(q)],
            sum_sem(q, k),
            kv_recv.at[q, hops(source, target)],
            {"tp": target},
        )

    def relay_copy(q, k, slot, target):
        return remote(
            g_buf.at[own_place(q), pl.ds(pl.multiple_of(k * span, HEAD_SIZE), span)],
            x_buf.at[1, 2, own_place(q), pl.ds(slot * span, span)],
            sum_sem(q, k),
            relay_recv.at[slot],
            {"tp": target},
        )

    def square_copy(q, k, source, target):
        ref = square_buf.at[q, source]
        return remote(ref, ref, square_sem(q, k), sq_recv.at[q, hops(source, target)], {"tp": target})

    def relays(q):
        return q < 1

    def partial_sum(q, target):
        return jnp.dot(
            y_buf[0 : pieces[own_pieces[q]][2], :],
            gate_w[0:features, pl.ds(pl.multiple_of(target * span, HEAD_SIZE), span)],
            preferred_element_type=jnp.float32,
        )

    def start_kv(q):
        _, first, count = pieces[own_pieces[q]]
        place = pl.ds(first, count)
        stream_copy(q).wait_recv()
        total = jnp.zeros((count, 128), jnp.float32)
        for j in range(lane_tiles):
            lanes = slice(j * 128, (j + 1) * 128)
            x = stream_in[place, lanes].astype(jnp.float32)
            total = total + x * x
            gain = kv_gain_ref[0:1, pl.ds(pl.multiple_of(t * features + j * 128, 128), 128)]
            y_buf[0:count, lanes] = (x * gain).astype(jnp.bfloat16)
        if count < 128:
            square_tmp[...] = jnp.zeros_like(square_tmp)
        square_tmp[0:count, :] = jnp.broadcast_to(
            jnp.sum(total, axis=1, keepdims=True), (count, 128)
        )
        square_buf[q, t] = jnp.transpose(square_tmp[...])[0:8]
        for k in range(1, tp_count):
            square_copy(q, k, t, lax.rem(t + k, tp_count)).start()
        for j in range(tp_count - 1):
            near = t >= tp_count // 2
            target = jnp.where(near, j, tp_count - 1 - j)
            target = jnp.where(near & (j >= t), j + 1, target)
            target = jnp.where(jnp.logical_not(near) & (tp_count - 1 - j <= t), tp_count - 2 - j, target)
            k = lax.rem(target - t + tp_count, tp_count)
            lanes = pl.ds(pl.multiple_of(k * span, HEAD_SIZE), span)
            term = partial_sum(q, target)
            if not relays(q):
                g_buf[place, lanes] = term.astype(jnp.bfloat16)
                kv_copy(q, k, t, target).start()
            else:
                low = (target == 0) & (t >= 1)
                high = (target == tp_count - 1) & (t <= tp_count - 2)
                at_relay = (low & (t == 1)) | (high & (t == tp_count - 2))

                @pl.when(at_relay)
                def _():
                    relay_sum[0:count, :] = term

                @pl.when(jnp.logical_not(at_relay))
                def _():
                    g_buf[place, lanes] = term.astype(jnp.bfloat16)

                @pl.when(low & (t >= 2))
                def _():
                    relay_copy(q, k, lax.rem(t - 2 + tp_count, tp_count), 1).start()

                @pl.when(high & (t <= tp_count - 3))
                def _():
                    slot = lax.rem(2 * tp_count - 3 - t, tp_count)
                    relay_copy(q, k, slot, tp_count - 2).start()

                @pl.when(jnp.logical_not(low) & jnp.logical_not(high))
                def _():
                    kv_copy(q, k, t, target).start()

        kv_own[place, :] = partial_sum(q, t)

    def relay_kv(q):
        _, first, count = pieces[own_pieces[q]]
        place = pl.ds(first, count)
        for end, relay in ((0, 1), (tp_count - 1, tp_count - 2)):
            k = (end - relay + tp_count) % tp_count

            @pl.when(t == relay)
            def _():
                total = relay_sum[0:count, :]
                for slot in range(tp_count - 2):
                    relay_copy(q, k, slot, relay).wait_recv()
                    total = total + x_buf[
                        1, 2, place, slot * span : (slot + 1) * span
                    ].astype(jnp.float32)
                g_buf[place, k * span : (k + 1) * span] = total.astype(jnp.bfloat16)
                kv_copy(q, k, t, end).start()

    def kv_out_copy(q):
        _, first, count = pieces[own_pieces[q]]
        return pltpu.make_async_copy(
            kv_out.at[pl.ds(first, count)],
            kv_next_ref.at[0, pl.ds(first, count)],
            out_sem.at[kv_heads + 3 + q],
        )

    def finish_kv(q):
        _, first, count = pieces[own_pieces[q]]
        place = pl.ds(first, count)
        square = square_buf[q, t]
        for k in range(1, tp_count):
            source = lax.rem(t + tp_count - k, tp_count)
            square_copy(q, k, source, t).wait_recv()
            square = square + square_buf[q, source]
        column = jnp.transpose(jnp.broadcast_to(square[0:1], (128, 128)))[0:count, 0:1]
        scale = lax.rsqrt(column / width + epsilon)
        for k in range(1, tp_count):
            source = lax.rem(t + tp_count - k, tp_count)
            through = ((t == 0) & (source > 1)) | (
                (t == tp_count - 1) & (source < tp_count - 2)
            )
            if relays(q):

                @pl.when(jnp.logical_not(through))
                def _():
                    kv_copy(q, k, source, t).wait_recv()
                    kv_own[place, :] += kv_in[source, place, :].astype(jnp.float32)

            else:
                kv_copy(q, k, source, t).wait_recv()
                kv_own[place, :] += kv_in[source, place, :].astype(jnp.float32)
        total = kv_own[place, :]
        total = total * scale
        heads_here = span // HEAD_SIZE
        for h in range(heads_here):
            lanes = slice(h * HEAD_SIZE, (h + 1) * HEAD_SIZE)
            x = total[:, lanes]
            mean_square = jnp.mean(x * x, axis=1, keepdims=True)
            after = x * lax.rsqrt(mean_square + epsilon) * k_gain_ref[0:1, :]
            head = jnp.zeros_like(x, jnp.int32) + (t * heads_here + h)
            kv_out[place, lanes] = jnp.where(head < KEY_VALUE_HEADS, after, x).astype(jnp.bfloat16)
        kv_out_copy(q).start()

    def x_left():
        for c in (0, 1):

            def one(block, carry):
                for d in (0, 1):
                    came = (block - t) * (1 - 2 * d) >= 0

                    @pl.when(has_next(d) & came)
                    def _():
                        for half in x_halves(c):
                            x_line(d, half, block).wait_send()

                x_across(c, block).wait_send()
                return carry

            lax.fori_loop(0, tp_count, one, 0)

    def hidden_left(piece):
        def one(block, carry):
            for d in (0, 1):
                came = (block - t) * (1 - 2 * d) >= 0

                @pl.when(has_next(d) & came)
                def _():
                    for sub in subs_of(piece):
                        h_line(d, piece, block, sub).wait_send()

            return carry

        lax.fori_loop(0, tp_count, one, 0)

    def kv_left(q):
        stream_copy(q).wait_send()
        layer_copy(q).wait()
        for k in range(1, tp_count):
            kv_copy(q, k, t, lax.rem(t + k, tp_count)).wait_send()
            square_copy(q, k, t, lax.rem(t + k, tp_count)).wait_send()

    last = tp_count
    for name in ("ffn_gain", "kv_gain", "k_gain", "gate"):
        loads[name].wait()
    loads["up"].wait()
    normalise(0, 0, 0)
    middle = full_tiles // 2 - 1

    def inner_x():
        for k in range(2, tp_count - 1):
            x_events(1, k)

    hidden_group(
        (0,), {middle - 1: inner_x, middle: functools.partial(send_hidden, 0, early)}
    )
    send_hidden(0, late)
    x_events(1, tp_count - 1)
    wait_other_x(0)
    forward(0, early, 1)
    normalise(1, 0, 0)
    normalise(0, 1, parts[0])

    hidden_group(
        (1, 3, 4),
        {
            middle - 1: functools.partial(forward, 0, late, 1),
            middle: functools.partial(send_hidden, 1, early),
            middle + 1: functools.partial(forwards, 0, early, 2),
            full_tiles - 1: functools.partial(forwards, 0, late, 2),
        },
    )
    send_hidden(1, late)
    wait_other_x(1)
    forward(1, early, 1)
    normalise(1, 1, 0)
    hidden_group(
        (2,),
        {
            middle: functools.partial(send_hidden, 2, early, False),
            middle + 1: functools.partial(forward, 1, late, 1),
            middle + 2: functools.partial(forwards, 1, early, 2),
        },
    )
    send_hidden(2, late, False)
    hidden_left(0)
    send_hidden(3, subs_of(3), False)
    send_hidden(4, subs_of(4), False)
    load(
        "kv",
        kv_weight_ref.at[0],
        gate_w.at[pl.ds(0, features), pl.ds(0, tp_count * span)],
    )
    loads["down0"].wait()
    loads["down1"].wait()
    down((0,), t, True)
    forwards(1, late, 2)
    send_hidden(2, whole, True)
    down_others((0,), 1, last)
    down((1,), t, True)
    forward(2, whole, 1)
    down_others((1,), 1, last)
    send_part(0)
    down((2,), t, True)
    forwards(2, whole, 2)
    send_hidden(3, subs_of(3), True)
    send_hidden(4, subs_of(4), True)
    down_others((2,), 1, last)
    send_part(1)
    x_left()
    forward(3, subs_of(3), 1)
    forward(4, subs_of(4), 1)
    part_copy(0).wait_recv()
    finish_layer(0)
    down((3, 4), t, True)
    down_others((3, 4), 1, 2)
    hidden_left(1)
    loads["kv"].wait()
    forwards(3, subs_of(3), 2)
    start_kv(0)
    forwards(4, subs_of(4), 2)
    down_others((3, 4), 2, last - 1)
    down_others((3,), last - 1, last)
    part_copy(1).wait_recv()
    finish_layer(1)
    relay_kv(0)
    down_others((4,), last - 1, last)
    finish_layer(2)
    for piece in (2, 3, 4):
        hidden_left(piece)
    start_kv(1)
    for which in (0, 1):
        a_across(which).wait_send()
        part_copy(which).wait_send()
    start_kv(2)
    finish_kv(0)
    kv_left(0)
    finish_kv(1)
    kv_left(1)
    finish_kv(2)
    kv_left(2)
    for q in range(3):
        kv_out_copy(q).wait()


def settle_kernel(cuts, a_ref, b_ref, c_ref, a_out, b_out, c_out, a_buf, b_buf, c_buf, sem):
    into, out = [], []
    for src, buf, dst, cut in zip(
        (a_ref, b_ref, c_ref), (a_buf, b_buf, c_buf), (a_out, b_out, c_out), cuts
    ):
        count = src.shape[1] // cut
        for i in range(cut):
            place = pl.ds(i * count, count)
            n = len(into)
            into.append(
                pltpu.make_async_copy(src.at[:, place], buf.at[:, place], sem.at[0, n])
            )
            out.append(pltpu.make_async_copy(buf.at[:, place], dst.at[:, place], sem.at[1, n]))
    for copy in into:
        copy.start()
    for first, second in zip(into, out):
        first.wait()
        second.start()
    for copy in out:
        copy.wait()


def fits(shape, queries, keys, doc_lengths, resid, w_gate, w_down, key_value_weight):
    rows, features = resid.shape[1:]
    units = w_gate.shape[2]
    span = key_value_weight.shape[2] // shape["tp"]
    tp_span = key_value_weight.shape[2]
    group_span = HEAD_SIZE * queries.shape[2] // keys.shape[2]
    return (
        shape["seq"] == 2
        and shape["pp"] >= 3
        and shape["tp"] >= 3
        and rows % 64 == 0
        and features % 128 == 0
        and units % 128 in (0, 64)
        and units >= 512
        and 128 <= rows <= 192
        and part_rows(rows)[0] <= 128
        and (shape["tp"] - 2) * span <= features
        and span % HEAD_SIZE == 0
        and features <= units
        and tp_span <= resid.shape[2] * shape["tp"]
        and 2 * span <= features
        and group_span <= features
        and keys.shape[2] * 2 <= features
        and 2 * rows <= features
        and queries.shape[2] // group_span * rows + 2 * rows < w_down.shape[1]
    )


def body(
    shape,
    queries,
    keys,
    values,
    doc_lengths,
    resid,
    ffn_gain,
    w_gate,
    w_up,
    w_down,
    kv_gain,
    key_value_weight,
    k_gain,
):
    if not fits(shape, queries, keys, doc_lengths, resid, w_gate, w_down, key_value_weight):
        return plain_body(
            queries,
            keys,
            values,
            doc_lengths,
            resid,
            ffn_gain,
            w_gate,
            w_up,
            w_down,
            kv_gain,
            key_value_weight,
            k_gain,
        )
    sizes = (shape["seq"], shape["tp"], shape["pp"])
    tp_count = shape["tp"]
    rows, features = resid.shape[1:]
    width, units = w_gate.shape[1:]
    span = key_value_weight.shape[2] // tp_count
    half = part_rows(rows)[0]
    kv_heads = keys.shape[2] // HEAD_SIZE
    bf16, f32 = jnp.bfloat16, jnp.float32
    hbm = pl.BlockSpec(memory_space=pl.ANY)
    dma = pltpu.SemaphoreType.DMA
    parts = pl.pallas_call(
            functools.partial(relay_kernel, sizes),
            out_shape=(
                jax.ShapeDtypeStruct(queries.shape, bf16),
                jax.ShapeDtypeStruct(resid.shape, bf16),
                jax.ShapeDtypeStruct((1, rows, span), bf16),
            ),
            in_specs=[hbm] * 12,
            out_specs=(hbm, hbm, hbm),
            scratch_shapes=[
                pltpu.VMEM((units, width), bf16),
                pltpu.VMEM((units, width), bf16),
                pltpu.VMEM(w_down.shape[1:], bf16),
                pltpu.VMEM((2, tp_count, rows, features), bf16),
                pltpu.VMEM((tp_count, 2 * rows, units // 128 * 128), bf16),
                pltpu.VMEM((tp_count, rows, 128), bf16),
                pltpu.VMEM((rows, width), bf16),
                pltpu.VMEM((rows, features), f32),
                pltpu.VMEM((half, features), f32),
                pltpu.VMEM((rows, features), bf16),
                pltpu.VMEM((rows, features), bf16),
                pltpu.VMEM((half, features), bf16),
                pltpu.VMEM((tp_count, rows, span), bf16),
                pltpu.VMEM((rows, span), f32),
                pltpu.VMEM((3, tp_count, 8, 128), f32),
                pltpu.VMEM((128, 128), f32),
                pltpu.VMEM((rows, span), bf16),
                dma((kv_heads + 12,)),
                dma((kv_heads + 6,)),
                dma((3, tp_count + 1)),
                dma((3, tp_count - 1)),
                dma((2, tp_count)),
                dma((2, tp_count)),
                dma((2,)),
                dma((2,)),
                dma((10, tp_count + 1)),
                dma((13, tp_count - 1)),
                dma((2,)),
                dma((2,)),
                dma((3,)),
                dma((3,)),
                dma((3, tp_count)),
                dma((3, tp_count)),
                dma((3, tp_count)),
                dma((tp_count - 2,)),
                pltpu.VMEM((half, span), f32),
                pltpu.SMEM(doc_lengths.shape, doc_lengths.dtype),
                pltpu.VMEM(ffn_gain.shape, f32),
                pltpu.VMEM(kv_gain.shape, f32),
                pltpu.VMEM(k_gain.shape, f32),
            ],
            compiler_params=pltpu.CompilerParams(
                collective_id=0, has_side_effects=True, vmem_limit_bytes=67043328
            ),
            name="relay_step",
        )(
            doc_lengths,
            queries,
            keys,
            values,
            resid,
            ffn_gain,
            jnp.swapaxes(w_gate, 1, 2),
            jnp.swapaxes(w_up, 1, 2),
            w_down,
            kv_gain,
            key_value_weight,
            k_gain,
        )
    hbm_shapes = [jax.ShapeDtypeStruct(part.shape, part.dtype) for part in parts]
    return tuple(
        pl.pallas_call(
            functools.partial(settle_kernel, (4, 2, 1)),
            out_shape=tuple(hbm_shapes),
            in_specs=[hbm] * 3,
            out_specs=(hbm,) * 3,
            scratch_shapes=[pltpu.VMEM(part.shape, part.dtype) for part in parts] + [dma((2, 7))],
            name="settle",
        )(*parts)
    )


def solution(mesh):
    placed = (
        P("pp", "seq", "tp"),
        P("pp", "seq", "tp"),
        P("pp", "seq", "tp"),
        P("pp", None),
        P("pp", "seq", "tp"),
        P("pp", None),
        P("pp", None, ("seq", "tp")),
        P("pp", None, ("seq", "tp")),
        P("pp", "seq", "tp"),
        P("pp", None),
        P("pp", "tp", None),
        P("pp", None),
    )
    return jax.shard_map(
        functools.partial(body, dict(mesh.shape)),
        mesh=mesh,
        in_specs=placed,
        out_specs=(P("pp", "seq", "tp"), P("pp", "seq", "tp"), P("pp", "seq", "tp")),
        check_vma=False,
    )
```
